128 devices in a mesh: tp: 16 (over z, y), dp: 8 (over x, core).
Axes of the slice: x: 4, y: 4, z: 4, core: 2. Of those that a mesh axis runs over, the one named last changes fastest.
Arguments:
- x_in: bfloat16 [2, 8192, 3072], P(None, ('dp', 'tp'))
- w_gate: bfloat16 [3072, 8192], P('dp', 'tp')
- w_up: bfloat16 [3072, 8192], P('dp', 'tp')
- w_down: bfloat16 [8192, 3072], P('tp', 'dp')
- grad_y: bfloat16 [2, 8192, 3072], P(None, ('dp', 'tp'))
Outputs:
- output 1: bfloat16 [2, 8192, 3072], P(None, ('dp', 'tp'))
- output 2: bfloat16 [2, 8192, 3072], P(None, ('dp', 'tp'))
- output 3: float32 [3072, 8192], P('dp', 'tp')
- output 4: float32 [3072, 8192], P('dp', 'tp')
- output 5: float32 [8192, 3072], P('tp', 'dp')
All inputs are finite; a program needn't handle non-finite values.
Results may differ from the reference program's by a relative error of at most 0.00102.
Values are sent between devices in bfloat16 or wider.
A program may use at most 1 GiB of HBM per device.

```python
import jax
import jax.numpy as jnp
from jax import lax

D = 3072
FF = 8192
T_ROWS = 64
DATA_SIZE = 8
MODEL_SIZE = 16
MICRO_STEPS = 2
ALL_ROWS = DATA_SIZE * MODEL_SIZE * T_ROWS


def setup_inputs(seed: int = 0) -> dict:
    keys = jax.random.split(jax.random.key(seed), 5)
    x_in = jax.random.normal(keys[0], (MICRO_STEPS, ALL_ROWS, D), jnp.float32)
    w_gate = jax.random.normal(keys[1], (D, FF), jnp.float32) * D ** -0.5
    w_up = jax.random.normal(keys[2], (D, FF), jnp.float32) * D ** -0.5
    w_down = jax.random.normal(keys[3], (FF, D), jnp.float32) * FF ** -0.5
    grad_y = jax.random.normal(keys[4], (MICRO_STEPS, ALL_ROWS, D), jnp.float32)
    return {"x_in": x_in.astype(jnp.bfloat16), "w_gate": w_gate.astype(jnp.bfloat16), "w_up": w_up.astype(jnp.bfloat16), "w_down": w_down.astype(jnp.bfloat16), "grad_y": grad_y.astype(jnp.bfloat16)}


def mlp_rows(x_blk, dy_blk, w_gate, w_up, w_down):
    gate_pre = jnp.dot(x_blk, w_gate, preferred_element_type=jnp.float32)
    up_pre = jnp.dot(x_blk, w_up, preferred_element_type=jnp.float32)
    sig_gate = jax.nn.sigmoid(gate_pre)
    act_gate = gate_pre * sig_gate
    hidden = (act_gate * up_pre).astype(jnp.bfloat16)
    y_blk = (x_blk.astype(jnp.float32) + jnp.dot(hidden, w_down, preferred_element_type=jnp.float32)).astype(jnp.bfloat16)
    grad_h = jnp.dot(dy_blk, w_down.T, preferred_element_type=jnp.float32)
    grad_gate = (grad_h * up_pre * sig_gate * (1.0 + gate_pre * (1.0 - sig_gate))).astype(jnp.bfloat16)
    grad_up = (grad_h * act_gate).astype(jnp.bfloat16)
    dx_blk = (dy_blk.astype(jnp.float32) + jnp.dot(grad_gate, w_gate.T, preferred_element_type=jnp.float32) + jnp.dot(grad_up, w_up.T, preferred_element_type=jnp.float32)).astype(jnp.bfloat16)
    dw_gate = jnp.dot(x_blk.T, grad_gate, preferred_element_type=jnp.float32)
    dw_up = jnp.dot(x_blk.T, grad_up, preferred_element_type=jnp.float32)
    dw_down = jnp.dot(hidden.T, dy_blk, preferred_element_type=jnp.float32)
    return y_blk, dx_blk, dw_gate, dw_up, dw_down


def reference(x_in, w_gate, w_up, w_down, grad_y):
    blocks = MICRO_STEPS * DATA_SIZE * MODEL_SIZE
    x_blocks = x_in.reshape(blocks, T_ROWS, D)
    dy_blocks = grad_y.reshape(blocks, T_ROWS, D)

    def scan_step(acc_sums, row_pair):
        y_blk, dx_blk, dw_gate, dw_up, dw_down = mlp_rows(row_pair[0], row_pair[1], w_gate, w_up, w_down)
        new_sums = (acc_sums[0] + dw_gate, acc_sums[1] + dw_up, acc_sums[2] + dw_down)
        return new_sums, (y_blk, dx_blk)

    zero_sums = (jnp.zeros((D, FF), jnp.float32), jnp.zeros((D, FF), jnp.float32), jnp.zeros((FF, D), jnp.float32))
    (sum_gate, sum_up, sum_down), (y_blocks, dx_blocks) = lax.scan(scan_step, zero_sums, (x_blocks, dy_blocks))
    return (y_blocks.reshape(x_in.shape), dx_blocks.reshape(x_in.shape), sum_gate, sum_up, sum_down)
```

```python
import functools
import heapq

import jax
import jax.numpy as jnp
from jax import lax
from jax.experimental import pallas as pl
from jax.experimental.pallas import tpu as pltpu
from jax.sharding import PartitionSpec as P

MESH = pl.DeviceIdType.MESH
F32 = jnp.float32
BF16 = jnp.bfloat16
ICI_RATE = 46.0e3
CORE_RATE = 550.0e3


class Place:
    def __init__(self):
        t = lax.axis_index("tp")
        d = lax.axis_index("dp")
        self.z, self.y = t // 4, t % 4
        self.x, self.c = d // 2, d % 2
        self.b = self.y % 2
        self.a = self.y // 2
        y_tok = self.y + 1 - 2 * self.b
        y_wgt = 3 - self.y
        at = lambda z, y, x, c: {"tp": z * 4 + y, "dp": x * 2 + c}
        z, y, x, c = self.z, self.y, self.x, self.c
        self.zp, self.zm, self.z2 = (z + 1) % 4, (z + 3) % 4, (z + 2) % 4
        self.xp, self.xm, self.x2 = (x + 1) % 4, (x + 3) % 4, (x + 2) % 4
        self.dev = {
            "z+": at(self.zp, y, x, c),
            "z-": at(self.zm, y, x, c),
            "x+": at(z, y, self.xp, c),
            "x-": at(z, y, self.xm, c),
            "tok": at(z, y_tok, x, c),
            "wgt": at(z, y_wgt, x, c),
            "core": at(z, y, x, 1 - c),
        }

    def barrier(self):
        sem = pltpu.get_barrier_semaphore()
        for dev in self.dev.values():
            pl.semaphore_signal(sem, inc=1, device_id=dev, device_id_type=MESH)
        pl.semaphore_wait(sem, len(self.dev))


class Net:
    def __init__(self, place, send_sems, recv_sems):
        self.place, self.send_sems, self.recv_sems = place, send_sems, recv_sems
        self.used = 0
        self.sent = []
        self.heap = []
        self.seq = 0
        self.now = 0.0
        self.free = {}

    def send(self, link, src, dst, land):
        i = self.used
        self.used += 1
        dev = self.place.dev[link]
        copy = pltpu.make_async_remote_copy(
            src_ref=src, dst_ref=dst, send_sem=self.send_sems.at[i], recv_sem=self.recv_sems.at[i],
            device_id=dev, device_id_type=MESH,
        )
        copy.start()
        self.sent.append(copy)
        arrive = pltpu.make_async_remote_copy(
            src_ref=land, dst_ref=land, send_sem=self.send_sems.at[i], recv_sem=self.recv_sems.at[i],
            device_id=dev, device_id_type=MESH,
        )
        size = 1
        for n in land.shape:
            size *= n
        size *= jnp.dtype(land.dtype).itemsize
        rate = CORE_RATE if link == "core" else ICI_RATE
        start = max(self.now, self.free.get(link, 0.0))
        self.free[link] = start + size / rate
        return [self.free[link] + 2.0, arrive, False]

    def when(self, arrivals, then, cost=0.0):
        self.seq += 1
        time = max([a[0] for a in arrivals], default=self.now)
        heapq.heappush(self.heap, (time, self.seq, arrivals, then, cost))

    def run(self):
        while self.heap:
            time, _, arrivals, then, cost = heapq.heappop(self.heap)
            self.now = max(self.now, time) + cost
            for a in arrivals:
                if not a[2]:
                    a[1].wait_recv()
                    a[2] = True
            then()
        for copy in self.sent:
            copy.wait_send()


def nothing():
    pass


def gather_ring_first(net, own, slot, half, ring, pair, me, each):
    r, rp, rm, r2, p = me
    up, down = ring
    from_down = net.send(up, own, slot(r, p), slot(rm, p))
    from_up = net.send(down, own, slot(r, p), slot(rp, p))
    other = net.send(pair, own, slot(r, p), slot(r, 1 - p))
    net.when([other], lambda: each(r, 1 - p))

    def pass_on(q):
        got = net.send(pair, slot(q, p), slot(q, p), slot(q, 1 - p))
        net.when([got], lambda: each(q, 1 - p))

    far = []

    def got_down():
        ref = half(slot(rm, p), 0)
        far.append(net.send(up, ref, ref, half(slot(r2, p), 0)))
        pass_on(rm)
        each(rm, p)
        if len(far) == 2:
            net.when(far, got_far)

    def got_up():
        ref = half(slot(rp, p), 1)
        far.append(net.send(down, ref, ref, half(slot(r2, p), 1)))
        pass_on(rp)
        each(rp, p)
        if len(far) == 2:
            net.when(far, got_far)

    def got_far():
        pass_on(r2)
        each(r2, p)

    net.when([from_down], got_down)
    net.when([from_up], got_up)


def gather_pair_first(net, own, slot, half, ring, pair, me, each):
    r, rp, rm, r2, p = me
    up, down = ring

    def around(src, q):
        from_down = net.send(up, src, slot(r, q), slot(rm, q))
        from_up = net.send(down, src, slot(r, q), slot(rp, q))
        far = []

        def got_down():
            ref = half(slot(rm, q), 0)
            far.append(net.send(up, ref, ref, half(slot(r2, q), 0)))
            each(rm, q)
            if len(far) == 2:
                net.when(far, lambda: each(r2, q))

        def got_up():
            ref = half(slot(rp, q), 1)
            far.append(net.send(down, ref, ref, half(slot(r2, q), 1)))
            each(rp, q)
            if len(far) == 2:
                net.when(far, lambda: each(r2, q))

        net.when([from_down], got_down)
        net.when([from_up], got_up)

    other = net.send(pair, own, slot(r, p), slot(r, 1 - p))

    def got_other():
        around(slot(r, 1 - p), 1 - p)
        each(r, 1 - p)

    net.when([other], got_other)
    around(own, p)


def gather_kernel(x_ref, dy_ref, wg_ref, wu_ref, wd_ref, x_all, dy_all, wg_all, wu_all, wd_all, own_sems, send_sems, recv_sems):
    here = Place()
    here.barrier()
    net = Net(here, send_sems, recv_sems)
    rows, cols = wg_ref.shape
    in_z = (here.z, here.zp, here.zm, here.z2, here.b)
    in_x = (here.x, here.xp, here.xm, here.x2, here.a)
    c = here.c

    tok_half = lambda ref, h: ref.at[h]
    up_half = lambda ref, h: ref.at[pl.ds(h * (rows // 2), rows // 2)]
    down_half = lambda ref, h: ref.at[pl.ds(h * (cols // 2), cols // 2)]

    def up_slot(ref, core):
        return lambda q, p: ref.at[p, q, core]

    def down_slot(core):
        def slot(q, p):
            return wd_all.at[p, :, pl.ds(pl.multiple_of((q * 2 + core) * rows, rows), rows)]
        return slot

    def across(mine, theirs):
        def each(q, p):
            got = net.send("core", mine(q, p), mine(q, p), theirs(q, p))
            net.when([got], nothing)
        return each

    jobs = []
    for fn, own, mine, theirs, half in (
        (gather_ring_first, wg_ref, up_slot(wg_all, c), up_slot(wg_all, 1 - c), up_half),
        (gather_pair_first, wu_ref, up_slot(wu_all, c), up_slot(wu_all, 1 - c), up_half),
        (gather_pair_first, wd_ref, down_slot(c), down_slot(1 - c), down_half),
    ):
        fn(net, own, mine, half, ("x+", "x-"), "wgt", in_x, across(mine, theirs))
        jobs.append((own, mine(here.x, here.a)))
        got = net.send("core", own, mine(here.x, here.a), theirs(here.x, here.a))
        net.when([got], nothing)
    gather_ring_first(net, x_ref, lambda q, p: x_all.at[q, p], tok_half, ("z+", "z-"), "tok", in_z, lambda q, p: None)
    gather_pair_first(net, dy_ref, lambda q, p: dy_all.at[q, p], tok_half, ("z+", "z-"), "tok", in_z, lambda q, p: None)
    jobs.append((x_ref, x_all.at[here.z, here.b]))
    jobs.append((dy_ref, dy_all.at[here.z, here.b]))
    keep = [pltpu.make_async_copy(src, dst, own_sems.at[i]) for i, (src, dst) in enumerate(jobs)]
    for copy in keep:
        copy.start()
    net.run()
    for copy in keep:
        copy.wait()


def add_rows(dst, src):
    if len(dst.shape) > 2:
        for i in range(dst.shape[0]):
            add_rows(dst.at[i], src.at[i])
        return
    step = 16

    @pl.loop(0, dst.shape[0] // step)
    def _(i):
        at = pl.ds(pl.multiple_of(i * step, step), step)
        dst[at, :] = dst[at, :] + src[at, :]


def reduce_kernel(
    x_ref, dy_ref, y_part, dx_part, g_part, u_part, d_part,
    y_out, dx_out, g_out, u_out, d_out,
    y_l1, y_l2, y_lp, dx_lp, dx_l1, dx_l2, g_lc, g_l1, g_l2, g_lp, u_lc, u_l1, u_l2, u_lp, d_lc, d_lp, d_l1, d_l2,
    y_st, dx_st, g_st, u_st, d_st, t_tmp, g_tmp, d_tmp, load_sems, send_sems, recv_sems,
):
    here = Place()
    here.barrier()
    net = Net(here, send_sems, recv_sems)
    z, zp, zm, z2, b = here.z, here.zp, here.zm, here.z2, here.b
    x, xp, xm, x2, a, c = here.x, here.xp, here.xm, here.x2, here.a, here.c
    rows = g_out.shape[0]
    cols = g_out.shape[1]

    def load(src, dst, sem=0):
        copy = pltpu.make_async_copy(src, dst, load_sems.at[sem])
        copy.start()
        return copy

    def fetch(src, dst):
        load(src, dst).wait()

    def add_from(dst, src, tmp):
        fetch(src, tmp)
        add_rows(dst, tmp)

    y_far = [
        net.send("z+", y_part.at[z2, :, 0], y_l1.at[0], y_l1.at[0]),
        net.send("z-", y_part.at[z2, :, 1], y_l1.at[1], y_l1.at[1]),
    ]
    y_near = []

    def y_pass(k, link, blk, last):
        def then():
            st = y_st.at[k]
            fetch(y_part.at[blk], st)
            tmp = t_tmp.at[:, 0]
            fetch(y_l1.at[k], tmp)
            for i in range(2):
                add_rows(st.at[i, k], tmp.at[i])
            y_near.append(net.send(link, st, y_l2.at[k], y_l2.at[k]))
            if len(y_near) == 2:
                net.when(y_near, y_own, 8.0)
        return then

    def y_own():
        st = y_st.at[2]
        fetch(y_part.at[z], st)
        add_from(st, y_l2.at[0], t_tmp)
        add_from(st, y_l2.at[1], t_tmp)
        last = net.send("tok", st.at[1 - b], y_lp, y_lp)
        net.when([last], y_end)

    def y_end():
        st = y_st.at[2, b]
        add_from(st, y_lp, t_tmp.at[0])
        for i in range(2):
            y_out[i] = (x_ref[i].astype(F32) + st[i]).astype(BF16)

    net.when([y_far[0]], y_pass(0, "z+", zp, y_far), 4.0)
    net.when([y_far[1]], y_pass(1, "z-", zm, y_far), 4.0)

    dx_pair = [net.send("tok", dx_part.at[s, 1 - b], dx_lp.at[k], dx_lp.at[k]) for k, s in enumerate((z2, zp, zm, z))]
    dx_near = []

    def dx_sum(k, s):
        st = dx_st.at[k]
        fetch(dx_part.at[s, b], st)
        add_from(st, dx_lp.at[k], t_tmp.at[0])
        return st

    def dx_begin():
        st = dx_sum(0, z2)
        one = net.send("z+", st.at[0], dx_l1.at[0], dx_l1.at[0])
        two = net.send("z-", st.at[1], dx_l1.at[1], dx_l1.at[1])
        net.when([one, dx_pair[1]], dx_pass(0, "z+", zp), 4.0)
        net.when([two, dx_pair[2]], dx_pass(1, "z-", zm), 4.0)

    def dx_pass(k, link, s):
        def then():
            st = dx_sum(1 + k, s)
            add_from(st.at[k], dx_l1.at[k], t_tmp.at[0, 0])
            dx_near.append(net.send(link, st, dx_l2.at[k], dx_l2.at[k]))
            if len(dx_near) == 2:
                net.when(dx_near + [dx_pair[3]], dx_end)
        return then

    def dx_end():
        st = dx_sum(3, z)
        add_from(st, dx_l2.at[0], t_tmp.at[0])
        add_from(st, dx_l2.at[1], t_tmp.at[0])
        for i in range(2):
            dx_out[i] = (dy_ref[i].astype(F32) + st[i]).astype(BF16)

    net.when([dx_pair[0]], dx_begin, 4.0)

    def up_blk(part):
        return lambda s, core: part.at[:, s, core]

    def down_blk(s, core):
        return d_part.at[:, :, pl.ds(pl.multiple_of((s * 2 + core) * rows, rows), rows)]

    order = (x2, xp, xm, x)
    sides = {}
    for k, s in enumerate(order):
        for name, blk, land in (("g", up_blk(g_part), g_lc), ("u", up_blk(u_part), u_lc), ("d", down_blk, d_lc)):
            sides[name, k] = net.send("core", blk(s, 1 - c), land.at[k], land.at[k])

    def w_sum(st, blk, land, tmp, k):
        fetch(blk(order[k], c), st.at[k])
        add_from(st.at[k], land.at[k], tmp)
        return st.at[k]

    def ring_first(name, blk, lc, l1, l2, lp, st, tmp, out):
        hold = {}

        def half(ref, h):
            return ref.at[:, pl.ds(h * (rows // 2), rows // 2)]

        def begin():
            v = w_sum(st, blk, lc, tmp, 0)
            one = net.send("x+", half(v, 0), l1.at[0], l1.at[0])
            two = net.send("x-", half(v, 1), l1.at[1], l1.at[1])
            net.when([sides[name, 1], one], go_on(0, "x+"), 3.0)
            net.when([sides[name, 2], two], go_on(1, "x-"), 3.0)

        def go_on(k, link):
            def then():
                v = w_sum(st, blk, lc, tmp, 1 + k)
                add_from(half(v, k), l1.at[k], half(tmp, 0))
                hold[k] = net.send(link, v, l2.at[k], l2.at[k])
                if len(hold) == 2:
                    net.when([hold[0], hold[1], sides[name, 3]], own, 4.0)
            return then

        def own():
            v = w_sum(st, blk, lc, tmp, 3)
            add_from(v, l2.at[0], tmp)
            add_from(v, l2.at[1], tmp)
            last = net.send("wgt", v.at[1 - a], lp, lp)
            net.when([last], end)

        def end():
            fetch(lp, tmp.at[0])
            out[...] = st[3, a] + tmp[0]

        net.when([sides[name, 0]], begin, 3.0)

    def pair_first(name, blk, lc, l1, l2, lp, st, tmp, out):
        hold = {}
        pairs = {}
        size = out.shape[0] // 2

        def half(ref, h):
            return ref.at[pl.ds(h * size, size)]

        def start(k):
            def then():
                v = w_sum(st, blk, lc, tmp, k)
                pairs[k] = net.send("wgt", v.at[1 - a], lp.at[k], lp.at[k])
                if k == 0:
                    net.when([pairs[0]], begin, 3.0)
            return then

        def join(k):
            v = st.at[k, a]
            add_from(v, lp.at[k], tmp.at[0])
            return v

        def begin():
            v = join(0)
            one = net.send("x+", half(v, 0), l1.at[0], l1.at[0])
            two = net.send("x-", half(v, 1), l1.at[1], l1.at[1])
            net.when([pairs[1], one], go_on(0, "x+"), 3.0)
            net.when([pairs[2], two], go_on(1, "x-"), 3.0)

        def go_on(k, link):
            def then():
                v = join(1 + k)
                add_from(half(v, k), l1.at[k], half(tmp.at[0], 0))
                hold[k] = net.send(link, v, l2.at[k], l2.at[k])
                if len(hold) == 2:
                    net.when([hold[0], hold[1], pairs[3]], end, 3.0)
            return then

        def end():
            v = join(3)
            add_from(v, l2.at[0], tmp.at[0])
            fetch(l2.at[1], tmp.at[0])
            out[...] = st[3, a] + tmp[0]

        for k in range(4):
            net.when([sides[name, k]], start(k), 3.0)

    ring_first("g", up_blk(g_part), g_lc, g_l1, g_l2, g_lp, g_st, g_tmp, g_out)
    ring_first("u", up_blk(u_part), u_lc, u_l1, u_l2, u_lp, u_st, g_tmp, u_out)
    pair_first("d", down_blk, d_lc, d_l1, d_l2, d_lp, d_st, d_tmp, d_out)
    net.run()


def solution(mesh):
    row_spec = P(None, ("dp", "tp"), None)
    in_specs = (row_spec, P("dp", "tp"), P("dp", "tp"), P("tp", "dp"), row_spec)
    out_specs = (row_spec, row_spec, P("dp", "tp"), P("dp", "tp"), P("tp", "dp"))
    vmem = pl.BlockSpec(memory_space=pltpu.VMEM)
    hbm = pl.BlockSpec(memory_space=pl.ANY)
    dma = pltpu.SemaphoreType.DMA
    S = jax.ShapeDtypeStruct

    def local_step(x_loc, wg, wu, wd, dy_loc):
        micro, rows, width = x_loc.shape
        wr, wc = wg.shape
        x_all, dy_all, wg_all, wu_all, wd_all = pl.pallas_call(
            gather_kernel,
            name="gather",
            out_shape=(
                S((4, 2, micro, rows, width), BF16),
                S((4, 2, micro, rows, width), BF16),
                S((2, 4, 2, wr, wc), BF16),
                S((2, 4, 2, wr, wc), BF16),
                S((2, wc, 8 * wr), BF16),
            ),
            in_specs=[vmem] * 5,
            out_specs=[hbm] * 5,
            scratch_shapes=[dma((5,)), dma((80,)), dma((80,))],
            compiler_params=pltpu.CompilerParams(collective_id=0, has_side_effects=True),
        )(x_loc, dy_loc, wg, wu, wd)

        n = 8 * micro * rows
        xs = x_all.reshape(n, width)
        ds = dy_all.reshape(n, width)
        hs, das, dbs, dgs, dus = [], [], [], [], []
        dx_part = None
        for k in range(2):
            wgk = wg_all[k].reshape(width, wc)
            wuk = wu_all[k].reshape(width, wc)
            wdk = wd_all[k]
            a = jnp.dot(xs, wgk, preferred_element_type=F32)
            b = jnp.dot(xs, wuk, preferred_element_type=F32)
            g = jnp.einsum("td,fd->tf", ds, wdk, preferred_element_type=F32)
            s = jax.nn.sigmoid(a)
            act = a * s
            h = (act * b).astype(BF16)
            da = (g * b * s * (1.0 + a * (1.0 - s))).astype(BF16)
            db = (g * act).astype(BF16)
            hs.append(h)
            part = jnp.einsum("tf,df->td", da, wgk, preferred_element_type=F32) + jnp.einsum("tf,df->td", db, wuk, preferred_element_type=F32)
            dx_part = part if dx_part is None else dx_part + part
            dgs.append(jnp.einsum("td,tf->df", xs, da, preferred_element_type=F32))
            dus.append(jnp.einsum("td,tf->df", xs, db, preferred_element_type=F32))
        h_all = jnp.concatenate(hs, axis=1)
        y_part = jnp.dot(h_all, wd_all.reshape(2 * wc, width), preferred_element_type=F32)
        d_part = jnp.einsum("tf,td->fd", h_all, ds, preferred_element_type=F32).reshape(2, wc, width)
        g_part = jnp.stack(dgs).reshape(2, 4, 2, wr, wc)
        u_part = jnp.stack(dus).reshape(2, 4, 2, wr, wc)
        y_part = y_part.reshape(4, 2, micro, rows, width)
        dx_part = dx_part.reshape(4, 2, micro, rows, width)

        tok = (micro, rows, width)
        up = (wr, wc)
        dn = (wc, wr)
        lands = [
            S((2, 2, rows, width), F32), S((2, 2) + tok, F32), S(tok, F32),
            S((4,) + tok, F32), S((2, rows, width), F32), S((2,) + tok, F32),
        ]
        for _ in range(2):
            lands += [S((4, 2) + up, F32), S((2, 2, wr // 2, wc), F32), S((2, 2) + up, F32), S(up, F32)]
        lands += [S((4, 2) + dn, F32), S((4,) + dn, F32), S((2, wc // 2, wr), F32), S((2,) + dn, F32)]
        outs = [S(tok, BF16), S(tok, BF16), S(up, F32), S(up, F32), S(dn, F32)]
        res = pl.pallas_call(
            reduce_kernel,
            name="reduce",
            out_shape=tuple(outs + lands),
            in_specs=[vmem] * 2 + [hbm] * 5,
            out_specs=[vmem] * 5 + [hbm] * len(lands),
            scratch_shapes=[
                pltpu.VMEM((3, 2) + tok, F32), pltpu.VMEM((4,) + tok, F32),
                pltpu.VMEM((4, 2) + up, F32), pltpu.VMEM((4, 2) + up, F32), pltpu.VMEM((4, 2) + dn, F32),
                pltpu.VMEM((2,) + tok, F32), pltpu.VMEM((2,) + up, F32), pltpu.VMEM((2,) + dn, F32),
                dma((2,)), dma((48,)), dma((48,)),
            ],
            compiler_params=pltpu.CompilerParams(collective_id=1, has_side_effects=True, vmem_limit_bytes=60 * 2**20),
        )(x_loc, dy_loc, y_part, dx_part, g_part, u_part, d_part)
        return res[0], res[1], res[2], res[3], res[4]

    return jax.shard_map(local_step, mesh=mesh, in_specs=in_specs, out_specs=out_specs, check_vma=False)
```

```python
import functools
import heapq

import jax
import jax.numpy as jnp
from jax import lax
from jax.experimental import pallas as pl
from jax.experimental.pallas import tpu as pltpu
from jax.sharding import PartitionSpec as P

MESH = pl.DeviceIdType.MESH
F32 = jnp.float32
BF16 = jnp.bfloat16
ICI_RATE = 44.0e3
CORE_RATE = 550.0e3
HBM_RATE = 2.5e6
MARGIN = 1.0
STEPS = (
    "Hoa", "H-a", "H-b", "R-", "H+a", "H+b", "R+", "Q-",
    "H2a", "H2b", "Hob", "W0a", "W0b", "Q+", "R2", "Q2",
    "W1a", "W1b", "Ro", "Qo", "W2a", "W2b", "W3a", "W3b",
)


def nbytes(ref):
    size = jnp.dtype(ref.dtype).itemsize
    for n in ref.shape:
        size *= n
    return size


class Place:
    def __init__(self):
        t = lax.axis_index("tp")
        d = lax.axis_index("dp")
        z, y, x, c = t // 4, t % 4, d // 2, d % 2
        self.z, self.y, self.x, self.c = z, y, x, c
        self.b = y % 2
        self.a = y // 2
        self.zp, self.zm, self.z2 = (z + 1) % 4, (z + 3) % 4, (z + 2) % 4
        self.xp, self.xm, self.x2 = (x + 1) % 4, (x + 3) % 4, (x + 2) % 4

        def at(z, y, x, c):
            return {"tp": z * 4 + y, "dp": x * 2 + c}

        self.dev = {
            "z+": at(self.zp, y, x, c),
            "z-": at(self.zm, y, x, c),
            "x+": at(z, y, self.xp, c),
            "x-": at(z, y, self.xm, c),
            "tok": at(z, y + 1 - 2 * self.b, x, c),
            "wgt": at(z, 3 - y, x, c),
            "core": at(z, y, x, 1 - c),
        }

    def barrier(self):
        sem = pltpu.get_barrier_semaphore()
        for dev in self.dev.values():
            pl.semaphore_signal(sem, inc=1, device_id=dev, device_id_type=MESH)
        pl.semaphore_wait(sem, len(self.dev))


class Handle:
    def __init__(self, time, wait, after=None):
        self.time, self._wait, self.after, self.done = time, wait, after, False

    def wait(self):
        if not self.done:
            self.done = True
            self._wait()
            if self.after is not None:
                self.after()


class Flag:
    def __init__(self, count=1):
        self.left = count

    def hit(self):
        self.left -= 1


class Pool:
    def __init__(self, refs):
        self.refs = refs
        self.back = [[] for _ in refs]
        self.free = [True] * len(refs)

    def when_ready(self, count):
        times = sorted(max((h.time for h in self.back[i]), default=0.0) for i in range(len(self.refs)) if self.free[i])
        return times[count - 1] if len(times) >= count else float("inf")

    def take(self, count):
        order = sorted(
            (max((h.time for h in self.back[i]), default=0.0), i) for i in range(len(self.refs)) if self.free[i]
        )
        got = [i for _, i in order[:count]]
        for i in got:
            for h in self.back[i]:
                h.wait()
            self.back[i] = []
            self.free[i] = False
        return got

    def give(self, i, handles=()):
        self.free[i] = True
        self.back[i] = list(handles)


class Net:
    def __init__(self, place, local_sems, send_sems, recv_sems):
        self.place, self.local_sems, self.send_sems, self.recv_sems = place, local_sems, send_sems, recv_sems
        self.used = 0
        self.local_used = 0
        self.local_free = []
        self.open = []
        self.heap = []
        self.jobs = []
        self.seq = 0
        self.now = 0.0
        self.free = {}
        self.log = []

    def send(self, link, src, dst, land=None):
        land = dst if land is None else land
        i = self.used
        self.used += 1
        dev = self.place.dev[link]

        def copy_of(a, b):
            return pltpu.make_async_remote_copy(
                src_ref=a, dst_ref=b, send_sem=self.send_sems.at[i], recv_sem=self.recv_sems.at[i],
                device_id=dev, device_id_type=MESH,
            )

        copy = copy_of(src, dst)
        copy.start()
        arrive = copy_of(land, land)
        rate = CORE_RATE if link == "core" else ICI_RATE
        end = max(self.now, self.free.get(link, 0.0)) + nbytes(land) / rate
        self.free[link] = end
        sent = Handle(end + 0.5, copy.wait_send)
        self.open.append(sent)
        return Handle(end + 2.0, arrive.wait_recv), sent

    def copy(self, src, dst):
        if self.local_free:
            i = self.local_free.pop(0)
        else:
            i = self.local_used
            self.local_used += 1
        copy = pltpu.make_async_copy(src, dst, self.local_sems.at[i])
        copy.start()
        end = max(self.now, self.free.get("hbm", 0.0)) + nbytes(src) / HBM_RATE
        self.free["hbm"] = end
        handle = Handle(end + 0.8, copy.wait, lambda: self.local_free.append(i))
        self.open.append(handle)
        return handle

    def when(self, handles, then):
        self.seq += 1
        heapq.heappush(self.heap, (max(h.time for h in handles), self.seq, handles, then))

    def job(self, flags, needs, then, cost, rank, line=None):
        self.seq += 1
        self.jobs.append((rank, self.seq, flags, needs, then, cost, line))
        self.jobs.sort(key=lambda j: j[:2])

    def run(self):
        while True:
            if self.heap and self.heap[0][0] + MARGIN <= self.now:
                self.event()
                continue
            chosen = None
            soonest = float("inf")
            held = set()
            for j in self.jobs:
                if j[6] is not None:
                    if j[6] in held:
                        continue
                    held.add(j[6])
                if any(f.left > 0 for f in j[2]):
                    continue
                ready = max((pool.when_ready(n) for pool, n in j[3]), default=0.0)
                if ready <= self.now:
                    chosen = j
                    break
                soonest = min(soonest, ready)
            if chosen is not None:
                self.jobs.remove(chosen)
                _, _, _, needs, then, cost, _ = chosen
                slots = [pool.take(n) for pool, n in needs]
                self.now += cost
                then(*slots)
                continue
            if self.heap and self.heap[0][0] <= soonest:
                self.event()
            elif soonest < float("inf"):
                self.now = max(self.now, soonest)
            else:
                break
        assert not self.jobs, "jobs left"
        for handle in self.open:
            handle.wait()

    def event(self):
        time, _, handles, then = heapq.heappop(self.heap)
        self.now = max(self.now, time)
        for h in handles:
            h.wait()
        then()

    def arrive(self, handle, flag):
        self.when([handle], flag.hit)


def nothing():
    pass


def gather_ring_first(net, own, slot, half, ring, pair, me, each):
    r, rp, rm, r2, p = me
    up, down = ring
    from_down, _ = net.send(up, own, slot(r, p), slot(rm, p))
    from_up, _ = net.send(down, own, slot(r, p), slot(rp, p))
    other, _ = net.send(pair, own, slot(r, p), slot(r, 1 - p))
    net.when([other], lambda: each("o", 1, r, 1 - p))

    def pass_on(name, q):
        got, _ = net.send(pair, slot(q, p), slot(q, p), slot(q, 1 - p))
        net.when([got], lambda: each(name, 1, q, 1 - p))

    far = []

    def got_near(name, q, h, link):
        def then():
            ref = half(slot(q, p), h)
            far.append(net.send(link, ref, ref, half(slot(r2, p), h))[0])
            pass_on(name, q)
            each(name, 0, q, p)
            if len(far) == 2:
                net.when(far, got_far)
        return then

    def got_far():
        pass_on("2", r2)
        each("2", 0, r2, p)

    net.when([from_down], got_near("-", rm, 0, up))
    net.when([from_up], got_near("+", rp, 1, down))


def gather_pair_first(net, own, slot, half, ring, pair, me, each, late=False):
    r, rp, rm, r2, p = me
    up, down = ring

    def around(src, q, k):
        from_down, _ = net.send(up, src, slot(r, q), slot(rm, q))
        from_up, _ = net.send(down, src, slot(r, q), slot(rp, q))
        far = []

        def got_near(name, s, h, link):
            def then():
                ref = half(slot(s, q), h)
                far.append(net.send(link, ref, ref, half(slot(r2, q), h))[0])
                each(name, k, s, q)
                if k == 0 and late:
                    go_other()
                if len(far) == 2:
                    net.when(far, lambda: each("2", k, r2, q))
            return then

        net.when([from_down], got_near("-", rm, 0, up))
        net.when([from_up], got_near("+", rp, 1, down))

    other, _ = net.send(pair, own, slot(r, p), slot(r, 1 - p))
    before = Flag(3 if late else 1)

    def go_other():
        before.hit()
        if before.left == 0:
            around(slot(r, 1 - p), 1 - p, 1)

    def got_other():
        each("o", 1, r, 1 - p)
        go_other()

    net.when([other], got_other)
    around(own, p, 0)


def sum_rows(dst, srcs):
    if len(dst.shape) > 2:
        for i in range(dst.shape[0]):
            sum_rows(dst.at[i], [s.at[i] for s in srcs])
        return
    step = 16

    @pl.loop(0, dst.shape[0] // step)
    def _(i):
        at = pl.ds(pl.multiple_of(i * step, step), step)
        total = dst[at, :]
        for s in srcs:
            total = total + s[at, :]
        dst[at, :] = total


def dot(a, b, ca, cb):
    return lax.dot_general(a, b, (((ca,), (cb,)), ((), ())), preferred_element_type=F32)


def layer_kernel(
    x_ref, dy_ref, wg_ref, wu_ref, wd_ref,
    r_own, r_lp, q_own, q_l2, gu_own, gu_lp, d_own, d_l2,
    x_all, dy_all, r_pt, q_pt, w_pt, r_l1, r_l2, q_lp, q_l1, w_lc, gu_l1, gu_l2, d_lp, d_l1,
    wg_all, wu_all, wd_all, h_all, da_all, db_all, xb, db, xs, ds, r_out, q_out, tw, tk, wk,
    local_sems, send_sems, recv_sems,
):
    here = Place()
    here.barrier()
    net = Net(here, local_sems, send_sems, recv_sems)
    z, zp, zm, z2, b = here.z, here.zp, here.zm, here.z2, here.b
    x, xp, xm, x2, a, c = here.x, here.xp, here.xm, here.x2, here.a, here.c
    micro, rows, width = x_ref.shape
    wr, wc = wg_ref.shape
    edge = width // 8
    n_blk = 2 * micro * rows
    zs = {"o": z, "+": zp, "-": zm, "2": z2}
    xs_of = {"o": x, "+": xp, "-": xm, "2": x2}

    def rows_at(start, size):
        return pl.ds(pl.multiple_of(start, size), size)

    weights_in = [Flag(24), Flag(24)]
    tokens_in = {k: Flag(0) for k in zs}

    def up_slot(ref, core):
        return lambda q, p: ref.at[rows_at((q * 2 + core) * wr, wr), rows_at(p * wc, wc)]

    def down_slot(core):
        return lambda q, p: wd_all.at[rows_at(p * wc, wc), rows_at((q * 2 + core) * wr, wr)]

    def up_half(ref, h):
        return ref.at[pl.ds(h * (wr // 2), wr // 2)]

    def down_half(ref, h):
        return ref.at[pl.ds(h * (wc // 2), wc // 2)]

    def tok_half(ref, h):
        return ref.at[h]

    in_z = (z, zp, zm, z2, b)
    in_x = (x, xp, xm, x2, a)

    def across(mine, theirs):
        def each(name, k, q, p):
            weights_in[k].hit()
            got, _ = net.send("core", mine(q, p), mine(q, p), theirs(q, p))
            net.arrive(got, weights_in[k])
        return each

    def count_tokens(name, k, q, p):
        tokens_in[name].hit()

    for fn, own, mine, theirs, half in (
        (gather_ring_first, wg_ref, up_slot(wg_all, c), up_slot(wg_all, 1 - c), up_half),
        (functools.partial(gather_pair_first, late=True), wu_ref, up_slot(wu_all, c), up_slot(wu_all, 1 - c), up_half),
        (functools.partial(gather_pair_first, late=True), wd_ref, down_slot(c), down_slot(1 - c), down_half),
    ):
        fn(net, own, mine, half, ("x+", "x-"), "wgt", in_x, across(mine, theirs))
        got, _ = net.send("core", own, mine(x, a), theirs(x, a))
        net.arrive(got, weights_in[0])
        net.arrive(net.copy(own, mine(x, a)), weights_in[0])
    for name, f in tokens_in.items():
        f.left += 5 if name == "o" else 6
    for fn, own, dst, cols in (
        (gather_pair_first, x_ref, x_all, pl.ds(width - edge, edge)),
        (gather_ring_first, x_ref, x_all, pl.ds(0, width - edge)),
        (gather_pair_first, dy_ref, dy_all, pl.ds(0, width)),
    ):
        slot = functools.partial(lambda q, p, dst, cols: dst.at[q, p, :, :, cols], dst=dst, cols=cols)
        fn(net, own.at[:, :, cols], slot, tok_half, ("z+", "z-"), "tok", in_z, count_tokens)
    net.arrive(net.copy(x_ref, x_all.at[z, b]), tokens_in["o"])
    net.arrive(net.copy(dy_ref, dy_all.at[z, b]), tokens_in["o"])

    tok_pool = Pool([(xb.at[i], db.at[i]) for i in range(xb.shape[0])])
    cut_pool = Pool([(xs.at[i], ds.at[i]) for i in range(xs.shape[0])])
    r_pool = Pool([r_out.at[i] for i in range(r_out.shape[0])])
    q_pool = Pool([q_out.at[i] for i in range(q_out.shape[0])])
    wout_pool = Pool([tw.at[i] for i in range(tw.shape[0])])
    tk_pool = Pool([tk.at[i] for i in range(tk.shape[0])])
    wk_pool = Pool([wk.at[i] for i in range(wk.shape[0])])

    hidden = {k: Flag(2) for k in zs}
    tile_h = min(256, wc)

    def hidden_of(name, turn, rank):
        cols_at = a * wc if turn == 0 else (1 - a) * wc
        loaded = Flag()
        held = []

        def load(slots):
            i = slots[0]
            held.append(i)
            one, two = tok_pool.refs[i]
            first = net.copy(x_all.at[zs[name]], one)
            second = net.copy(dy_all.at[zs[name]], two)
            net.when([first, second], loaded.hit)

        def multiply():
            i = held[0]
            one, two = tok_pool.refs[i]
            at = rows_at(zs[name] * n_blk, n_blk)

            @pl.loop(0, wc // tile_h)
            def _(j):
                cols = rows_at(cols_at + j * tile_h, tile_h)
                x_blk = one[...].reshape(n_blk, width)
                dy_blk = two[...].reshape(n_blk, width)
                pre = dot(x_blk, wg_all[:, cols], 1, 0)
                up = dot(x_blk, wu_all[:, cols], 1, 0)
                g = dot(dy_blk, wd_all[cols, :], 1, 1)
                s = jax.nn.sigmoid(pre)
                act = pre * s
                h_all[at, cols] = (act * up).astype(BF16)
                da_all[at, cols] = (g * up * s * (1.0 + pre * (1.0 - s))).astype(BF16)
                db_all[at, cols] = (g * act).astype(BF16)

            tok_pool.give(i)
            hidden[name].hit()

        net.job([tokens_in[name]], [(tok_pool, 1)], load, 0.1, rank * 0.01, "load")
        net.job([loaded, weights_in[turn]], [], multiply, 2.8, rank, "mxu")

    r_in = {k: Flag() for k in zs}
    q_in = {k: Flag() for k in zs}
    tile_y = width // 2
    tile_dx = 2 * edge

    def rows_of(name, rank_r, rank_q):
        at = rows_at(zs[name] * n_blk, n_blk)
        s = zs[name]
        half_way = Flag()
        held = []

        def put(ref, cols, val):
            ref[:, :, :, cols] = val.reshape(2, micro, rows, val.shape[-1])

        def dx_tile(cols):
            return dot(da_all[at, :], wg_all[cols, :], 1, 1) + dot(db_all[at, :], wu_all[cols, :], 1, 1)

        def first(slots_r, slots_q):
            i = slots_r[0]
            ref = r_pool.refs[i]
            held.append(slots_q[0])

            @pl.loop(0, width // tile_y)
            def _(j):
                cols = rows_at(j * tile_y, tile_y)
                put(ref, cols, dot(h_all[at, :], wd_all[:, cols], 1, 0))

            val = dx_tile(pl.ds(0, tile_dx))
            put(ref, pl.ds(width, edge), val[:, :edge])
            put(q_pool.refs[held[0]], pl.ds(0, edge), val[:, edge:])
            done = net.copy(ref, r_pt.at[s])
            r_pool.give(i, [done])
            net.when([done], r_in[name].hit)
            half_way.hit()

        def second():
            i = held[0]
            ref = q_pool.refs[i]

            @pl.loop(1, width // tile_dx)
            def _(j):
                cols = rows_at(j * tile_dx, tile_dx)
                put(ref, pl.ds(pl.multiple_of(j * tile_dx - edge, edge), tile_dx), dx_tile(cols))

            done = net.copy(ref, q_pt.at[s])
            q_pool.give(i, [done])
            net.when([done], q_in[name].hit)

        net.job([hidden[name]], [(r_pool, 1), (q_pool, 1)], first, 3.0, rank_r, "mxu")
        net.job([half_way], [], second, 3.0, rank_q, "mxu")

    ranks = {step: 10 + i for i, step in enumerate(STEPS)}
    for name in zs:
        hidden_of(name, 0, ranks["H" + name + "a"])
        hidden_of(name, 1, ranks["H" + name + "b"])
        rows_of(name, ranks["R" + name], ranks["Q" + name])
    order = ("2", "+", "-", "o")

    def add_up(flags, pool, srcs, view, then, rank=1):
        def begin(slots):
            refs = [view(pool.refs[i]) for i in slots]
            loads = [net.copy(src, ref) for src, ref in zip(srcs, refs)]

            def add():
                sum_rows(refs[0], refs[1:])
                net.now += 0.25 * len(refs) * nbytes(refs[0]) / 1.0e6
                for i in slots[1:]:
                    pool.give(i)
                then(refs[0], slots[0])

            net.when(loads, add)

        net.job(flags, [(pool, len(srcs))], begin, 0.1, rank)

    def put_back(pool, ref, i, pairs, then):
        copies = [net.copy(src, dst) for src, dst in pairs]
        pool.give(i, copies)
        net.when(copies, then)

    y_from = {k: Flag() for k in ("z+", "z-")}
    y_near = [Flag(2), Flag(2)]

    def send_y2():
        for k, link in enumerate(("z+", "z-")):
            got, _ = net.send(link, r_pt.at[z2, :, k], r_l1.at[k])
            net.arrive(got, y_from[link])

    net.job([r_in["2"]], [], send_y2, 0.1, 1)

    def y_next(k, link, name):
        s = zs[name]

        def send_half(h):
            got, _ = net.send(link, r_pt.at[s, :, h], r_l2.at[k, h])
            net.arrive(got, y_near[h])

        net.job([r_in[name]], [], lambda: send_half(1 - k), 0.1, 1)

        def summed(ref, i):
            put_back(tk_pool, ref, i, [(ref, r_pt.at[s, :, k])], lambda: send_half(k))

        add_up([r_in[name], y_from[link]], tk_pool, [r_pt.at[s, :, k], r_l1.at[k]], lambda r: r, summed)

    y_next(0, "z+", "+")
    y_next(1, "z-", "-")

    def y_last(h):
        def summed(ref, i):
            def go():
                got, _ = net.send("tok", r_pt.at[z, 1 - b, h], r_lp.at[h])
                net.when([got], nothing)
            put_back(tk_pool, ref, i, [(ref.at[1 - b], r_pt.at[z, 1 - b, h]), (ref.at[b], r_own.at[h])], go)

        add_up([r_in["o"], y_near[h]], tk_pool, [r_pt.at[z, :, h], r_l2.at[0, h], r_l2.at[1, h]], lambda r: r, summed)

    y_last(0)
    y_last(1)

    def q_view(ref):
        return ref.at[:, :, pl.ds(0, width - edge)]

    dx_pair = {k: Flag() for k in zs}
    dx_from = {k: Flag() for k in ("z+", "z-")}

    def pair_dx(k, name):
        def go():
            got, _ = net.send("tok", q_pt.at[zs[name], 1 - b], q_lp.at[k])
            net.arrive(got, dx_pair[name])
        net.job([q_in[name]], [], go, 0.1, 1)

    for k, name in enumerate(order):
        pair_dx(k, name)

    def dx_far(ref, i):
        def go():
            for k, link in enumerate(("z+", "z-")):
                got, _ = net.send(link, q_pt.at[z2, b, k], q_l1.at[k])
                net.arrive(got, dx_from[link])
        put_back(tk_pool, ref, i, [(ref, q_pt.at[z2, b])], go)

    add_up([q_in["2"], dx_pair["2"]], tk_pool, [q_pt.at[z2, b], q_lp.at[0]], q_view, dx_far)

    def dx_next(k, link, name):
        s = zs[name]

        def half(h, flags, more):
            def summed(ref, i):
                def go():
                    got, _ = net.send(link, q_pt.at[s, b, h], q_l2.at[k, h])
                    net.when([got], nothing)
                put_back(tk_pool, ref, i, [(ref, q_pt.at[s, b, h])], go)
            srcs = [q_pt.at[s, b, h], q_lp.at[1 + k, h]] + more
            add_up([q_in[name], dx_pair[name]] + flags, tk_pool, srcs, lambda r: q_view(r).at[0], summed)

        half(1 - k, [], [])
        half(k, [dx_from[link]], [q_l1.at[k]])

    dx_next(0, "z+", "+")
    dx_next(1, "z-", "-")

    def dx_last(ref, i):
        put_back(tk_pool, ref, i, [(ref, q_own)], nothing)

    add_up([q_in["o"], dx_pair["o"]], tk_pool, [q_pt.at[z, b], q_lp.at[3]], q_view, dx_last)

    tile_w = wc
    n_tok = 4 * n_blk
    w_in = {(m, k): Flag() for m in range(3) for k in range(4)}
    w_side = {(m, k): Flag() for m in range(3) for k in range(4)}
    all_hidden = list(hidden.values())

    def grads_of(k, name, core, turn):
        loaded = Flag()
        held = []
        cols = rows_at((xs_of[name] * 2 + core) * wr, wr)

        def load(slots):
            i = slots[0]
            held.append(i)
            one, two = cut_pool.refs[i]
            first = net.copy(x_all.at[:, :, :, :, cols], one)
            second = net.copy(dy_all.at[:, :, :, :, cols], two)
            net.when([first, second], loaded.hit)

        def multiply(slots):
            i = held[0]
            one, two = cut_pool.refs[i]
            outs = [wout_pool.refs[j] for j in slots]

            @pl.loop(0, 2 * wc // tile_w)
            def _(j):
                at = rows_at(j * tile_w, tile_w)
                x_cut = one[...].reshape(n_tok, wr)
                dy_cut = two[...].reshape(n_tok, wr)
                outs[0][:, at] = dot(x_cut, da_all[:, at], 0, 0)
                outs[1][:, at] = dot(x_cut, db_all[:, at], 0, 0)
                outs[2][:, at] = dot(dy_cut, h_all[:, at], 0, 0)

            cut_pool.give(i)
            for m, (j, ref) in enumerate(zip(slots, outs)):
                if turn == 0:
                    got, sent = net.send("core", ref, w_lc.at[m, k])
                    wout_pool.give(j, [sent])
                    net.arrive(got, w_side[m, k])
                else:
                    done = net.copy(ref, w_pt.at[m, k])
                    wout_pool.give(j, [done])
                    net.when([done], w_in[m, k].hit)

        rank = ranks["W%d%s" % (k, "ab"[turn])]
        net.job(list(tokens_in.values()), [(cut_pool, 1)], load, 0.1, 2 + 0.01 * rank, "cut")
        net.job([loaded] + all_hidden, [(wout_pool, 3)], multiply, 2.9, rank, "mxu")

    for k, name in enumerate(order):
        grads_of(k, name, 1 - c, 0)
        grads_of(k, name, c, 1)

    hr = wr // 2

    def part(ref, h):
        return ref.at[pl.ds(h * hr, hr)]

    def w_ring_first(m):
        have = {k: [w_in[m, k], w_side[m, k]] for k in range(4)}
        come = [Flag(), Flag()]
        near = [Flag(2), Flag(2)]

        def far(h, link):
            def summed(ref, i):
                def go():
                    got, _ = net.send(link, part(w_pt.at[m, 0], h), gu_l1.at[m, h])
                    net.arrive(got, come[h])
                put_back(wk_pool, ref, i, [(ref, part(w_pt.at[m, 0], h))], go)
            add_up(have[0], wk_pool, [part(w_pt.at[m, 0], h), part(w_lc.at[m, 0], h)], lambda r: r, summed)

        far(0, "x+")
        far(1, "x-")

        def on(k, link):
            def half(h, flags, more):
                def summed(ref, i):
                    def go():
                        got, _ = net.send(link, part(w_pt.at[m, 1 + k], h), gu_l2.at[m, k, h])
                        net.arrive(got, near[h])
                    put_back(wk_pool, ref, i, [(ref, part(w_pt.at[m, 1 + k], h))], go)
                srcs = [part(w_pt.at[m, 1 + k], h), part(w_lc.at[m, 1 + k], h)] + more
                add_up(have[1 + k] + flags, wk_pool, srcs, lambda r: r, summed)
            half(1 - k, [], [])
            half(k, [come[k]], [gu_l1.at[m, k]])

        on(0, "x+")
        on(1, "x-")

        def last(h):
            def summed(ref, i):
                mine = ref.at[:, rows_at(a * wc, wc)]
                other = ref.at[:, rows_at((1 - a) * wc, wc)]
                away = part(w_pt.at[m, 3], h).at[:, rows_at((1 - a) * wc, wc)]

                def go():
                    got, _ = net.send("wgt", away, part(gu_lp.at[m], h))
                    net.when([got], nothing)
                put_back(wk_pool, ref, i, [(other, away), (mine, part(gu_own.at[m], h))], go)
            srcs = [part(w_pt.at[m, 3], h), part(w_lc.at[m, 3], h), gu_l2.at[m, 0, h], gu_l2.at[m, 1, h]]
            add_up(have[3] + [near[h]], wk_pool, srcs, lambda r: r, summed)

        last(0)
        last(1)

    def w_pair_first(m):
        mine = rows_at(a * wc, wc)
        other = rows_at((1 - a) * wc, wc)
        have = {k: [w_in[m, k], w_side[m, k]] for k in range(4)}
        pair = {(k, h): Flag() for k in range(4) for h in range(2)}
        come = [Flag(), Flag()]

        def view(r):
            return r.at[:, pl.ds(0, wc)]

        def away(k, h):
            dst = part(w_pt.at[m, k], h).at[:, other]

            def summed(ref, i):
                def go():
                    got, _ = net.send("wgt", dst, part(d_lp.at[k], h))
                    net.arrive(got, pair[k, h])
                put_back(wk_pool, ref, i, [(ref, dst)], go)
            add_up(have[k], wk_pool, [dst, part(w_lc.at[m, k], h).at[:, other]], view, summed)

        def stay(k, h, flags, more, dst, then):
            srcs = [part(w_pt.at[m, k], h).at[:, mine], part(w_lc.at[m, k], h).at[:, mine], part(d_lp.at[k], h)] + more

            def summed(ref, i):
                put_back(wk_pool, ref, i, [(ref, dst)], then)
            add_up(have[k] + [pair[k, h]] + flags, wk_pool, srcs, view, summed)

        for k in range(4):
            for h in range(2):
                away(k, h)

        def far(h, link):
            dst = part(w_pt.at[m, 0], h).at[:, mine]

            def go():
                got, _ = net.send(link, dst, d_l1.at[h])
                net.arrive(got, come[h])
            stay(0, h, [], [], dst, go)

        far(0, "x+")
        far(1, "x-")

        def on(k, link, h):
            dst = part(w_pt.at[m, 1 + k], h).at[:, mine]

            def go():
                got, _ = net.send(link, dst, d_l2.at[k, h])
                net.when([got], nothing)
            same = h == k
            stay(1 + k, h, [come[k]] if same else [], [d_l1.at[k]] if same else [], dst, go)

        for k, link in enumerate(("x+", "x-")):
            on(k, link, 1 - k)
            on(k, link, k)
        for h in range(2):
            stay(3, h, [], [], part(d_own, h), nothing)

    w_ring_first(0)
    w_ring_first(1)
    w_pair_first(2)
    net.run()


def solution(mesh):
    row_spec = P(None, ("dp", "tp"), None)
    in_specs = (row_spec, P("dp", "tp"), P("dp", "tp"), P("tp", "dp"), row_spec)
    out_specs = (row_spec, row_spec, P("dp", "tp"), P("dp", "tp"), P("tp", "dp"))
    vmem = pl.BlockSpec(memory_space=pltpu.VMEM)
    hbm = pl.BlockSpec(memory_space=pl.ANY)
    dma = pltpu.SemaphoreType.DMA
    V = pltpu.VMEM
    S = jax.ShapeDtypeStruct

    def local_step(x_loc, wg, wu, wd, dy_loc):
        micro, rows, width = x_loc.shape
        wr, wc = wg.shape
        edge = width // 8
        tok = (micro, rows, width)
        tok_r = (micro, rows, width + edge)
        tok_q = (micro, rows, width - edge)
        n = 8 * micro * rows
        outs = [
            S(tok_r, F32), S(tok_r, F32), S(tok_q, F32), S((2,) + tok_q, F32),
            S((2, wr, wc), F32), S((2, wr, wc), F32), S((wr, wc), F32), S((2, 2, wr // 2, wc), F32),
        ]
        space = [
            S((4, 2) + tok, BF16), S((4, 2) + tok, BF16), S((4, 2) + tok_r, F32), S((4, 2) + tok_q, F32),
            S((3, 4, wr, 2 * wc), F32),
            S((2, 2) + tok_r[1:], F32), S((2, 2, 2) + tok_r[1:], F32),
            S((4,) + tok_q, F32), S((2,) + tok_q[1:], F32),
            S((3, 4, wr, 2 * wc), F32),
            S((2, 2, wr // 2, 2 * wc), F32), S((2, 2, 2, wr // 2, 2 * wc), F32),
            S((4, wr, wc), F32), S((2, wr // 2, wc), F32),
        ]
        res = pl.pallas_call(
            layer_kernel,
            name="layer",
            out_shape=tuple(outs + space),
            in_specs=[vmem] * 2 + [hbm] * 3,
            out_specs=[hbm] * (len(outs) + len(space)),
            scratch_shapes=[
                V((width, 2 * wc), BF16), V((width, 2 * wc), BF16), V((2 * wc, width), BF16),
                V((n, 2 * wc), BF16), V((n, 2 * wc), BF16), V((n, 2 * wc), BF16),
                V((2, 2) + tok, BF16), V((2, 2) + tok, BF16),
                V((2, 4, 2, micro, rows, wr), BF16), V((2, 4, 2, micro, rows, wr), BF16),
                V((1, 2) + tok_r, F32), V((2, 2) + tok_q, F32), V((6, wr, 2 * wc), F32),
                V((3, 2) + tok_r[1:], F32), V((6, wr // 2, 2 * wc), F32),
                dma((96,)), dma((144,)), dma((144,)),
            ],
            compiler_params=pltpu.CompilerParams(
                collective_id=0, has_side_effects=True, vmem_limit_bytes=67_000_000
            ),
        )(x_loc, dy_loc, wg, wu, wd)
        r_own, r_lp, q_own, q_l2, gu_own, gu_lp, d_own, d_l2 = res[: len(outs)]
        r = r_own + r_lp
        q = q_own + q_l2[0] + q_l2[1]
        y = (x_loc.astype(F32) + r[:, :, :width]).astype(BF16)
        dx = (dy_loc.astype(F32) + jnp.concatenate([r[:, :, width:], q], axis=2)).astype(BF16)
        d_sum = d_own + d_l2[0].reshape(wr, wc) + d_l2[1].reshape(wr, wc)
        return y, dx, gu_own[0] + gu_lp[0], gu_own[1] + gu_lp[1], d_sum.T

    return jax.shard_map(local_step, mesh=mesh, in_specs=in_specs, out_specs=out_specs, check_vma=False)
```

```python
import functools
import heapq

import jax
import jax.numpy as jnp
from jax import lax
from jax.experimental import pallas as pl
from jax.experimental.pallas import tpu as pltpu
from jax.sharding import PartitionSpec as P

MESH = pl.DeviceIdType.MESH
F32 = jnp.float32
BF16 = jnp.bfloat16
ICI_RATE = 45.0e3
CORE_RATE = 550.0e3
HBM_RATE = 2.5e6
MARGIN = 1.0
STEPS = (
    "Hoa", "H-a", "Hob", "H-b", "H+b", "R-", "H+a", "H2b", "H2a", "R2",
    "W0a", "W0b", "Q2", "Y0", "Y2", "R+", "W2a", "W2b", "W1a", "W3a",
    "W1b", "Ro", "Q-", "Y1", "Y3", "Q+", "Qo", "W3b",
)


def nbytes(ref):
    size = jnp.dtype(ref.dtype).itemsize
    for n in ref.shape:
        size *= n
    return size


class Place:
    def __init__(self):
        t = lax.axis_index("tp")
        d = lax.axis_index("dp")
        z, y, x, c = t // 4, t % 4, d // 2, d % 2
        self.z, self.y, self.x, self.c = z, y, x, c
        self.b = y % 2
        self.a = y // 2
        self.zp, self.zm, self.z2 = (z + 1) % 4, (z + 3) % 4, (z + 2) % 4
        self.xp, self.xm, self.x2 = (x + 1) % 4, (x + 3) % 4, (x + 2) % 4

        def at(z, y, x, c):
            return {"tp": z * 4 + y, "dp": x * 2 + c}

        self.dev = {
            "z+": at(self.zp, y, x, c),
            "z-": at(self.zm, y, x, c),
            "x+": at(z, y, self.xp, c),
            "x-": at(z, y, self.xm, c),
            "tok": at(z, y + 1 - 2 * self.b, x, c),
            "wgt": at(z, 3 - y, x, c),
            "core": at(z, y, x, 1 - c),
        }

    def barrier(self):
        sem = pltpu.get_barrier_semaphore()
        for dev in self.dev.values():
            pl.semaphore_signal(sem, inc=1, device_id=dev, device_id_type=MESH)
        pl.semaphore_wait(sem, len(self.dev))


class Handle:
    def __init__(self, time, wait, after=None):
        self.time, self._wait, self.after, self.done = time, wait, after, False

    def wait(self):
        if not self.done:
            self.done = True
            self._wait()
            if self.after is not None:
                self.after()


class Flag:
    def __init__(self, count=1):
        self.left = count

    def hit(self):
        self.left -= 1


class Pool:
    def __init__(self, refs):
        self.refs = refs
        self.back = [[] for _ in refs]
        self.free = [True] * len(refs)

    def when_ready(self, count):
        times = sorted(max((h.time for h in self.back[i]), default=0.0) for i in range(len(self.refs)) if self.free[i])
        return times[count - 1] if len(times) >= count else float("inf")

    def take(self, count):
        order = sorted(
            (max((h.time for h in self.back[i]), default=0.0), i) for i in range(len(self.refs)) if self.free[i]
        )
        got = [i for _, i in order[:count]]
        for i in got:
            for h in self.back[i]:
                h.wait()
            self.back[i] = []
            self.free[i] = False
        return got

    def give(self, i, handles=()):
        self.free[i] = True
        self.back[i] = list(handles)


class Net:
    def __init__(self, place, local_sems, send_sems, recv_sems):
        self.place, self.local_sems, self.send_sems, self.recv_sems = place, local_sems, send_sems, recv_sems
        self.used = 0
        self.local_used = 0
        self.local_free = []
        self.open = []
        self.heap = []
        self.jobs = []
        self.seq = 0
        self.now = 0.0
        self.free = {}
        self.log = []

    def send(self, link, src, dst, land=None):
        land = dst if land is None else land
        i = self.used
        self.used += 1
        dev = self.place.dev[link]

        def copy_of(a, b):
            return pltpu.make_async_remote_copy(
                src_ref=a, dst_ref=b, send_sem=self.send_sems.at[i], recv_sem=self.recv_sems.at[i],
                device_id=dev, device_id_type=MESH,
            )

        copy = copy_of(src, dst)
        copy.start()
        arrive = copy_of(land, land)
        rate = CORE_RATE if link == "core" else ICI_RATE
        end = max(self.now, self.free.get(link, 0.0)) + nbytes(land) / rate
        self.free[link] = end
        sent = Handle(end + 0.5, copy.wait_send)
        self.open.append(sent)
        return Handle(end + 2.0, arrive.wait_recv), sent

    def copy(self, src, dst):
        if self.local_free:
            i = self.local_free.pop(0)
        else:
            i = self.local_used
            self.local_used += 1
        copy = pltpu.make_async_copy(src, dst, self.local_sems.at[i])
        copy.start()
        end = max(self.now, self.free.get("hbm", 0.0)) + nbytes(src) / HBM_RATE
        self.free["hbm"] = end
        handle = Handle(end + 0.8, copy.wait, lambda: self.local_free.append(i))
        self.open.append(handle)
        return handle

    def when(self, handles, then):
        self.seq += 1
        heapq.heappush(self.heap, (max(h.time for h in handles), self.seq, handles, then))

    def job(self, flags, needs, then, cost, rank, line=None):
        self.seq += 1
        self.jobs.append((rank, self.seq, flags, needs, then, cost, line))
        self.jobs.sort(key=lambda j: j[:2])

    def run(self):
        while True:
            if self.heap and self.heap[0][0] + MARGIN <= self.now:
                self.event()
                continue
            chosen = None
            soonest = float("inf")
            held = set()
            for j in self.jobs:
                if j[6] is not None:
                    if j[6] in held:
                        continue
                    held.add(j[6])
                if any(f.left > 0 for f in j[2]):
                    continue
                ready = max((pool.when_ready(n) for pool, n in j[3]), default=0.0)
                if ready <= self.now:
                    chosen = j
                    break
                soonest = min(soonest, ready)
            if chosen is not None:
                self.jobs.remove(chosen)
                _, _, _, needs, then, cost, _ = chosen
                slots = [pool.take(n) for pool, n in needs]
                self.now += cost
                then(*slots)
                continue
            if self.heap and self.heap[0][0] <= soonest:
                self.event()
            elif soonest < float("inf"):
                self.now = max(self.now, soonest)
            else:
                break
        assert not self.jobs, "jobs left"
        for handle in self.open:
            handle.wait()

    def event(self):
        time, _, handles, then = heapq.heappop(self.heap)
        self.now = max(self.now, time)
        for h in handles:
            h.wait()
        then()

    def arrive(self, handle, flag):
        self.when([handle], flag.hit)


def nothing():
    pass


def gather_ring_first(net, own, slot, half, ring, pair, me, each):
    r, rp, rm, r2, p = me
    up, down = ring
    from_down, _ = net.send(up, own, slot(r, p), slot(rm, p))
    from_up, _ = net.send(down, own, slot(r, p), slot(rp, p))
    other, _ = net.send(pair, own, slot(r, p), slot(r, 1 - p))
    net.when([other], lambda: each("o", 1, r, 1 - p))

    def pass_on(name, q):
        got, _ = net.send(pair, slot(q, p), slot(q, p), slot(q, 1 - p))
        net.when([got], lambda: each(name, 1, q, 1 - p))

    far = []

    def got_near(name, q, h, link):
        def then():
            ref = half(slot(q, p), h)
            far.append(net.send(link, ref, ref, half(slot(r2, p), h))[0])
            pass_on(name, q)
            each(name, 0, q, p)
            if len(far) == 2:
                net.when(far, got_far)
        return then

    def got_far():
        pass_on("2", r2)
        each("2", 0, r2, p)

    net.when([from_down], got_near("-", rm, 0, up))
    net.when([from_up], got_near("+", rp, 1, down))


def gather_pair_first(net, own, slot, half, ring, pair, me, each, late=False):
    r, rp, rm, r2, p = me
    up, down = ring

    def around(src, q, k):
        from_down, _ = net.send(up, src, slot(r, q), slot(rm, q))
        from_up, _ = net.send(down, src, slot(r, q), slot(rp, q))
        far = []

        def got_near(name, s, h, link):
            def then():
                ref = half(slot(s, q), h)
                far.append(net.send(link, ref, ref, half(slot(r2, q), h))[0])
                each(name, k, s, q)
                if k == 0 and late:
                    go_other()
                if len(far) == 2:
                    net.when(far, lambda: each("2", k, r2, q))
            return then

        net.when([from_down], got_near("-", rm, 0, up))
        net.when([from_up], got_near("+", rp, 1, down))

    other, _ = net.send(pair, own, slot(r, p), slot(r, 1 - p))
    before = Flag(3 if late else 1)

    def go_other():
        before.hit()
        if before.left == 0:
            around(slot(r, 1 - p), 1 - p, 1)

    def got_other():
        each("o", 1, r, 1 - p)
        go_other()

    net.when([other], got_other)
    around(own, p, 0)


def sum_rows(dst, srcs):
    if len(dst.shape) > 2:
        for i in range(dst.shape[0]):
            sum_rows(dst.at[i], [s.at[i] for s in srcs])
        return
    step = 16

    @pl.loop(0, dst.shape[0] // step)
    def _(i):
        at = pl.ds(pl.multiple_of(i * step, step), step)
        total = dst[at, :]
        for s in srcs:
            total = total + s[at, :]
        dst[at, :] = total


def dot(a, b, ca, cb):
    return lax.dot_general(a, b, (((ca,), (cb,)), ((), ())), preferred_element_type=F32)


def nth(refs, i, n):
    size = refs.shape[0] // n
    return refs.at[pl.ds(i * size, size)]


ORDER = ("2", "+", "-", "o")


class Adder:
    def __init__(self, net, pool, view):
        self.net, self.pool, self.view = net, pool, view

    def add(self, flags, srcs, outs, then):
        net, pool = self.net, self.pool

        def begin(slots):
            refs = [self.view(pool.refs[i], srcs[0].shape) for i in slots]
            loads = [net.copy(src, ref) for src, ref in zip(srcs, refs)]

            def done():
                sum_rows(refs[0], refs[1:])
                net.now += 0.25 * len(refs) * nbytes(refs[0]) / 1.0e6
                for i in slots[1:]:
                    pool.give(i)
                copies = [net.copy(src, dst) for src, dst in outs(refs[0])]
                pool.give(slots[0], copies)
                net.when(copies, then)

            net.when(loads, done)

        net.job(flags, [(pool, len(srcs))], begin, 0.1, 1)


def ring_reduce(net, adder, ready, srcs, l1, l2, links, near):
    come = [Flag(), Flag()]

    def go(name, h, more, flags, link, dst, flag):
        terms = srcs(name, h) + more

        def send():
            got, _ = net.send(link, terms[0], dst)
            net.arrive(got, flag)

        if len(terms) == 1:
            net.job(ready(name, h) + flags, [], send, 0.1, 1)
        else:
            adder.add(ready(name, h) + flags, terms, lambda ref: [(ref, terms[0])], send)

    for h, link in enumerate(links):
        go("2", h, [], [], link, l1.at[h], come[h])
    for k, (link, name) in enumerate(zip(links, "+-")):
        go(name, 1 - k, [], [], link, l2.at[k, 1 - k], near[1 - k])
        go(name, k, [l1.at[k]], [come[k]], link, l2.at[k, k], near[k])


def layer_kernel(
    x_ref, dy_ref, wg_ref, wu_ref, wd_ref,
    y_own, y_l2, r_own, r_lp, q_own, q_l2, g_own, g_lp, u_own, u_lp, v_own, v_l2, d_own, d_l2,
    x_all, dy_all, wd_ext, y_pt, r_pt, q_pt, w_pt, y_l1, r_l1, r_l2, q_lp, q_l1, w_lc,
    g_l1, g_l2, u_l1, u_l2, v_lp, v_l1, d_lp, d_l1,
    wg_all, wu_all, wd_all, h_all, da_all, db_all, h_ext, xb, db, xs, ds, r_out, q_out, y_out, wx, tw, tk, wk,
    local_sems, send_sems, recv_sems,
):
    here = Place()
    here.barrier()
    net = Net(here, local_sems, send_sems, recv_sems)
    z, zp, zm, z2, b = here.z, here.zp, here.zm, here.z2, here.b
    x, xp, xm, x2, a, c = here.x, here.xp, here.xm, here.x2, here.a, here.c
    micro, rows, width = x_ref.shape
    wr, wc = wg_ref.shape
    half_width = width // 2
    edge = width * 5 // 24
    m_blk = micro * rows
    n_blk = 2 * m_blk
    zs = {"o": z, "+": zp, "-": zm, "2": z2}
    xs_of = {"o": x, "+": xp, "-": xm, "2": x2}
    ring_z, ring_x = ("z+", "z-"), ("x+", "x-")

    def rows_at(start, size):
        return pl.ds(pl.multiple_of(start, size), size)

    weights_in = [Flag(24), Flag(24)]
    tokens_in = {k: Flag(5 if k == "o" else 6) for k in zs}
    ext_in = Flag(16)

    def up_slot(ref, core):
        return lambda q, p: ref.at[rows_at((q * 2 + core) * wr, wr), rows_at(p * wc, wc)]

    def down_slot(ref, core):
        return lambda q, p: ref.at[rows_at(p * wc, wc), rows_at((q * 2 + core) * wr, wr)]

    def row_half(ref, h):
        return nth(ref, h, 2)

    def tok_half(ref, h):
        return ref.at[h]

    in_z = (z, zp, zm, z2, b)
    in_x = (x, xp, xm, x2, a)

    def across(mine, theirs):
        def each(name, k, q, p):
            weights_in[k].hit()
            got, _ = net.send("core", mine(q, p), mine(q, p), theirs(q, p))
            net.arrive(got, weights_in[k])
        return each

    for fn, own, mine, theirs in (
        (gather_ring_first, wg_ref, up_slot(wg_all, c), up_slot(wg_all, 1 - c)),
        (functools.partial(gather_pair_first, late=True), wu_ref, up_slot(wu_all, c), up_slot(wu_all, 1 - c)),
        (functools.partial(gather_pair_first, late=True), wd_ref, down_slot(wd_all, c), down_slot(wd_all, 1 - c)),
    ):
        fn(net, own, mine, row_half, ring_x, "wgt", in_x, across(mine, theirs))
        got, _ = net.send("core", own, mine(x, a), theirs(x, a))
        net.arrive(got, weights_in[0])
        net.arrive(net.copy(own, mine(x, a)), weights_in[0])

    ext, ext_side = down_slot(wd_ext, c), down_slot(wd_ext, 1 - c)

    def ext_each(q, p):
        ext_in.hit()
        got, _ = net.send("core", ext(q, p), ext(q, p), ext_side(q, p))
        net.arrive(got, ext_in)

    def ext_round(p):
        from_down, _ = net.send("x+", ext(x, p), ext(x, p), ext(xm, p))
        from_up, _ = net.send("x-", ext(x, p), ext(x, p), ext(xp, p))
        far = []

        def near(q, h, link):
            def then():
                ref = row_half(ext(q, p), h)
                far.append(net.send(link, ref, ref, row_half(ext(x2, p), h))[0])
                ext_each(q, p)
                if len(far) == 2:
                    net.when(far, lambda: ext_each(x2, p))
            return then

        net.when([from_down], near(xm, 0, "x+"))
        net.when([from_up], near(xp, 1, "x-"))
        ext_each(x, p)

    def ext_start():
        got, _ = net.send("tok", wd_ref, ext(x, a))

        def pass_on():
            more, _ = net.send("wgt", ext(x, a), ext(x, a), ext(x, 1 - a))
            net.when([more], lambda: ext_round(1 - a))
            ext_round(a)

        net.when([got], pass_on)

    started = []

    def count_tokens(name, k, q, p):
        tokens_in[name].hit()

    def count_main(name, k, q, p):
        count_tokens(name, k, q, p)
        if name == "-" and not started:
            started.append(True)
            ext_start()

    for fn, own, dst, cols, each in (
        (gather_pair_first, x_ref, x_all, pl.ds(width - edge, edge), count_tokens),
        (gather_ring_first, x_ref, x_all, pl.ds(0, width - edge), count_main),
        (gather_pair_first, dy_ref, dy_all, pl.ds(0, width), count_tokens),
    ):
        slot = functools.partial(lambda q, p, dst, cols: dst.at[q, p, :, :, cols], dst=dst, cols=cols)
        fn(net, own.at[:, :, cols], slot, tok_half, ring_z, "tok", in_z, each)

    tok_pool = Pool([(xb.at[i], db.at[i]) for i in range(xb.shape[0])])
    cut_pool = Pool([(xs.at[i], ds.at[i]) for i in range(xs.shape[0])])
    r_pool = Pool([r_out.at[i] for i in range(r_out.shape[0])])
    q_pool = Pool([q_out.at[i] for i in range(q_out.shape[0])])
    y_pool = Pool([y_out.at[i] for i in range(y_out.shape[0])])
    ext_pool = Pool([wx.at[i] for i in range(wx.shape[0])])
    wout_pool = Pool([tw.at[i] for i in range(tw.shape[0])])
    tk_pool = Pool([tk.at[i] for i in range(tk.shape[0])])
    wk_pool = Pool([wk.at[i] for i in range(wk.shape[0])])

    first_slot = tok_pool.take(1)[0]
    bounce = tok_pool.refs[first_slot]
    into = [net.copy(src, ref.at[0]) for src, ref in zip((x_ref, dy_ref), bounce)]

    def own_rows():
        out = [net.copy(ref.at[0], dst.at[z, b]) for ref, dst in zip(bounce, (x_all, dy_all))]
        tok_pool.give(first_slot, out)
        for handle in out:
            net.arrive(handle, tokens_in["o"])

    net.when(into, own_rows)

    ranks = {step: 10 + i for i, step in enumerate(STEPS)}

    hidden = {k: Flag(2) for k in zs}
    ext_rows = Flag(4)
    tile_h = min(256, wc)

    def block(name):
        return rows_at(zs[name] * n_blk, n_blk)

    def hidden_of(name, turn):
        cols_at = a * wc if turn == 0 else (1 - a) * wc
        rank = ranks["H" + name + "ab"[turn]]
        loaded = Flag()
        held = []

        def load(slots):
            i = slots[0]
            held.append(i)
            one, two = tok_pool.refs[i]
            net.when([net.copy(x_all.at[zs[name]], one), net.copy(dy_all.at[zs[name]], two)], loaded.hit)

        def multiply():
            i = held[0]
            one, two = tok_pool.refs[i]
            at = block(name)

            @pl.loop(0, wc // tile_h)
            def _(j):
                cols = rows_at(cols_at + j * tile_h, tile_h)
                x_blk = one[...].reshape(n_blk, width)
                dy_blk = two[...].reshape(n_blk, width)
                pre = dot(x_blk, wg_all[:, cols], 1, 0)
                up = dot(x_blk, wu_all[:, cols], 1, 0)
                g = dot(dy_blk, wd_all[cols, :], 1, 1)
                s = jax.nn.sigmoid(pre)
                act = pre * s
                h_all[at, cols] = (act * up).astype(BF16)
                da_all[at, cols] = (g * up * s * (1.0 + pre * (1.0 - s))).astype(BF16)
                db_all[at, cols] = (g * act).astype(BF16)

            tok_pool.give(i)
            hidden[name].hit()

        net.job([tokens_in[name]], [(tok_pool, 1)], load, 0.1, rank * 0.01, "load")
        net.job([loaded, weights_in[turn]], [], multiply, 2.8, rank, "mxu")

    def give_hidden(name):
        def go():
            src = h_all.at[rows_at(zs[name] * n_blk + (1 - b) * m_blk, m_blk), :]
            got, _ = net.send("tok", src, h_ext.at[rows_at(zs[name] * m_blk, m_blk), :])
            net.arrive(got, ext_rows)
        net.job([hidden[name]], [], go, 0.1, 1)

    for name in zs:
        hidden_of(name, 0)
        hidden_of(name, 1)
        give_hidden(name)

    r_in = {k: Flag() for k in zs}
    q_in = {k: Flag() for k in zs}
    tile_dx = half_width // 2

    def rows_of(name, pool, part, flag, col0, rank):
        at = block(name)

        def multiply(slots):
            i = slots[0]
            ref = pool.refs[i]

            @pl.loop(0, half_width // tile_dx)
            def _(j):
                src = rows_at(col0 + j * tile_dx, tile_dx)
                val = dot(da_all[at, :], wg_all[src, :], 1, 1) + dot(db_all[at, :], wu_all[src, :], 1, 1)
                ref[:, :, :, rows_at(j * tile_dx, tile_dx)] = val.reshape(2, micro, rows, tile_dx)

            done = net.copy(ref, part.at[zs[name]])
            pool.give(i, [done])
            net.when([done], flag.hit)

        net.job([hidden[name]], [(pool, 1)], multiply, 1.9, rank, "mxu")

    for name in zs:
        rows_of(name, r_pool, r_pt, r_in[name], 0, ranks["R" + name])
        rows_of(name, q_pool, q_pt, q_in[name], half_width, ranks["Q" + name])

    quarter = width // 4
    tile_y = quarter // 3 if quarter % 3 == 0 else quarter
    y_in = [Flag(2), Flag(2)]

    def y_of(j):
        loaded = Flag()
        held = []
        cols = pl.ds(j * quarter, quarter)

        def load(slots):
            held.append(slots[0])
            net.when([net.copy(wd_ext.at[:, cols], ext_pool.refs[slots[0]])], loaded.hit)

        def multiply(slots):
            i = slots[0]
            ref = y_pool.refs[i]
            w_ref = ext_pool.refs[held[0]]
            mine = [rows_at(zs[name] * n_blk + b * m_blk, m_blk) for name in ORDER]
            other = [rows_at(zs[name] * m_blk, m_blk) for name in ORDER]

            @pl.loop(0, quarter // tile_y)
            def _(n):
                near = jnp.concatenate([h_all[at, :] for at in mine], axis=0)
                far = jnp.concatenate([h_ext[at, :] for at in other], axis=0)
                at = rows_at(n * tile_y, tile_y)
                val = dot(near, wd_all[:, rows_at(j * quarter + n * tile_y, tile_y)], 1, 0) + dot(far, w_ref[:, at], 1, 0)
                ref[:, :, :, at] = val.reshape(4, micro, rows, tile_y)

            ext_pool.give(held[0])
            half = pl.ds((j % 2) * quarter, quarter)
            out = [net.copy(ref.at[k], y_pt.at[j // 2, k, :, :, half]) for k in range(3)]
            out.append(net.copy(ref.at[3], y_own.at[:, :, cols]))
            y_pool.give(i, out)
            net.when(out, y_in[j // 2].hit)

        net.job([ext_in], [(ext_pool, 1)], load, 0.1, 3 + 0.01 * j, "ext")
        net.job([loaded, ext_rows], [(y_pool, 1)], multiply, 1.9, ranks["Y%d" % j], "mxu")

    for j in range(4):
        y_of(j)

    def tok_view(ref, shape):
        return ref if len(shape) == 3 else ref.at[0]

    tok_add = Adder(net, tk_pool, tok_view)
    names = {name: k for k, name in enumerate(ORDER)}

    r_near = [Flag(2), Flag(2)]
    ring_reduce(
        net, tok_add, lambda name, h: [r_in[name]], lambda name, h: [r_pt.at[zs[name], :, h]],
        r_l1, r_l2, ring_z, r_near,
    )

    def r_last(h):
        away = r_pt.at[z, 1 - b, h]

        def go():
            got, _ = net.send("tok", away, r_lp.at[h])
            net.when([got], nothing)

        tok_add.add(
            [r_in["o"], r_near[h]], [r_pt.at[z, :, h], r_l2.at[0, h], r_l2.at[1, h]],
            lambda ref: [(ref.at[1 - b], away), (ref.at[b], r_own.at[h])], go,
        )

    r_last(0)
    r_last(1)

    for j in range(2):
        ring_reduce(
            net, tok_add, lambda name, h, j=j: [y_in[j]], lambda name, h, j=j: [y_pt.at[j, names[name], h]],
            y_l1.at[j], y_l2.at[j], ring_z, [Flag(2), Flag(2)],
        )

    q_pair = {k: Flag() for k in zs}

    def pair_q(name):
        def go():
            got, _ = net.send("tok", q_pt.at[zs[name], 1 - b], q_lp.at[names[name]])
            net.arrive(got, q_pair[name])
        net.job([q_in[name]], [], go, 0.1, 1)

    for name in ORDER:
        pair_q(name)
    ring_reduce(
        net, tok_add, lambda name, h: [q_in[name], q_pair[name]],
        lambda name, h: [q_pt.at[zs[name], b, h], q_lp.at[names[name], h]], q_l1, q_l2, ring_z, [Flag(2), Flag(2)],
    )
    tok_add.add(
        [q_in["o"], q_pair["o"]], [q_pt.at[z, b], q_lp.at[3]], lambda ref: [(ref, q_own)], nothing,
    )

    tile_w = wc
    n_tok = 4 * n_blk
    w_in = {(m, k): Flag() for m in range(3) for k in range(4)}
    w_side = {(m, k): Flag() for m in range(3) for k in range(4)}
    all_hidden = list(hidden.values())

    def grads_of(k, name, core, turn):
        loaded = Flag()
        held = []
        cols = rows_at((xs_of[name] * 2 + core) * wr, wr)

        def load(slots):
            i = slots[0]
            held.append(i)
            one, two = cut_pool.refs[i]
            net.when([net.copy(x_all.at[:, :, :, :, cols], one), net.copy(dy_all.at[:, :, :, :, cols], two)], loaded.hit)

        def out(m, j, ref):
            if turn == 0:
                got, sent = net.send("core", ref, w_lc.at[m, k])
                wout_pool.give(j, [sent])
                net.arrive(got, w_side[m, k])
            else:
                done = net.copy(ref, w_pt.at[m, k])
                wout_pool.give(j, [done])
                net.when([done], w_in[m, k].hit)

        def from_x(slots):
            one, _ = cut_pool.refs[held[0]]
            outs = [wout_pool.refs[j] for j in slots]

            @pl.loop(0, 2 * wc // tile_w)
            def _(j):
                at = rows_at(j * tile_w, tile_w)
                cut = one[...].reshape(n_tok, wr)
                outs[0][:, at] = dot(cut, da_all[:, at], 0, 0)
                outs[1][:, at] = dot(cut, db_all[:, at], 0, 0)

            for m in range(2):
                out(m, slots[m], outs[m])

        def from_dy(slots):
            _, two = cut_pool.refs[held[0]]
            ref = wout_pool.refs[slots[0]]

            @pl.loop(0, 2 * wc // tile_w)
            def _(j):
                at = rows_at(j * tile_w, tile_w)
                ref[:, at] = dot(two[...].reshape(n_tok, wr), h_all[:, at], 0, 0)

            cut_pool.give(held[0])
            out(2, slots[0], ref)

        rank = ranks["W%d%s" % (k, "ab"[turn])]
        net.job(list(tokens_in.values()), [(cut_pool, 1)], load, 0.1, 2 + 0.01 * rank, "cut")
        net.job([loaded] + all_hidden, [(wout_pool, 2)], from_x, 2.0, rank, "mxu")
        net.job([loaded] + all_hidden, [(wout_pool, 1)], from_dy, 1.1, rank + 0.5, "mxu")

    for k, name in enumerate(ORDER):
        grads_of(k, name, 1 - c, 0)
        grads_of(k, name, c, 1)

    def w_view(ref, shape):
        return ref.at[pl.ds(0, shape[0]), pl.ds(0, shape[1])]

    w_add = Adder(net, wk_pool, w_view)
    mine, other = rows_at(a * wc, wc), rows_at((1 - a) * wc, wc)

    def w_ring_first(m, row0, size, l1, l2, lp, own):
        def part(ref, h):
            return ref.at[pl.ds(row0 + h * (size // 2), size // 2)]

        near = [Flag(2), Flag(2)]
        ring_reduce(
            net, w_add, lambda name, h: [w_in[m, names[name]], w_side[m, names[name]]],
            lambda name, h: [part(w_pt.at[m, names[name]], h), part(w_lc.at[m, names[name]], h)], l1, l2, ring_x, near,
        )

        def last(h):
            block = part(w_pt.at[m, 3], h)
            away = block.at[:, other]

            def go():
                got, _ = net.send("wgt", away, row_half(lp, h))
                net.when([got], nothing)

            w_add.add(
                [w_in[m, 3], w_side[m, 3], near[h]], [block, part(w_lc.at[m, 3], h), l2.at[0, h], l2.at[1, h]],
                lambda ref: [(ref.at[:, other], away), (ref.at[:, mine], row_half(own, h))], go,
            )

        last(0)
        last(1)

    def w_pair_first(m, row0, size, lp, l1, l2, own):
        def part(ref, h):
            return ref.at[pl.ds(row0 + h * (size // 2), size // 2)]

        have = {k: [w_in[m, k], w_side[m, k]] for k in range(4)}
        pair = {(k, h): Flag() for k in range(4) for h in range(2)}

        def away(k, h):
            dst = part(w_pt.at[m, k], h).at[:, other]

            def go():
                got, _ = net.send("wgt", dst, row_half(lp.at[k], h))
                net.arrive(got, pair[k, h])

            w_add.add(have[k], [dst, part(w_lc.at[m, k], h).at[:, other]], lambda ref: [(ref, dst)], go)

        for k in range(4):
            for h in range(2):
                away(k, h)

        def terms(name, h):
            k = names[name]
            return [part(w_pt.at[m, k], h).at[:, mine], part(w_lc.at[m, k], h).at[:, mine], row_half(lp.at[k], h)]

        def ready(name, h):
            return have[names[name]] + [pair[names[name], h]]

        ring_reduce(net, w_add, ready, terms, l1, l2, ring_x, [Flag(2), Flag(2)])
        for h in range(2):
            w_add.add(ready("o", h), terms("o", h), lambda ref, h=h: [(ref, row_half(own, h))], nothing)

    most = wr * 2 // 3
    w_ring_first(0, 0, wr, g_l1, g_l2, g_lp, g_own)
    w_pair_first(2, 0, wr, d_lp, d_l1, d_l2, d_own)
    w_ring_first(1, 0, most, u_l1, u_l2, u_lp, u_own)
    w_pair_first(1, most, wr - most, v_lp, v_l1, v_l2, v_own)
    net.run()


def solution(mesh):
    row_spec = P(None, ("dp", "tp"), None)
    in_specs = (row_spec, P("dp", "tp"), P("dp", "tp"), P("tp", "dp"), row_spec)
    out_specs = (row_spec, row_spec, P("dp", "tp"), P("dp", "tp"), P("tp", "dp"))
    hbm = pl.BlockSpec(memory_space=pl.ANY)
    dma = pltpu.SemaphoreType.DMA
    V = pltpu.VMEM
    S = jax.ShapeDtypeStruct

    def local_step(x_loc, wg, wu, wd, dy_loc):
        micro, rows, width = x_loc.shape
        wr, wc = wg.shape
        half = width // 2
        most = wr * 2 // 3
        tok = (micro, rows, width)
        tok_h = (micro, rows, half)
        n = 8 * micro * rows

        def ring_first(size):
            return S((2, size // 2, 2 * wc), F32), S((2, 2, size // 2, 2 * wc), F32)

        def pair_first(size):
            return S((4, size, wc), F32), S((2, size // 2, wc), F32)

        def pair_last(size):
            return S((size, wc), F32), S((2, 2, size // 2, wc), F32)

        outs = [
            S(tok, F32), S((2, 2) + tok_h, F32), S(tok_h, F32), S(tok_h, F32), S(tok_h, F32), S((2,) + tok_h, F32),
            S((wr, wc), F32), S((wr, wc), F32), S((most, wc), F32), S((most, wc), F32),
            *pair_last(wr - most), *pair_last(wr),
        ]
        space = [
            S((4, 2) + tok, BF16), S((4, 2) + tok, BF16), S((2 * wc, width), BF16),
            S((2, 3) + tok_h, F32), S((4, 2) + tok_h, F32), S((4, 2) + tok_h, F32), S((3, 4, wr, 2 * wc), F32),
            S((2, 2) + tok_h[1:], F32), S((2, 2) + tok_h[1:], F32), S((2, 2, 2) + tok_h[1:], F32),
            S((4,) + tok_h, F32), S((2,) + tok_h[1:], F32), S((3, 4, wr, 2 * wc), F32),
            *ring_first(wr), *ring_first(most), *pair_first(wr - most), *pair_first(wr),
        ]
        res = pl.pallas_call(
            layer_kernel,
            name="layer",
            out_shape=tuple(outs + space),
            in_specs=[hbm] * 5,
            out_specs=[hbm] * (len(outs) + len(space)),
            scratch_shapes=[
                V((width, 2 * wc), BF16), V((width, 2 * wc), BF16), V((2 * wc, width), BF16),
                V((n, 2 * wc), BF16), V((n, 2 * wc), BF16), V((n, 2 * wc), BF16), V((n // 2, 2 * wc), BF16),
                V((2, 2) + tok, BF16), V((2, 2) + tok, BF16),
                V((2, 4, 2, micro, rows, wr), BF16), V((2, 4, 2, micro, rows, wr), BF16),
                V((1, 2) + tok_h, F32), V((2, 2) + tok_h, F32),
                V((2, 4, micro, rows, width // 4), F32), V((2, 2 * wc, width // 4), BF16), V((5, wr, 2 * wc), F32),
                V((6, 2, rows, half), F32), V((6, wr // 2, 2 * wc), F32),
                dma((128,)), dma((200,)), dma((200,)),
            ],
            compiler_params=pltpu.CompilerParams(
                collective_id=0, has_side_effects=True, vmem_limit_bytes=67_000_000
            ),
        )(x_loc, dy_loc, wg, wu, wd)
        y_own, y_l2, r_own, r_lp, q_own, q_l2, g_own, g_lp, u_own, u_lp, v_own, v_l2, d_own, d_l2 = res[: len(outs)]
        y_in = jnp.concatenate([y_l2[j, 0] + y_l2[j, 1] for j in range(2)], axis=2)
        y = (x_loc.astype(F32) + (y_own + y_in)).astype(BF16)
        dx = (dy_loc.astype(F32) + jnp.concatenate([r_own + r_lp, q_own + q_l2[0] + q_l2[1]], axis=2)).astype(BF16)
        u_sum = jnp.concatenate([u_own + u_lp, v_own + (v_l2[0] + v_l2[1]).reshape(v_own.shape)], axis=0)
        d_sum = d_own + (d_l2[0] + d_l2[1]).reshape(d_own.shape)
        return y, dx, g_own + g_lp, u_sum, d_sum.T

    return jax.shard_map(local_step, mesh=mesh, in_specs=in_specs, out_specs=out_specs, check_vma=False)
```

```python
import functools
import heapq

import jax
import jax.numpy as jnp
from jax import lax
from jax.experimental import pallas as pl
from jax.experimental.pallas import tpu as pltpu
from jax.sharding import PartitionSpec as P

MESH = pl.DeviceIdType.MESH
F32 = jnp.float32
BF16 = jnp.bfloat16
ICI_RATE = 45.0e3
CORE_RATE = 550.0e3
HBM_RATE = 2.5e6
MARGIN = 0.5
FIRST, NEXT, EARLY = 0.5, 1, 0.01
SIDES = (0, 1)
RING = 4
AROUND = (1, 3, 2)
BLOCKS = {
    "A": (("o", 0), ("o", 1)), "B": (("-", 0), ("+", 0)), "C": (("-", 1), ("+", 1)), "D": (("2", 0),), "E": (("2", 1),),
}
STEPS = (
    "HAa", "HBa", "HBb", "HAb", "HDb", "HCb", "HCa", "HDa", "HEb", "HEa",
    "R2", "W0au", "W0ad", "W0bu", "W0bd", "R+", "W0bg", "W0ag", "W2a", "R-",
    "Q+", "Q2", "W2b", "W1a", "W3b", "Y2", "W1b", "Y0", "Y1", "Qo",
    "Q-", "Ro", "W3a", "Y3",
)


def nbytes(ref):
    size = jnp.dtype(ref.dtype).itemsize
    for n in ref.shape:
        size *= n
    return size


class Place:
    def __init__(self):
        t = lax.axis_index("tp")
        d = lax.axis_index("dp")
        z, y, x, c = t // RING, t % RING, d // 2, d % 2
        self.z, self.y, self.x, self.c = z, y, x, c
        self.b = y % 2
        self.a = y // 2
        self.zp, self.zm, self.z2 = ((z + n) % RING for n in AROUND)
        self.xp, self.xm, self.x2 = ((x + n) % RING for n in AROUND)

        def at(z, y, x, c):
            return {"tp": z * RING + y, "dp": x * 2 + c}

        self.dev = {
            "z+": at(self.zp, y, x, c),
            "z-": at(self.zm, y, x, c),
            "x+": at(z, y, self.xp, c),
            "x-": at(z, y, self.xm, c),
            "tok": at(z, y + 1 - 2 * self.b, x, c),
            "wgt": at(z, 3 - y, x, c),
            "core": at(z, y, x, 1 - c),
        }

    def barrier(self):
        sem = pltpu.get_barrier_semaphore()
        for dev in self.dev.values():
            pl.semaphore_signal(sem, inc=1, device_id=dev, device_id_type=MESH)
        pl.semaphore_wait(sem, len(self.dev))


class Handle:
    def __init__(self, time, wait, after=None):
        self.time, self._wait, self.after, self.done = time, wait, after, False

    def wait(self):
        if not self.done:
            self.done = True
            self._wait()
            if self.after is not None:
                self.after()


class Flag:
    def __init__(self, count=1):
        self.left = count

    def hit(self):
        self.left -= 1


class Pool:
    def __init__(self, refs):
        self.refs = refs
        self.back = [[] for _ in refs]
        self.free = [True] * len(refs)

    def when_ready(self, count):
        times = sorted(max((h.time for h in self.back[i]), default=0.0) for i in range(len(self.refs)) if self.free[i])
        return times[count - 1] if len(times) >= count else float("inf")

    def take(self, count):
        order = sorted(
            (max((h.time for h in self.back[i]), default=0.0), i) for i in range(len(self.refs)) if self.free[i]
        )
        got = [i for _, i in order[:count]]
        for i in got:
            for h in self.back[i]:
                h.wait()
            self.back[i] = []
            self.free[i] = False
        return got

    def give(self, i, handles=()):
        self.free[i] = True
        self.back[i] = list(handles)


class Net:
    def __init__(self, place, local_sems, send_sems, recv_sems):
        self.place, self.local_sems, self.send_sems, self.recv_sems = place, local_sems, send_sems, recv_sems
        self.used = 0
        self.local_used = 0
        self.local_free = []
        self.open = []
        self.heap = []
        self.jobs = []
        self.seq = 0
        self.now = 0.0
        self.free = {}
        self.log = []

    def send(self, link, src, dst, land=None):
        land = dst if land is None else land
        i = self.used
        self.used += 1
        dev = self.place.dev[link]

        def copy_of(a, b):
            return pltpu.make_async_remote_copy(
                src_ref=a, dst_ref=b, send_sem=self.send_sems.at[i], recv_sem=self.recv_sems.at[i],
                device_id=dev, device_id_type=MESH,
            )

        copy = copy_of(src, dst)
        copy.start()
        arrive = copy_of(land, land)
        rate = CORE_RATE if link == "core" else ICI_RATE
        end = max(self.now, self.free.get(link, 0.0)) + nbytes(land) / rate
        self.free[link] = end
        sent = Handle(end + 0.5, copy.wait_send)
        self.open.append(sent)
        return Handle(end + 2.0, arrive.wait_recv), sent

    def copy(self, src, dst):
        if self.local_free:
            i = self.local_free.pop(0)
        else:
            i = self.local_used
            self.local_used += 1
        copy = pltpu.make_async_copy(src, dst, self.local_sems.at[i])
        copy.start()
        end = max(self.now, self.free.get("hbm", 0.0)) + nbytes(src) / HBM_RATE
        self.free["hbm"] = end
        handle = Handle(end + 0.8, copy.wait, lambda: self.local_free.append(i))
        self.open.append(handle)
        return handle

    def when(self, handles, then):
        self.seq += 1
        heapq.heappush(self.heap, (max(h.time for h in handles), self.seq, handles, then))

    def job(self, flags, needs, then, rank, line=None, cost=0.1):
        self.seq += 1
        self.jobs.append((rank, self.seq, flags, needs, then, cost, line))
        self.jobs.sort(key=lambda j: j[:2])

    def run(self):
        while True:
            if self.heap and self.heap[0][0] + MARGIN <= self.now:
                self.event()
                continue
            chosen = None
            soonest = float("inf")
            held = set()
            for j in self.jobs:
                if j[6] is not None:
                    if j[6] in held:
                        continue
                    held.add(j[6])
                if any(f.left > 0 for f in j[2]):
                    continue
                ready = max((pool.when_ready(n) for pool, n in j[3]), default=0.0)
                if ready <= self.now:
                    chosen = j
                    break
                soonest = min(soonest, ready)
            if chosen is not None:
                self.jobs.remove(chosen)
                _, _, _, needs, then, cost, _ = chosen
                slots = [pool.take(n) for pool, n in needs]
                self.now += cost
                then(*slots)
                continue
            if self.heap and self.heap[0][0] <= soonest:
                self.event()
            elif soonest < float("inf"):
                self.now = max(self.now, soonest)
            else:
                break
        assert not self.jobs, "jobs left"
        for handle in self.open:
            handle.wait()

    def event(self):
        time, _, handles, then = heapq.heappop(self.heap)
        self.now = max(self.now, time)
        for h in handles:
            h.wait()
        then()

    def arrive(self, handle, flag):
        self.when([handle], flag.hit)


def nothing():
    pass


def gather_ring_first(net, own, slot, half, ring, pair, me, each):
    r, rp, rm, r2, p = me
    up, down = ring
    from_down, _ = net.send(up, own, slot(r, p), slot(rm, p))
    from_up, _ = net.send(down, own, slot(r, p), slot(rp, p))
    other, _ = net.send(pair, own, slot(r, p), slot(r, 1 - p))
    net.when([other], lambda: each("o", 1, r, 1 - p))

    def pass_on(name, q):
        got, _ = net.send(pair, slot(q, p), slot(q, p), slot(q, 1 - p))
        net.when([got], lambda: each(name, 1, q, 1 - p))

    far = []

    def got_near(name, q, h, link):
        def then():
            ref = half(slot(q, p), h)
            far.append(net.send(link, ref, ref, half(slot(r2, p), h))[0])
            pass_on(name, q)
            each(name, 0, q, p)
            if len(far) == 2:
                net.when(far, got_far)
        return then

    def got_far():
        pass_on("2", r2)
        each("2", 0, r2, p)

    net.when([from_down], got_near("-", rm, 0, up))
    net.when([from_up], got_near("+", rp, 1, down))


def gather_pair_first(net, own, slot, half, ring, pair, me, each, late=False):
    r, rp, rm, r2, p = me
    up, down = ring

    def around(src, q, k):
        from_down, _ = net.send(up, src, slot(r, q), slot(rm, q))
        from_up, _ = net.send(down, src, slot(r, q), slot(rp, q))
        far = []

        def got_near(name, s, h, link):
            def then():
                ref = half(slot(s, q), h)
                far.append(net.send(link, ref, ref, half(slot(r2, q), h))[0])
                each(name, k, s, q)
                if k == 0 and late:
                    go_other()
                if len(far) == 2:
                    net.when(far, lambda: each("2", k, r2, q))
            return then

        net.when([from_down], got_near("-", rm, 0, up))
        net.when([from_up], got_near("+", rp, 1, down))

    other, _ = net.send(pair, own, slot(r, p), slot(r, 1 - p))
    before = Flag(3 if late else 1)

    def go_other():
        before.hit()
        if before.left == 0:
            around(slot(r, 1 - p), 1 - p, 1)

    def got_other():
        each("o", 1, r, 1 - p)
        go_other()

    net.when([other], got_other)
    around(own, p, 0)


def sum_rows(dst, srcs):
    if len(dst.shape) > 2:
        for i in range(dst.shape[0]):
            sum_rows(dst.at[i], [s.at[i] for s in srcs])
        return
    step = 16

    @pl.loop(0, dst.shape[0] // step)
    def _(i):
        at = pl.ds(pl.multiple_of(i * step, step), step)
        total = dst[at, :]
        for s in srcs:
            total = total + s[at, :]
        dst[at, :] = total


def dot(a, b, ca, cb):
    return lax.dot_general(a, b, (((ca,), (cb,)), ((), ())), preferred_element_type=F32)


def nth(refs, i, n):
    size = refs.shape[0] // n
    return refs.at[pl.ds(i * size, size)]


ORDER = ("2", "+", "-", "o")


class Adder:
    def __init__(self, net, pool, view):
        self.net, self.pool, self.view = net, pool, view

    def add(self, flags, srcs, outs, then):
        net, pool = self.net, self.pool

        def begin(slots):
            refs = [self.view(pool.refs[i], srcs[0].shape) for i in slots]
            loads = [net.copy(src, ref) for src, ref in zip(srcs, refs)]

            def done():
                sum_rows(refs[0], refs[1:])
                net.now += 0.25 * len(refs) * nbytes(refs[0]) / 1.0e6
                for i in slots[1:]:
                    pool.give(i)
                copies = [net.copy(src, dst) for src, dst in outs(refs[0])]
                pool.give(slots[0], copies)
                net.when(copies, then)

            net.when(loads, done)

        net.job(flags, [(pool, len(srcs))], begin, NEXT)


def ring_reduce(net, adder, ready, srcs, l1, l2, links, near):
    come = [Flag(), Flag()]

    def go(name, h, more, flags, link, dst, flag):
        terms = srcs(name, h) + more

        def send():
            got, _ = net.send(link, terms[0], dst)
            net.arrive(got, flag)

        if len(terms) == 1:
            net.job(ready(name, h) + flags, [], send, NEXT)
        else:
            adder.add(ready(name, h) + flags, terms, lambda ref: [(ref, terms[0])], send)

    for h, link in enumerate(links):
        go("2", h, [], [], link, l1.at[h], come[h])
    for k, (link, name) in enumerate(zip(links, "+-")):
        go(name, 1 - k, [], [], link, l2.at[k, 1 - k], near[1 - k])
        go(name, k, [l1.at[k]], [come[k]], link, l2.at[k, k], near[k])


def layer_kernel(
    x_ref, dy_ref, wg_ref, wu_ref, wd_ref,
    y_own, y_l2, r_own, r_lp, q_own, q_l2, g_own, g_lp, u_own, u_lp, v_own, v_l2, d_own, d_l2,
    x_all, dy_all, wd_ext, y_pt, r_pt, q_pt, w_pt, y_l1, r_l1, r_l2, q_lp, q_l1, w_lc,
    g_l1, g_l2, u_l1, u_l2, v_lp, v_l1, d_lp, d_l1,
    wg_all, wu_all, wd_all, h_all, da_all, db_all, h_ext, xb, db, xs, ds, r_out, q_out, y_out, wx, tw, tk, wk,
    local_sems, send_sems, recv_sems,
):
    here = Place()
    here.barrier()
    net = Net(here, local_sems, send_sems, recv_sems)
    z, zp, zm, z2, b = here.z, here.zp, here.zm, here.z2, here.b
    x, xp, xm, x2, a, c = here.x, here.xp, here.xm, here.x2, here.a, here.c
    micro, rows, width = x_ref.shape
    wr, wc = wg_ref.shape
    half_width = width // 2
    edge = width * 5 // 24
    m_blk = micro * rows
    n_blk = 2 * m_blk
    zs = {"o": z, "+": zp, "-": zm, "2": z2}
    xs_of = {"o": x, "+": xp, "-": xm, "2": x2}
    ring_z, ring_x = ("z+", "z-"), ("x+", "x-")

    def rows_at(start, size):
        return pl.ds(pl.multiple_of(start, size), size)

    weights_in = [Flag(24), Flag(24)]
    pieces = [(name, side) for name in zs for side in range(2)]
    tokens_in = {piece: Flag(2 if piece == ("o", 0) else 3) for piece in pieces}
    ext_in = Flag(16)

    def up_slot(ref, core):
        return lambda q, p: ref.at[rows_at((q * 2 + core) * wr, wr), rows_at(p * wc, wc)]

    def down_slot(ref, core):
        return lambda q, p: ref.at[rows_at(p * wc, wc), rows_at((q * 2 + core) * wr, wr)]

    def row_half(ref, h):
        return nth(ref, h, 2)

    def tok_half(ref, h):
        return ref.at[h]

    in_z = (z, zp, zm, z2, b)
    in_x = (x, xp, xm, x2, a)

    def across(mine, theirs):
        def each(name, k, q, p):
            weights_in[k].hit()
            got, _ = net.send("core", mine(q, p), mine(q, p), theirs(q, p))
            net.arrive(got, weights_in[k])
        return each

    for fn, own, mine, theirs in (
        (gather_ring_first, wg_ref, up_slot(wg_all, c), up_slot(wg_all, 1 - c)),
        (functools.partial(gather_pair_first, late=True), wu_ref, up_slot(wu_all, c), up_slot(wu_all, 1 - c)),
        (functools.partial(gather_pair_first, late=True), wd_ref, down_slot(wd_all, c), down_slot(wd_all, 1 - c)),
    ):
        fn(net, own, mine, row_half, ring_x, "wgt", in_x, across(mine, theirs))
        got, _ = net.send("core", own, mine(x, a), theirs(x, a))
        net.arrive(got, weights_in[0])
        net.arrive(net.copy(own, mine(x, a)), weights_in[0])

    ext, ext_side = down_slot(wd_ext, c), down_slot(wd_ext, 1 - c)

    def ext_each(q, p):
        ext_in.hit()
        got, _ = net.send("core", ext(q, p), ext(q, p), ext_side(q, p))
        net.arrive(got, ext_in)

    def ext_round(p):
        from_down, _ = net.send("x+", ext(x, p), ext(x, p), ext(xm, p))
        from_up, _ = net.send("x-", ext(x, p), ext(x, p), ext(xp, p))
        far = []

        def near(q, h, link):
            def then():
                ref = row_half(ext(q, p), h)
                far.append(net.send(link, ref, ref, row_half(ext(x2, p), h))[0])
                ext_each(q, p)
                if len(far) == 2:
                    net.when(far, lambda: ext_each(x2, p))
            return then

        net.when([from_down], near(xm, 0, "x+"))
        net.when([from_up], near(xp, 1, "x-"))
        ext_each(x, p)

    def ext_start():
        got, _ = net.send("tok", wd_ref, ext(x, a))

        def pass_on():
            more, _ = net.send("wgt", ext(x, a), ext(x, a), ext(x, 1 - a))
            net.when([more], lambda: ext_round(1 - a))
            ext_round(a)

        net.when([got], pass_on)

    started = []

    def count_tokens(name, k, q, p):
        tokens_in[name, k].hit()

    def count_main(name, k, q, p):
        count_tokens(name, k, q, p)
        if name == "-" and not started:
            started.append(True)
            ext_start()

    for fn, own, dst, cols, each in (
        (gather_pair_first, x_ref, x_all, pl.ds(width - edge, edge), count_tokens),
        (gather_ring_first, x_ref, x_all, pl.ds(0, width - edge), count_main),
        (gather_pair_first, dy_ref, dy_all, pl.ds(0, width), count_tokens),
    ):
        slot = functools.partial(lambda q, p, dst, cols: dst.at[q, p, :, :, cols], dst=dst, cols=cols)
        fn(net, own.at[:, :, cols], slot, tok_half, ring_z, "tok", in_z, each)

    tok_pool = Pool([(xb.at[i], db.at[i]) for i in range(xb.shape[0])])
    cut_pool = Pool([(xs.at[i], ds.at[i]) for i in range(xs.shape[0])])
    r_pool = Pool([r_out.at[i] for i in range(r_out.shape[0])])
    q_pool = Pool([q_out.at[i] for i in range(q_out.shape[0])])
    y_pool = Pool([y_out.at[i] for i in range(y_out.shape[0])])
    ext_pool = Pool([wx.at[i] for i in range(wx.shape[0])])
    wout_pool = Pool([tw.at[i] for i in range(tw.shape[0])])
    tk_pool = Pool([tk.at[i] for i in range(tk.shape[0])])
    wk_pool = Pool([wk.at[i] for i in range(wk.shape[0])])

    first_slot = tok_pool.take(1)[0]
    bounce = tok_pool.refs[first_slot]
    into = [net.copy(src, ref.at[0]) for src, ref in zip((x_ref, dy_ref), bounce)]

    def own_rows():
        out = [net.copy(ref.at[0], dst.at[z, b]) for ref, dst in zip(bounce, (x_all, dy_all))]
        tok_pool.give(first_slot, out)
        for handle in out:
            net.arrive(handle, tokens_in["o", 0])

    net.when(into, own_rows)

    ranks = {step: 10 + i for i, step in enumerate(STEPS)}

    hidden = {piece: Flag(2) for piece in pieces}
    ext_rows = Flag(4)
    tile_h = min(256, wc)

    def piece_rows(piece):
        name, side = piece
        return rows_at(zs[name] * n_blk + (b if side == 0 else 1 - b) * m_blk, m_blk)

    def hidden_of(key, turn):
        block = BLOCKS[key]
        count = len(block)
        cols_at = a * wc if turn == 0 else (1 - a) * wc
        rank = ranks["H" + key + "ab"[turn]]
        loaded = Flag()
        held = []

        def load(slots):
            i = slots[0]
            held.append(i)
            copies = []
            for n, (name, side) in enumerate(block):
                for ref, src in zip(tok_pool.refs[i], (x_all, dy_all)):
                    copies.append(net.copy(src.at[zs[name], b if side == 0 else 1 - b], ref.at[n]))
            net.when(copies, loaded.hit)

        def multiply():
            i = held[0]
            one, two = tok_pool.refs[i]

            @pl.loop(0, wc // tile_h)
            def _(j):
                cols = rows_at(cols_at + j * tile_h, tile_h)
                x_blk = one[:count].reshape(count * m_blk, width)
                dy_blk = two[:count].reshape(count * m_blk, width)
                pre = dot(x_blk, wg_all[:, cols], 1, 0)
                up = dot(x_blk, wu_all[:, cols], 1, 0)
                g = dot(dy_blk, wd_all[cols, :], 1, 1)
                s = jax.nn.sigmoid(pre)
                act = pre * s
                h = (act * up).astype(BF16)
                da = (g * up * s * (1.0 + pre * (1.0 - s))).astype(BF16)
                db = (g * act).astype(BF16)
                for n, piece in enumerate(block):
                    at = piece_rows(piece)
                    cut = slice(n * m_blk, (n + 1) * m_blk)
                    h_all[at, cols] = h[cut]
                    da_all[at, cols] = da[cut]
                    db_all[at, cols] = db[cut]

            tok_pool.give(i)
            for piece in block:
                hidden[piece].hit()

        net.job([tokens_in[piece] for piece in block], [(tok_pool, 1)], load, rank * EARLY, "load")
        net.job([loaded, weights_in[turn]], [], multiply, rank, "mxu", 1.2 + 0.8 * count)

    def give_hidden(name):
        def go():
            got, _ = net.send("tok", h_all.at[piece_rows((name, 1)), :], h_ext.at[rows_at(zs[name] * m_blk, m_blk), :])
            net.arrive(got, ext_rows)
        net.job([hidden[name, 1]], [], go, NEXT)

    for key in BLOCKS:
        hidden_of(key, 0)
        hidden_of(key, 1)
    for name in zs:
        give_hidden(name)

    r_in = {k: Flag() for k in zs}
    q_in = {k: Flag() for k in zs}
    tile_dx = half_width // 2

    def rows_of(name, pool, part, flag, col0, rank):
        at = rows_at(zs[name] * n_blk, n_blk)

        def multiply(slots):
            i = slots[0]
            ref = pool.refs[i]

            @pl.loop(0, half_width // tile_dx)
            def _(j):
                src = rows_at(col0 + j * tile_dx, tile_dx)
                val = dot(da_all[at, :], wg_all[src, :], 1, 1) + dot(db_all[at, :], wu_all[src, :], 1, 1)
                ref[:, :, :, rows_at(j * tile_dx, tile_dx)] = val.reshape(2, micro, rows, tile_dx)

            done = net.copy(ref, part.at[zs[name]])
            pool.give(i, [done])
            net.when([done], flag.hit)

        net.job([hidden[name, side] for side in SIDES], [(pool, 1)], multiply, rank, "mxu", 2.0)

    for name in zs:
        rows_of(name, r_pool, r_pt, r_in[name], 0, ranks["R" + name])
        rows_of(name, q_pool, q_pt, q_in[name], half_width, ranks["Q" + name])

    quarter = width // 4
    tile_y = quarter // 3 if quarter % 3 == 0 else quarter
    y_in = [Flag(2), Flag(2)]

    def y_of(j):
        loaded = Flag()
        held = []
        cols = pl.ds(j * quarter, quarter)

        def load(slots):
            held.append(slots[0])
            net.when([net.copy(wd_ext.at[:, cols], ext_pool.refs[slots[0]])], loaded.hit)

        def multiply(slots):
            i = slots[0]
            ref = y_pool.refs[i]
            w_ref = ext_pool.refs[held[0]]
            mine = [rows_at(zs[name] * n_blk + b * m_blk, m_blk) for name in ORDER]
            other = [rows_at(zs[name] * m_blk, m_blk) for name in ORDER]

            @pl.loop(0, quarter // tile_y)
            def _(n):
                near = jnp.concatenate([h_all[at, :] for at in mine], axis=0)
                far = jnp.concatenate([h_ext[at, :] for at in other], axis=0)
                at = rows_at(n * tile_y, tile_y)
                val = dot(near, wd_all[:, rows_at(j * quarter + n * tile_y, tile_y)], 1, 0) + dot(far, w_ref[:, at], 1, 0)
                ref[:, :, :, at] = val.reshape(4, micro, rows, tile_y)

            ext_pool.give(held[0])
            half = pl.ds((j % 2) * quarter, quarter)
            out = [net.copy(ref.at[k], y_pt.at[j // 2, k, :, :, half]) for k in range(3)]
            out.append(net.copy(ref.at[3], y_own.at[:, :, cols]))
            y_pool.give(i, out)
            net.when(out, y_in[j // 2].hit)

        net.job([ext_in], [(ext_pool, 1)], load, ranks["Y%d" % j] * EARLY, "ext")
        own = [hidden[name, 0] for name in zs]
        net.job([loaded, ext_rows] + own, [(y_pool, 1)], multiply, ranks["Y%d" % j], "mxu", 2.1)

    for j in range(4):
        y_of(j)

    def tok_view(ref, shape):
        return ref if len(shape) == 3 else ref.at[0]

    tok_add = Adder(net, tk_pool, tok_view)
    names = {name: k for k, name in enumerate(ORDER)}

    r_near = [Flag(2), Flag(2)]
    ring_reduce(
        net, tok_add, lambda name, h: [r_in[name]], lambda name, h: [r_pt.at[zs[name], :, h]],
        r_l1, r_l2, ring_z, r_near,
    )

    def r_last(h):
        away = r_pt.at[z, 1 - b, h]

        def go():
            got, _ = net.send("tok", away, r_lp.at[h])
            net.when([got], nothing)

        tok_add.add(
            [r_in["o"], r_near[h]], [r_pt.at[z, :, h], r_l2.at[0, h], r_l2.at[1, h]],
            lambda ref: [(ref.at[1 - b], away), (ref.at[b], r_own.at[h])], go,
        )

    r_last(0)
    r_last(1)

    for j in range(2):
        ring_reduce(
            net, tok_add, lambda name, h, j=j: [y_in[j]], lambda name, h, j=j: [y_pt.at[j, names[name], h]],
            y_l1.at[j], y_l2.at[j], ring_z, [Flag(2), Flag(2)],
        )

    q_pair = {k: Flag() for k in zs}

    def pair_q(name):
        def go():
            got, _ = net.send("tok", q_pt.at[zs[name], 1 - b], q_lp.at[names[name]])
            net.arrive(got, q_pair[name])
        net.job([q_in[name]], [], go, NEXT)

    for name in ORDER:
        pair_q(name)
    ring_reduce(
        net, tok_add, lambda name, h: [q_in[name], q_pair[name]],
        lambda name, h: [q_pt.at[zs[name], b, h], q_lp.at[names[name], h]], q_l1, q_l2, ring_z, [Flag(2), Flag(2)],
    )
    tok_add.add(
        [q_in["o"], q_pair["o"]], [q_pt.at[z, b], q_lp.at[3]], lambda ref: [(ref, q_own)], nothing,
    )

    tile_w = wc
    n_tok = 4 * n_blk
    w_in = {(m, k): Flag() for m in range(3) for k in range(4)}
    w_side = {(m, k): Flag() for m in range(3) for k in range(4)}
    all_hidden = list(hidden.values())
    mats = range(3)

    def grads_of(k, name, core, turn):
        loaded = Flag()
        held = []
        cols = rows_at((xs_of[name] * 2 + core) * wr, wr)

        def load(slots):
            i = slots[0]
            held.append(i)
            one, two = cut_pool.refs[i]
            net.when([net.copy(x_all.at[:, :, :, :, cols], one), net.copy(dy_all.at[:, :, :, :, cols], two)], loaded.hit)

        def out(m, j, ref):
            if turn == 0:
                got, sent = net.send("core", ref, w_lc.at[m, k])
                wout_pool.give(j, [sent])
                net.arrive(got, w_side[m, k])
                return

            def begin(slots):
                halves = [(nth(ref, h, 2), wk_pool.refs[i]) for h, i in enumerate(slots)]
                loads = [net.copy(nth(w_lc.at[m, k], h, 2), slot) for h, (_, slot) in enumerate(halves)]

                def add():
                    for i, (dst, slot) in zip(slots, halves):
                        sum_rows(dst, [slot])
                        wk_pool.give(i)
                    net.now += 0.8
                    done = net.copy(ref, w_pt.at[m, k])
                    wout_pool.give(j, [done])
                    net.when([done], w_in[m, k].hit)

                net.when(loads, add)

            net.job([w_side[m, k]], [(wk_pool, 2)], begin, FIRST)

        def multiply(which, free):
            def then(slots):
                refs = [wout_pool.refs[j] for j in slots]
                one, two = cut_pool.refs[held[0]]

                @pl.loop(0, 2 * wc // tile_w)
                def _(j):
                    at = rows_at(j * tile_w, tile_w)
                    for m, ref in zip(which, refs):
                        cut = (two if m == 2 else one)[...].reshape(n_tok, wr)
                        ref[:, at] = dot(cut, (da_all, db_all, h_all)[m][:, at], 0, 0)

                if free:
                    cut_pool.give(held[0])
                for m, j, ref in zip(which, slots, refs):
                    out(m, j, ref)
            return then

        flags = [loaded] + all_hidden
        step = "W%d%s" % (k, "ab"[turn])
        first = min(ranks[step + m] for m in "gud") if k == 0 else ranks[step]
        net.job(list(tokens_in.values()), [(cut_pool, 1)], load, first * EARLY, "cut")
        if k == 0:
            last = max(mats, key=lambda m: ranks[step + "gud"[m]])
            for m in range(3):
                net.job(flags, [(wout_pool, 1)], multiply([m], m == last), ranks[step + "gud"[m]], "mxu", 1.15)
        else:
            net.job(flags, [(wout_pool, len(mats))], multiply(mats, True), ranks[step], "mxu", 2.8)

    for k, name in enumerate(ORDER):
        grads_of(k, name, 1 - c, 0)
        grads_of(k, name, c, 1)

    def w_view(ref, shape):
        return ref.at[pl.ds(0, shape[0]), pl.ds(0, shape[1])]

    w_add = Adder(net, wk_pool, w_view)
    mine, other = rows_at(a * wc, wc), rows_at((1 - a) * wc, wc)

    def w_ring_first(m, row0, size, l1, l2, lp, own):
        def part(ref, h):
            return ref.at[pl.ds(row0 + h * (size // 2), size // 2)]

        near = [Flag(2), Flag(2)]
        ring_reduce(
            net, w_add, lambda name, h: [w_in[m, names[name]]],
            lambda name, h: [part(w_pt.at[m, names[name]], h)], l1, l2, ring_x, near,
        )

        def last(h):
            block = part(w_pt.at[m, 3], h)
            away = block.at[:, other]

            def go():
                got, _ = net.send("wgt", away, row_half(lp, h))
                net.when([got], nothing)

            w_add.add(
                [w_in[m, 3], near[h]], [block, l2.at[0, h], l2.at[1, h]],
                lambda ref: [(ref.at[:, other], away), (ref.at[:, mine], row_half(own, h))], go,
            )

        last(0)
        last(1)

    def w_pair_first(m, row0, size, lp, l1, l2, own):
        def part(ref, h):
            return ref.at[pl.ds(row0 + h * (size // 2), size // 2)]

        have = {k: [w_in[m, k]] for k in range(4)}
        pair = {(k, h): Flag() for k in range(4) for h in range(2)}

        def away(k, h):
            def go():
                got, _ = net.send("wgt", part(w_pt.at[m, k], h).at[:, other], row_half(lp.at[k], h))
                net.arrive(got, pair[k, h])

            net.job(have[k], [], go, NEXT)

        for k in range(4):
            for h in range(2):
                away(k, h)

        def terms(name, h):
            k = names[name]
            return [part(w_pt.at[m, k], h).at[:, mine], row_half(lp.at[k], h)]

        def ready(name, h):
            return have[names[name]] + [pair[names[name], h]]

        ring_reduce(net, w_add, ready, terms, l1, l2, ring_x, [Flag(2), Flag(2)])
        for h in range(2):
            w_add.add(ready("o", h), terms("o", h), lambda ref, h=h: [(ref, row_half(own, h))], nothing)

    most = wr * 2 // 3
    w_ring_first(0, 0, wr, g_l1, g_l2, g_lp, g_own)
    w_pair_first(2, 0, wr, d_lp, d_l1, d_l2, d_own)
    w_ring_first(1, 0, most, u_l1, u_l2, u_lp, u_own)
    w_pair_first(1, most, wr - most, v_lp, v_l1, v_l2, v_own)
    net.run()


def finish_kernel(
    x_ref, dy_ref, y_own, y_l2, r_own, r_lp, q_own, q_l2, g_own, g_lp, u_own, u_lp, v_own, v_l2, d_own, d_l2,
    y_ref, dx_ref, g_ref, u_ref, d_ref,
):
    i = pl.program_id(0)
    half = r_own.shape[-1]
    for j in range(2):
        cols = pl.ds(j * half, half)
        total = y_own[:, :, cols] + y_l2[j, 0] + y_l2[j, 1]
        y_ref[:, :, cols] = (x_ref[:, :, cols].astype(F32) + total).astype(BF16)
    low, high = pl.ds(0, half), pl.ds(half, half)
    dx_ref[:, :, low] = (dy_ref[:, :, low].astype(F32) + (r_own[...] + r_lp[...])).astype(BF16)
    dx_ref[:, :, high] = (dy_ref[:, :, high].astype(F32) + (q_own[...] + q_l2[0] + q_l2[1])).astype(BF16)
    g_ref[...] = g_own[...] + g_lp[...]
    most, size, rest = u_own.shape[0] * pl.num_programs(0), u_own.shape[0], v_own.shape[0]
    u_ref[pl.ds(pl.multiple_of(i * size, size), size), :] = u_own[...] + u_lp[...]
    u_ref[pl.ds(pl.multiple_of(4 * size + i * rest, rest), rest), :] = v_own[...] + v_l2[0, 0] + v_l2[1, 0]
    rows, cols = d_own.shape
    total = d_own[...] + d_l2[0].reshape(rows, cols) + d_l2[1].reshape(rows, cols)
    d_ref[...] = total.T


def finish(x, dy, y_own, y_l2, r_own, r_lp, q_own, q_l2, g_own, g_lp, u_own, u_lp, v_own, v_l2, d_own, d_l2):
    micro, rows, width = x.shape
    wr, wc = g_own.shape
    half = width // 2
    n = 4
    B = pl.BlockSpec
    S = jax.ShapeDtypeStruct

    def tok(cols):
        return B((micro, rows // n, cols), lambda i: (0, i, 0))

    def flat(rows, cols):
        return B((rows // n, cols), lambda i: (i, 0))

    most, rest = u_own.shape[0], v_own.shape[0]
    return pl.pallas_call(
        finish_kernel,
        name="finish",
        grid=(n,),
        out_shape=(S(x.shape, BF16), S(x.shape, BF16), S((wr, wc), F32), S((wr, wc), F32), S((wc, wr), F32)),
        in_specs=[
            tok(width), tok(width), tok(width), B((2, 2, micro, rows // n, half), lambda i: (0, 0, 0, i, 0)),
            tok(half), tok(half), tok(half), B((2, micro, rows // n, half), lambda i: (0, 0, i, 0)),
            flat(wr, wc), flat(wr, wc), flat(most, wc), flat(most, wc),
            flat(rest, wc), B((2, 1, rest // n, wc), lambda i: (0, i // 2, i % 2, 0)),
            B((wr, wc // n), lambda i: (0, i)), B((2, 2, wr // 2, wc // n), lambda i: (0, 0, 0, i)),
        ],
        out_specs=[tok(width), tok(width), flat(wr, wc), B((wr, wc), lambda i: (0, 0)), B((wc // n, wr), lambda i: (i, 0))],
        compiler_params=pltpu.CompilerParams(vmem_limit_bytes=60 * 2**20),
    )(x, dy, y_own, y_l2, r_own, r_lp, q_own, q_l2, g_own, g_lp, u_own, u_lp, v_own, v_l2, d_own, d_l2)


def solution(mesh):
    row_spec = P(None, ("dp", "tp"), None)
    in_specs = (row_spec, P("dp", "tp"), P("dp", "tp"), P("tp", "dp"), row_spec)
    out_specs = (row_spec, row_spec, P("dp", "tp"), P("dp", "tp"), P("tp", "dp"))
    hbm = pl.BlockSpec(memory_space=pl.ANY)
    dma = pltpu.SemaphoreType.DMA
    V = pltpu.VMEM
    S = jax.ShapeDtypeStruct

    def local_step(x_loc, wg, wu, wd, dy_loc):
        micro, rows, width = x_loc.shape
        wr, wc = wg.shape
        fw = 2 * wc
        half = width // 2
        most = wr * 2 // 3
        tok = (micro, rows, width)
        tok_h = (micro, rows, half)
        n = 8 * micro * rows

        def ring_first(size):
            return S((2, size // 2, fw), F32), S((2, 2, size // 2, fw), F32)

        def pair_first(size):
            return S((4, size, wc), F32), S((2, size // 2, wc), F32)

        def pair_last(size):
            return S((size, wc), F32), S((2, 2, size // 2, wc), F32)

        outs = [
            S(tok, F32), S((2, 2) + tok_h, F32), S(tok_h, F32), S(tok_h, F32), S(tok_h, F32), S((2,) + tok_h, F32),
            S((wr, wc), F32), S((wr, wc), F32), S((most, wc), F32), S((most, wc), F32),
            *pair_last(wr - most), *pair_last(wr),
        ]
        space = [
            S((4, 2) + tok, BF16), S((4, 2) + tok, BF16), S((fw, width), BF16),
            S((2, 3) + tok_h, F32), S((4, 2) + tok_h, F32), S((4, 2) + tok_h, F32), S((3, 4, wr, fw), F32),
            S((2, 2) + tok_h[1:], F32), S((2, 2) + tok_h[1:], F32), S((2, 2, 2) + tok_h[1:], F32),
            S((4,) + tok_h, F32), S((2,) + tok_h[1:], F32), S((3, 4, wr, fw), F32),
            *ring_first(wr), *ring_first(most), *pair_first(wr - most), *pair_first(wr),
        ]
        res = pl.pallas_call(
            layer_kernel,
            name="layer",
            out_shape=tuple(outs + space),
            in_specs=[hbm] * 5,
            out_specs=[hbm] * (len(outs) + len(space)),
            scratch_shapes=[
                V((width, fw), BF16), V((width, fw), BF16), V((fw, width), BF16),
                V((n, fw), BF16), V((n, fw), BF16), V((n, fw), BF16), V((n // 2, fw), BF16),
                V((2, 2) + tok, BF16), V((2, 2) + tok, BF16),
                V((2, 4, 2, micro, rows, wr), BF16), V((2, 4, 2, micro, rows, wr), BF16),
                V((1, 2) + tok_h, F32), V((2, 2) + tok_h, F32),
                V((2, 4, micro, rows, width // 4), F32), V((2, fw, width // 4), BF16), V((6, wr, fw), F32),
                V((5, 2, rows, half), F32), V((6, wr // 2, fw), F32),
                dma((128,)), dma((200,)), dma((200,)),
            ],
            compiler_params=pltpu.CompilerParams(
                collective_id=0, has_side_effects=True, vmem_limit_bytes=67_000_000
            ),
        )(x_loc, dy_loc, wg, wu, wd)
        return finish(x_loc, dy_loc, *res[: len(outs)])

    return jax.shard_map(local_step, mesh=mesh, in_specs=in_specs, out_specs=out_specs, check_vma=False)
```

```python
import functools
import heapq

import jax
import jax.numpy as jnp
from jax import lax
from jax.experimental import pallas as pl
from jax.experimental.pallas import tpu as pltpu
from jax.sharding import PartitionSpec as P

MESH = pl.DeviceIdType.MESH
F32 = jnp.float32
BF16 = jnp.bfloat16
ICI_RATE = 45.0e3
CORE_RATE = 550.0e3
HBM_RATE = 2.5e6
MARGIN = 0.3
FIRST, NEXT, EARLY = 0.5, 1, 0.01
SIDES = (0, 1)
TW, TR, TK, WK = 6, 3, 4, 6
RING = 4
AROUND = (1, 3, 2)
BLOCKS = {
    "A": (("o", 0), ("o", 1)), "B": (("-", 0), ("+", 0)), "C": (("-", 1), ("+", 1)), "D": (("2", 0),), "E": (("2", 1),),
}
STEPS = (
    "HBa", "HAa", "HBb", "HAb", "HDb", "HCb", "HDa", "HCa", "HEb", "HEa",
    "W0au", "W0ad", "W0bu", "R2", "W0bd", "R+", "W0ag", "W0bg", "W1a", "Q+",
    "R-", "Y1", "W1b", "W2a", "Q2", "Y0", "Q-", "W2b", "Ro", "Y2",
    "Qo", "Y3", "W3b", "W3a",
)


def nbytes(ref):
    size = jnp.dtype(ref.dtype).itemsize
    for n in ref.shape:
        size *= n
    return size


class Place:
    def __init__(self):
        t = lax.axis_index("tp")
        d = lax.axis_index("dp")
        z, y, x, c = t // RING, t % RING, d // 2, d % 2
        self.z, self.y, self.x, self.c = z, y, x, c
        self.b = y % 2
        self.a = y // 2
        self.zp, self.zm, self.z2 = ((z + n) % RING for n in AROUND)
        self.xp, self.xm, self.x2 = ((x + n) % RING for n in AROUND)

        def at(z, y, x, c):
            return {"tp": z * RING + y, "dp": x * 2 + c}

        self.dev = {
            "z+": at(self.zp, y, x, c),
            "z-": at(self.zm, y, x, c),
            "x+": at(z, y, self.xp, c),
            "x-": at(z, y, self.xm, c),
            "tok": at(z, y + 1 - 2 * self.b, x, c),
            "wgt": at(z, 3 - y, x, c),
            "core": at(z, y, x, 1 - c),
        }

    def barrier(self):
        sem = pltpu.get_barrier_semaphore()
        for dev in self.dev.values():
            pl.semaphore_signal(sem, inc=1, device_id=dev, device_id_type=MESH)
        pl.semaphore_wait(sem, len(self.dev))


class Handle:
    def __init__(self, time, wait, after=None):
        self.time, self._wait, self.after, self.done = time, wait, after, False

    def wait(self):
        if not self.done:
            self.done = True
            self._wait()
            if self.after is not None:
                self.after()


class Flag:
    def __init__(self, count=1):
        self.left = count

    def hit(self):
        self.left -= 1


class Pool:
    def __init__(self, refs):
        self.refs = refs
        self.back = [[] for _ in refs]
        self.free = [True] * len(refs)

    def when_ready(self, count):
        times = sorted(max((h.time for h in self.back[i]), default=0.0) for i in range(len(self.refs)) if self.free[i])
        return times[count - 1] if len(times) >= count else float("inf")

    def take(self, count):
        order = sorted(
            (max((h.time for h in self.back[i]), default=0.0), i) for i in range(len(self.refs)) if self.free[i]
        )
        got = [i for _, i in order[:count]]
        for i in got:
            for h in self.back[i]:
                h.wait()
            self.back[i] = []
            self.free[i] = False
        return got

    def give(self, i, handles=()):
        self.free[i] = True
        self.back[i] = list(handles)


class Net:
    def __init__(self, place, local_sems, send_sems, recv_sems):
        self.place, self.local_sems, self.send_sems, self.recv_sems = place, local_sems, send_sems, recv_sems
        self.used = 0
        self.local_used = 0
        self.local_free = []
        self.open = []
        self.heap = []
        self.jobs = []
        self.seq = 0
        self.now = 0.0
        self.free = {}
        self.log = []

    def send(self, link, src, dst, land=None):
        land = dst if land is None else land
        i = self.used
        self.used += 1
        dev = self.place.dev[link]

        def copy_of(a, b):
            return pltpu.make_async_remote_copy(
                src_ref=a, dst_ref=b, send_sem=self.send_sems.at[i], recv_sem=self.recv_sems.at[i],
                device_id=dev, device_id_type=MESH,
            )

        copy = copy_of(src, dst)
        copy.start()
        arrive = copy_of(land, land)
        rate = CORE_RATE if link == "core" else ICI_RATE
        end = max(self.now, self.free.get(link, 0.0)) + nbytes(land) / rate
        self.free[link] = end
        sent = Handle(end + 0.5, copy.wait_send)
        self.open.append(sent)
        return Handle(end + 2.0, arrive.wait_recv), sent

    def copy(self, src, dst):
        if self.local_free:
            i = self.local_free.pop(0)
        else:
            i = self.local_used
            self.local_used += 1
        copy = pltpu.make_async_copy(src, dst, self.local_sems.at[i])
        copy.start()
        end = max(self.now, self.free.get("hbm", 0.0)) + nbytes(src) / HBM_RATE
        self.free["hbm"] = end
        handle = Handle(end + 0.8, copy.wait, lambda: self.local_free.append(i))
        self.open.append(handle)
        return handle

    def when(self, handles, then):
        self.seq += 1
        heapq.heappush(self.heap, (max(h.time for h in handles), self.seq, handles, then))

    def job(self, flags, needs, then, rank, line=None, cost=0.1):
        self.seq += 1
        self.jobs.append((rank, self.seq, flags, needs, then, cost, line))
        self.jobs.sort(key=lambda j: j[:2])

    def run(self):
        while True:
            if self.heap and self.heap[0][0] + MARGIN <= self.now:
                self.event()
                continue
            chosen = None
            soonest = float("inf")
            held = set()
            for j in self.jobs:
                if j[6] is not None:
                    if j[6] in held:
                        continue
                    held.add(j[6])
                if any(f.left > 0 for f in j[2]):
                    continue
                ready = max((pool.when_ready(n) for pool, n in j[3]), default=0.0)
                if ready <= self.now:
                    chosen = j
                    break
                soonest = min(soonest, ready)
            if chosen is not None:
                self.jobs.remove(chosen)
                _, _, _, needs, then, cost, _ = chosen
                slots = [pool.take(n) for pool, n in needs]
                self.now += cost
                then(*slots)
                continue
            if self.heap and self.heap[0][0] <= soonest:
                self.event()
            elif soonest < float("inf"):
                self.now = max(self.now, soonest)
            else:
                break
        assert not self.jobs, "jobs left"
        for handle in self.open:
            handle.wait()

    def event(self):
        time, _, handles, then = heapq.heappop(self.heap)
        self.now = max(self.now, time)
        for h in handles:
            h.wait()
        then()

    def arrive(self, handle, flag):
        self.when([handle], flag.hit)


def nothing():
    pass


def gather_ring_first(net, own, slot, half, ring, pair, me, each):
    r, rp, rm, r2, p = me
    up, down = ring
    from_down, _ = net.send(up, own, slot(r, p), slot(rm, p))
    from_up, _ = net.send(down, own, slot(r, p), slot(rp, p))
    other, _ = net.send(pair, own, slot(r, p), slot(r, 1 - p))
    net.when([other], lambda: each("o", 1, r, 1 - p))

    def pass_on(name, q):
        got, _ = net.send(pair, slot(q, p), slot(q, p), slot(q, 1 - p))
        net.when([got], lambda: each(name, 1, q, 1 - p))

    far = []

    def got_near(name, q, h, link):
        def then():
            ref = half(slot(q, p), h)
            far.append(net.send(link, ref, ref, half(slot(r2, p), h))[0])
            pass_on(name, q)
            each(name, 0, q, p)
            if len(far) == 2:
                net.when(far, got_far)
        return then

    def got_far():
        pass_on("2", r2)
        each("2", 0, r2, p)

    net.when([from_down], got_near("-", rm, 0, up))
    net.when([from_up], got_near("+", rp, 1, down))


def gather_pair_first(net, own, slot, half, ring, pair, me, each, late=False):
    r, rp, rm, r2, p = me
    up, down = ring

    def around(src, q, k):
        from_down, _ = net.send(up, src, slot(r, q), slot(rm, q))
        from_up, _ = net.send(down, src, slot(r, q), slot(rp, q))
        far = []

        def got_near(name, s, h, link):
            def then():
                ref = half(slot(s, q), h)
                far.append(net.send(link, ref, ref, half(slot(r2, q), h))[0])
                each(name, k, s, q)
                if k == 0 and late:
                    go_other()
                if len(far) == 2:
                    net.when(far, lambda: each("2", k, r2, q))
            return then

        net.when([from_down], got_near("-", rm, 0, up))
        net.when([from_up], got_near("+", rp, 1, down))

    other, _ = net.send(pair, own, slot(r, p), slot(r, 1 - p))
    before = Flag(3 if late else 1)

    def go_other():
        before.hit()
        if before.left == 0:
            around(slot(r, 1 - p), 1 - p, 1)

    def got_other():
        each("o", 1, r, 1 - p)
        go_other()

    net.when([other], got_other)
    around(own, p, 0)


def sum_rows(dst, srcs):
    if len(dst.shape) > 2:
        for i in range(dst.shape[0]):
            sum_rows(dst.at[i], [s.at[i] for s in srcs])
        return
    step = 16

    @pl.loop(0, dst.shape[0] // step)
    def _(i):
        at = pl.ds(pl.multiple_of(i * step, step), step)
        total = dst[at, :]
        for s in srcs:
            total = total + s[at, :]
        dst[at, :] = total


def dot(a, b, ca, cb):
    return lax.dot_general(a, b, (((ca,), (cb,)), ((), ())), preferred_element_type=F32)


def nth(refs, i, n):
    size = refs.shape[0] // n
    return refs.at[pl.ds(i * size, size)]


ORDER = ("2", "+", "-", "o")


class Adder:
    def __init__(self, net, pool, view):
        self.net, self.pool, self.view = net, pool, view

    def add(self, flags, srcs, outs, then):
        net, pool = self.net, self.pool

        def begin(slots):
            refs = [self.view(pool.refs[i], srcs[0].shape) for i in slots]
            loads = [net.copy(src, ref) for src, ref in zip(srcs, refs)]

            def done():
                sum_rows(refs[0], refs[1:])
                net.now += 0.25 * len(refs) * nbytes(refs[0]) / 1.0e6
                for i in slots[1:]:
                    pool.give(i)
                copies = [net.copy(src, dst) for src, dst in outs(refs[0])]
                pool.give(slots[0], copies)
                net.when(copies, then)

            net.when(loads, done)

        net.job(flags, [(pool, len(srcs))], begin, NEXT)


def ring_reduce(net, adder, ready, srcs, l1, l2, links, near):
    come = [Flag(), Flag()]

    def go(name, h, more, flags, link, dst, flag):
        terms = srcs(name, h) + more

        def send():
            got, _ = net.send(link, terms[0], dst)
            net.arrive(got, flag)

        if len(terms) == 1:
            net.job(ready(name, h) + flags, [], send, NEXT)
        else:
            adder.add(ready(name, h) + flags, terms, lambda ref: [(ref, terms[0])], send)

    for h, link in enumerate(links):
        go("2", h, [], [], link, l1.at[h], come[h])
    for k, (link, name) in enumerate(zip(links, "+-")):
        go(name, 1 - k, [], [], link, l2(k, 1 - k), near[1 - k][1])
        go(name, k, [l1.at[k]], [come[k]], link, l2(k, k), near[k][0])


def layer_kernel(
    x_ref, dy_ref, wg_ref, wu_ref, wd_ref,
    y_own, y_late, r_own, r_lp, q_own, q_late, g_own, g_lp, u_own, u_lp, v_own, v_late, d_own, d_late,
    x_all, dy_all, wd_ext, y_pt, y_mine, r_pt, q_pt, w_pt, y_l1, y_soon, r_l1, r_l2, q_lp, q_l1, q_soon, w_lc,
    g_l1, g_l2, u_l1, u_l2, v_lp, v_l1, v_soon, d_lp, d_l1, d_soon,
    wg_all, wu_all, wd_all, h_all, da_all, db_all, h_ext, xb, db, xs, ds, r_out, q_out, y_out, wx, tw, tr, tk, wk,
    local_sems, send_sems, recv_sems,
):
    here = Place()
    here.barrier()
    net = Net(here, local_sems, send_sems, recv_sems)
    z, zp, zm, z2, b = here.z, here.zp, here.zm, here.z2, here.b
    x, xp, xm, x2, a, c = here.x, here.xp, here.xm, here.x2, here.a, here.c
    micro, rows, width = x_ref.shape
    wr, wc = wg_ref.shape
    r_cols = width // 3
    q_cols = width - r_cols
    edge = width * 5 // 24
    m_blk = micro * rows
    n_blk = 2 * m_blk
    zs = {"o": z, "+": zp, "-": zm, "2": z2}
    xs_of = {"o": x, "+": xp, "-": xm, "2": x2}
    ring_z, ring_x = ("z+", "z-"), ("x+", "x-")

    def rows_at(start, size):
        return pl.ds(pl.multiple_of(start, size), size)

    weights_in = [Flag(24), Flag(24)]
    pieces = [(name, side) for name in zs for side in range(2)]
    tokens_in = {piece: Flag(2 if piece == ("o", 0) else 3) for piece in pieces}
    ext_in = Flag(16)

    def up_slot(ref, core):
        return lambda q, p: ref.at[rows_at((q * 2 + core) * wr, wr), rows_at(p * wc, wc)]

    def down_slot(ref, core):
        return lambda q, p: ref.at[rows_at(p * wc, wc), rows_at((q * 2 + core) * wr, wr)]

    def row_half(ref, h):
        return nth(ref, h, 2)

    def tok_half(ref, h):
        return ref.at[h]

    in_z = (z, zp, zm, z2, b)
    in_x = (x, xp, xm, x2, a)

    def across(mine, theirs):
        def each(name, k, q, p):
            weights_in[k].hit()
            got, _ = net.send("core", mine(q, p), mine(q, p), theirs(q, p))
            net.arrive(got, weights_in[k])
        return each

    for fn, own, mine, theirs in (
        (gather_ring_first, wg_ref, up_slot(wg_all, c), up_slot(wg_all, 1 - c)),
        (functools.partial(gather_pair_first, late=True), wu_ref, up_slot(wu_all, c), up_slot(wu_all, 1 - c)),
        (functools.partial(gather_pair_first, late=True), wd_ref, down_slot(wd_all, c), down_slot(wd_all, 1 - c)),
    ):
        fn(net, own, mine, row_half, ring_x, "wgt", in_x, across(mine, theirs))
        got, _ = net.send("core", own, mine(x, a), theirs(x, a))
        net.arrive(got, weights_in[0])
        net.arrive(net.copy(own, mine(x, a)), weights_in[0])

    ext, ext_side = down_slot(wd_ext, c), down_slot(wd_ext, 1 - c)

    def ext_each(q, p):
        ext_in.hit()
        got, _ = net.send("core", ext(q, p), ext(q, p), ext_side(q, p))
        net.arrive(got, ext_in)

    def ext_round(p):
        from_down, _ = net.send("x+", ext(x, p), ext(x, p), ext(xm, p))
        from_up, _ = net.send("x-", ext(x, p), ext(x, p), ext(xp, p))
        far = []

        def near(q, h, link):
            def then():
                ref = row_half(ext(q, p), h)
                far.append(net.send(link, ref, ref, row_half(ext(x2, p), h))[0])
                ext_each(q, p)
                if len(far) == 2:
                    net.when(far, lambda: ext_each(x2, p))
            return then

        net.when([from_down], near(xm, 0, "x+"))
        net.when([from_up], near(xp, 1, "x-"))
        ext_each(x, p)

    def ext_start():
        got, _ = net.send("tok", wd_ref, ext(x, a))

        def pass_on():
            more, _ = net.send("wgt", ext(x, a), ext(x, a), ext(x, 1 - a))
            net.when([more], lambda: ext_round(1 - a))
            ext_round(a)

        net.when([got], pass_on)

    started = []

    def count_tokens(name, k, q, p):
        tokens_in[name, k].hit()

    def count_main(name, k, q, p):
        count_tokens(name, k, q, p)
        if name == "-" and not started:
            started.append(True)
            ext_start()

    for fn, own, dst, cols, each in (
        (gather_pair_first, x_ref, x_all, pl.ds(width - edge, edge), count_tokens),
        (gather_ring_first, x_ref, x_all, pl.ds(0, width - edge), count_main),
        (gather_pair_first, dy_ref, dy_all, pl.ds(0, width), count_tokens),
    ):
        slot = functools.partial(lambda q, p, dst, cols: dst.at[q, p, :, :, cols], dst=dst, cols=cols)
        fn(net, own.at[:, :, cols], slot, tok_half, ring_z, "tok", in_z, each)

    tok_pool = Pool([(xb.at[i], db.at[i]) for i in range(xb.shape[0])])
    cut_pool = Pool([(xs.at[i], ds.at[i]) for i in range(xs.shape[0])])
    r_pool = Pool([r_out.at[i] for i in range(r_out.shape[0])])
    q_pool = Pool([q_out.at[i] for i in range(q_out.shape[0])])
    y_pool = Pool([y_out.at[i] for i in range(y_out.shape[0])])
    ext_pool = Pool([wx.at[i] for i in range(wx.shape[0])])
    wout_pool = Pool([tw.at[i] for i in range(tw.shape[0])])
    pair_pool = Pool([tr.at[i] for i in range(tr.shape[0])])
    row_pool = Pool([tk.at[i] for i in range(tk.shape[0])])
    wk_pool = Pool([wk.at[i] for i in range(wk.shape[0])])

    first_slot = tok_pool.take(1)[0]
    bounce = tok_pool.refs[first_slot]
    into = [net.copy(src, ref.at[0]) for src, ref in zip((x_ref, dy_ref), bounce)]

    def own_rows():
        out = [net.copy(ref.at[0], dst.at[z, b]) for ref, dst in zip(bounce, (x_all, dy_all))]
        tok_pool.give(first_slot, out)
        for handle in out:
            net.arrive(handle, tokens_in["o", 0])

    net.when(into, own_rows)

    ranks = {step: 10 + i for i, step in enumerate(STEPS)}

    hidden = {piece: Flag(2) for piece in pieces}
    ext_rows = Flag(4)
    tile_h = min(256, wc)

    def piece_rows(piece):
        name, side = piece
        return rows_at(zs[name] * n_blk + (b if side == 0 else 1 - b) * m_blk, m_blk)

    def hidden_of(key, turn):
        block = BLOCKS[key]
        count = len(block)
        cols_at = a * wc if turn == 0 else (1 - a) * wc
        rank = ranks["H" + key + "ab"[turn]]
        loaded = Flag()
        held = []

        def load(slots):
            i = slots[0]
            held.append(i)
            copies = []
            for n, (name, side) in enumerate(block):
                for ref, src in zip(tok_pool.refs[i], (x_all, dy_all)):
                    copies.append(net.copy(src.at[zs[name], b if side == 0 else 1 - b], ref.at[n]))
            net.when(copies, loaded.hit)

        def multiply():
            i = held[0]
            one, two = tok_pool.refs[i]

            @pl.loop(0, wc // tile_h)
            def _(j):
                cols = rows_at(cols_at + j * tile_h, tile_h)
                x_blk = one[:count].reshape(count * m_blk, width)
                dy_blk = two[:count].reshape(count * m_blk, width)
                pre = dot(x_blk, wg_all[:, cols], 1, 0)
                up = dot(x_blk, wu_all[:, cols], 1, 0)
                g = dot(dy_blk, wd_all[cols, :], 1, 1)
                s = jax.nn.sigmoid(pre)
                act = pre * s
                h = (act * up).astype(BF16)
                da = (g * up * s * (1.0 + pre * (1.0 - s))).astype(BF16)
                db = (g * act).astype(BF16)
                for n, piece in enumerate(block):
                    at = piece_rows(piece)
                    cut = slice(n * m_blk, (n + 1) * m_blk)
                    h_all[at, cols] = h[cut]
                    da_all[at, cols] = da[cut]
                    db_all[at, cols] = db[cut]

            tok_pool.give(i)
            for piece in block:
                hidden[piece].hit()

        net.job([tokens_in[piece] for piece in block], [(tok_pool, 1)], load, rank * EARLY, "load")
        net.job([loaded, weights_in[turn]], [], multiply, rank, "mxu", 1.3 + 0.85 * count)

    def give_hidden(name):
        def go():
            got, _ = net.send("tok", h_all.at[piece_rows((name, 1)), :], h_ext.at[rows_at(zs[name] * m_blk, m_blk), :])
            net.arrive(got, ext_rows)
        net.job([hidden[name, 1]], [], go, NEXT)

    for key in BLOCKS:
        hidden_of(key, 0)
        hidden_of(key, 1)
    for name in zs:
        give_hidden(name)

    r_in = {k: Flag() for k in zs}
    q_in = {k: Flag() for k in zs}
    tile_dx = r_cols

    def rows_of(name, pool, part, flag, col0, cols, rank):
        at = rows_at(zs[name] * n_blk, n_blk)

        def multiply(slots):
            i = slots[0]
            ref = pool.refs[i]

            @pl.loop(0, cols // tile_dx)
            def _(j):
                src = rows_at(col0 + j * tile_dx, tile_dx)
                val = dot(da_all[at, :], wg_all[src, :], 1, 1) + dot(db_all[at, :], wu_all[src, :], 1, 1)
                ref[:, :, :, rows_at(j * tile_dx, tile_dx)] = val.reshape(2, micro, rows, tile_dx)

            done = net.copy(ref, part.at[zs[name]])
            pool.give(i, [done])
            net.when([done], flag.hit)

        net.job([hidden[name, side] for side in SIDES], [(pool, 1)], multiply, rank, "mxu", 1.4 * cols // tile_dx)

    for name in zs:
        rows_of(name, r_pool, r_pt, r_in[name], 0, r_cols, ranks["R" + name])
        rows_of(name, q_pool, q_pt, q_in[name], r_cols, q_cols, ranks["Q" + name])

    quarter = width // 4
    tile_y = quarter // 3 if quarter % 3 == 0 else quarter
    y_in = [Flag(2), Flag(2)]

    def y_of(j):
        loaded = Flag()
        held = []
        cols = pl.ds(j * quarter, quarter)

        def load(slots):
            held.append(slots[0])
            net.when([net.copy(wd_ext.at[:, cols], ext_pool.refs[slots[0]])], loaded.hit)

        def multiply(slots):
            i = slots[0]
            ref = y_pool.refs[i]
            w_ref = ext_pool.refs[held[0]]
            mine = [rows_at(zs[name] * n_blk + b * m_blk, m_blk) for name in ORDER]
            other = [rows_at(zs[name] * m_blk, m_blk) for name in ORDER]

            @pl.loop(0, quarter // tile_y)
            def _(n):
                near = jnp.concatenate([h_all[at, :] for at in mine], axis=0)
                far = jnp.concatenate([h_ext[at, :] for at in other], axis=0)
                at = rows_at(n * tile_y, tile_y)
                val = dot(near, wd_all[:, rows_at(j * quarter + n * tile_y, tile_y)], 1, 0) + dot(far, w_ref[:, at], 1, 0)
                ref[:, :, :, at] = val.reshape(4, micro, rows, tile_y)

            ext_pool.give(held[0])
            half = pl.ds((j % 2) * quarter, quarter)
            out = [net.copy(ref.at[k], y_pt.at[j // 2, k, :, :, half]) for k in range(3)]
            out.append(net.copy(ref.at[3], y_mine.at[j // 2, :, :, half]))
            y_pool.give(i, out)
            net.when(out, y_in[j // 2].hit)

        net.job([ext_in], [(ext_pool, 1)], load, ranks["Y%d" % j] * EARLY, "ext")
        own = [hidden[name, 0] for name in zs]
        net.job([loaded, ext_rows] + own, [(y_pool, 1)], multiply, ranks["Y%d" % j], "mxu", 2.3)

    for j in range(4):
        y_of(j)

    pair_add = Adder(net, pair_pool, lambda ref, shape: ref)
    row_add = Adder(net, row_pool, lambda ref, shape: ref.at[:, pl.ds(0, shape[-1])])
    names = {name: k for k, name in enumerate(ORDER)}

    r_near = [[Flag(), Flag()] for _ in SIDES]
    ring_reduce(
        net, pair_add, lambda name, h: [r_in[name]], lambda name, h: [r_pt.at[zs[name], :, h]],
        r_l1, lambda k, h: r_l2.at[k, h], ring_z, r_near,
    )

    def r_last(h):
        away = r_pt.at[z, 1 - b, h]

        def go():
            got, _ = net.send("tok", away, r_lp.at[h])
            net.when([got], nothing)

        pair_add.add(
            [r_in["o"], *r_near[h]], [r_pt.at[z, :, h], r_l2.at[0, h], r_l2.at[1, h]],
            lambda ref: [(ref.at[1 - b], away), (ref.at[b], r_own.at[h])], go,
        )

    r_last(0)
    r_last(1)

    for j in range(2):
        y_near = [[Flag(), Flag()] for _ in SIDES]
        ring_reduce(
            net, row_add, lambda name, h, j=j: [y_in[j]], lambda name, h, j=j: [y_pt.at[j, names[name], h]],
            y_l1.at[j], lambda k, h, j=j: (y_late if k == h else y_soon).at[j, h], ring_z, y_near,
        )
        for h in SIDES:
            row_add.add(
                [y_in[j], y_near[h][1]], [y_mine.at[j, h], y_soon.at[j, h]],
                lambda ref, j=j, h=h: [(ref, y_own.at[j, h])], nothing,
            )

    q_pair = {k: Flag() for k in zs}

    def pair_q(name):
        def go():
            got, _ = net.send("tok", q_pt.at[zs[name], 1 - b], q_lp.at[names[name]])
            net.arrive(got, q_pair[name])
        net.job([q_in[name]], [], go, NEXT)

    for name in ORDER:
        pair_q(name)
    q_near = [[Flag(), Flag()] for _ in SIDES]
    ring_reduce(
        net, row_add, lambda name, h: [q_in[name], q_pair[name]],
        lambda name, h: [q_pt.at[zs[name], b, h], q_lp.at[names[name], h]],
        q_l1, lambda k, h: (q_late if k == h else q_soon).at[h], ring_z, q_near,
    )
    for h in SIDES:
        row_add.add(
            [q_in["o"], q_pair["o"], q_near[h][1]], [q_pt.at[z, b, h], q_lp.at[3, h], q_soon.at[h]],
            lambda ref, h=h: [(ref, q_own.at[h])], nothing,
        )

    tile_w = wc
    n_tok = 4 * n_blk
    w_in = {(m, k): Flag() for m in range(3) for k in range(4)}
    w_side = {(m, k): Flag() for m in range(3) for k in range(4)}
    all_hidden = list(hidden.values())
    mats = range(3)

    def grads_of(k, name, core, turn):
        loaded = Flag()
        held = []
        cols = rows_at((xs_of[name] * 2 + core) * wr, wr)

        def load(slots):
            i = slots[0]
            held.append(i)
            one, two = cut_pool.refs[i]
            net.when([net.copy(x_all.at[:, :, :, :, cols], one), net.copy(dy_all.at[:, :, :, :, cols], two)], loaded.hit)

        def out(m, j, ref):
            if turn == 0:
                got, sent = net.send("core", ref, w_lc.at[m, k])
                wout_pool.give(j, [sent])
                net.arrive(got, w_side[m, k])
                return

            def begin(slots):
                halves = [(nth(ref, h, 2), wk_pool.refs[i]) for h, i in enumerate(slots)]
                loads = [net.copy(nth(w_lc.at[m, k], h, 2), slot) for h, (_, slot) in enumerate(halves)]

                def add():
                    for i, (dst, slot) in zip(slots, halves):
                        sum_rows(dst, [slot])
                        wk_pool.give(i)
                    net.now += 0.8
                    done = net.copy(ref, w_pt.at[m, k])
                    wout_pool.give(j, [done])
                    net.when([done], w_in[m, k].hit)

                net.when(loads, add)

            net.job([w_side[m, k]], [(wk_pool, 2)], begin, FIRST)

        def multiply(which, free):
            def then(slots):
                refs = [wout_pool.refs[j] for j in slots]
                one, two = cut_pool.refs[held[0]]

                @pl.loop(0, 2 * wc // tile_w)
                def _(j):
                    at = rows_at(j * tile_w, tile_w)
                    for m, ref in zip(which, refs):
                        cut = (two if m == 2 else one)[...].reshape(n_tok, wr)
                        ref[:, at] = dot(cut, (da_all, db_all, h_all)[m][:, at], 0, 0)

                if free:
                    cut_pool.give(held[0])
                for m, j, ref in zip(which, slots, refs):
                    out(m, j, ref)
            return then

        flags = [loaded] + all_hidden
        step = "W%d%s" % (k, "ab"[turn])
        first = min(ranks[step + m] for m in "gud") if k == 0 else ranks[step]
        net.job(list(tokens_in.values()), [(cut_pool, 1)], load, first * EARLY, "cut")
        if k == 0:
            last = max(mats, key=lambda m: ranks[step + "gud"[m]])
            for m in range(3):
                net.job(flags, [(wout_pool, 1)], multiply([m], m == last), ranks[step + "gud"[m]], "mxu", 1.25)
        else:
            net.job(flags, [(wout_pool, len(mats))], multiply(mats, True), ranks[step], "mxu", 3.0)

    for k, name in enumerate(ORDER):
        grads_of(k, name, 1 - c, 0)
        grads_of(k, name, c, 1)

    def w_view(ref, shape):
        return ref.at[pl.ds(0, shape[0]), pl.ds(0, shape[1])]

    w_add = Adder(net, wk_pool, w_view)
    mine, other = rows_at(a * wc, wc), rows_at((1 - a) * wc, wc)

    def w_ring_first(m, row0, size, l1, l2, lp, own):
        def part(ref, h):
            return ref.at[pl.ds(row0 + h * (size // 2), size // 2)]

        near = [[Flag(), Flag()] for _ in SIDES]
        ring_reduce(
            net, w_add, lambda name, h: [w_in[m, names[name]]],
            lambda name, h: [part(w_pt.at[m, names[name]], h)], l1, lambda k, h: l2.at[k, h], ring_x, near,
        )

        def last(h):
            block = part(w_pt.at[m, 3], h)
            away = block.at[:, other]

            def go():
                got, _ = net.send("wgt", away, row_half(lp, h))
                net.when([got], nothing)

            w_add.add(
                [w_in[m, 3], *near[h]], [block, l2.at[0, h], l2.at[1, h]],
                lambda ref: [(ref.at[:, other], away), (ref.at[:, mine], row_half(own, h))], go,
            )

        last(0)
        last(1)

    def w_pair_first(m, row0, size, lp, l1, soon, late, own):
        def part(ref, h):
            return ref.at[pl.ds(row0 + h * (size // 2), size // 2)]

        have = {k: [w_in[m, k]] for k in range(4)}
        pair = {(k, h): Flag() for k in range(4) for h in range(2)}

        def away(k, h):
            def go():
                got, _ = net.send("wgt", part(w_pt.at[m, k], h).at[:, other], row_half(lp.at[k], h))
                net.arrive(got, pair[k, h])

            net.job(have[k], [], go, NEXT)

        for k in range(4):
            for h in range(2):
                away(k, h)

        def terms(name, h):
            k = names[name]
            return [part(w_pt.at[m, k], h).at[:, mine], row_half(lp.at[k], h)]

        def ready(name, h):
            return have[names[name]] + [pair[names[name], h]]

        near = [[Flag(), Flag()] for _ in SIDES]
        ring_reduce(
            net, w_add, ready, terms, l1, lambda k, h: row_half(late if k == h else soon, h), ring_x, near,
        )
        for h in SIDES:
            w_add.add(
                ready("o", h) + [near[h][1]], terms("o", h) + [row_half(soon, h)],
                lambda ref, h=h: [(ref, row_half(own, h))], nothing,
            )

    most = wr * 2 // 3
    w_ring_first(0, 0, wr, g_l1, g_l2, g_lp, g_own)
    w_pair_first(2, 0, wr, d_lp, d_l1, d_soon, d_late, d_own)
    w_ring_first(1, 0, most, u_l1, u_l2, u_lp, u_own)
    w_pair_first(1, most, wr - most, v_lp, v_l1, v_soon, v_late, v_own)
    net.run()


def finish_kernel(
    x_ref, dy_ref, y_own, y_late, r_own, r_lp, q_own, q_late, g_own, g_lp, u_own, u_lp, v_own, v_late, d_own, d_late,
    y_ref, dx_ref, g_ref, u_ref, d_ref,
):
    half, low = y_own.shape[-1], r_own.shape[-1]
    for j in range(2):
        cols = pl.ds(j * half, half)
        y_ref[:, :, cols] = (x_ref[:, :, cols].astype(F32) + (y_own[j] + y_late[j])).astype(BF16)
    for cols, own, late in ((pl.ds(0, low), r_own, r_lp), (pl.ds(low, q_own.shape[-1]), q_own, q_late)):
        dx_ref[:, :, cols] = (dy_ref[:, :, cols].astype(F32) + (own[...] + late[...])).astype(BF16)
    g_ref[...] = g_own[...] + g_lp[...]
    row = 0
    for own, late in ((u_own, u_lp), (v_own, v_late)):
        size = own.shape[0]
        at = pl.multiple_of(row + pl.program_id(0) * size, size)
        u_ref[pl.ds(at, size), :] = own[...] + late[...]
        row = size * pl.num_programs(0)
    d_ref[...] = (d_own[...] + d_late[...]).T


def finish(x, dy, y_own, y_late, *others):
    micro, rows, width = x.shape
    r_own, g_own = others[0], others[4]
    wr, wc = g_own.shape
    n = 4
    S = jax.ShapeDtypeStruct

    def tok(array):
        return pl.BlockSpec((micro, rows // n, array.shape[-1]), lambda i: (0, i, 0))

    def flat(array):
        return pl.BlockSpec((array.shape[0] // n, wc), lambda i: (i, 0))

    halves = pl.BlockSpec((2, micro, rows // n, width // 2), lambda i: (0, 0, i, 0))
    turned = pl.BlockSpec((wr, wc // n), lambda i: (0, i))
    return pl.pallas_call(
        finish_kernel,
        name="finish",
        grid=(n,),
        out_shape=(S(x.shape, BF16), S(x.shape, BF16), S((wr, wc), F32), S((wr, wc), F32), S((wc, wr), F32)),
        in_specs=[
            tok(x), tok(x), halves, halves, *map(tok, others[:4]), *map(flat, others[4:10]), turned, turned,
        ],
        out_specs=[
            tok(x), tok(x), flat(g_own), pl.BlockSpec((wr, wc), lambda i: (0, 0)), pl.BlockSpec((wc // n, wr), lambda i: (i, 0)),
        ],
        compiler_params=pltpu.CompilerParams(vmem_limit_bytes=60 * 2**20),
    )(x, dy, y_own, y_late, *others)


def solution(mesh):
    row_spec = P(None, ("dp", "tp"), None)
    in_specs = (row_spec, P("dp", "tp"), P("dp", "tp"), P("tp", "dp"), row_spec)
    out_specs = (row_spec, row_spec, P("dp", "tp"), P("dp", "tp"), P("tp", "dp"))
    hbm = pl.BlockSpec(memory_space=pl.ANY)
    dma = pltpu.SemaphoreType.DMA
    V = pltpu.VMEM
    S = jax.ShapeDtypeStruct

    def local_step(x_loc, wg, wu, wd, dy_loc):
        micro, rows, width = x_loc.shape
        wr, wc = wg.shape
        fw = 2 * wc
        most = wr * 2 // 3
        few = wr - most
        r_cols = width // 3
        n = 8 * micro * rows
        tok = (micro, rows, width)
        half, tok_r, tok_q = ((micro, rows, w) for w in (width // 2, r_cols, width - r_cols))
        two = (2,)

        def f32(*shape):
            return S(shape, F32)

        outs = [
            f32(*two, *half), f32(*two, *half), f32(*tok_r), f32(*tok_r), f32(*tok_q), f32(*tok_q),
            *[f32(size, wc) for size in (wr, wr, most, most, few, few, wr, wr)],
        ]
        weights = f32(3, 4, wr, fw)
        space = [
            S((4, 2) + tok, BF16), S((4, 2) + tok, BF16), S((fw, width), BF16),
            f32(2, 3, *half), f32(*two, *half), f32(4, 2, *tok_r), f32(4, 2, *tok_q), weights,
            f32(*two, *half), f32(*two, *half), f32(*two, *tok_r), f32(*two, *two, *tok_r),
            f32(4, *tok_q), f32(*tok_q), f32(*tok_q), weights,
        ]
        for size in (wr // 2, most // 2):
            space += [f32(*two, size, fw), f32(*two, *two, size, fw)]
        for size in (few, wr):
            space += [f32(4, size, wc), f32(*two, size // 2, wc), f32(size, wc)]
        res = pl.pallas_call(
            layer_kernel,
            name="layer",
            out_shape=tuple(outs + space),
            in_specs=[hbm] * 5,
            out_specs=[hbm] * (len(outs) + len(space)),
            scratch_shapes=[
                V((width, fw), BF16), V((width, fw), BF16), V((fw, width), BF16),
                V((n, fw), BF16), V((n, fw), BF16), V((n, fw), BF16), V((n // 2, fw), BF16),
                V((2, 2) + tok, BF16), V((2, 2) + tok, BF16),
                V((2, 4, 2, micro, rows, wr), BF16), V((2, 4, 2, micro, rows, wr), BF16),
                V((1, 2) + tok_r, F32), V((2, 2) + tok_q, F32),
                V((2, 4, micro, rows, width // 4), F32), V((2, fw, width // 4), BF16), V((TW, wr, fw), F32),
                V((TR,) + tok_r, F32), V((TK,) + tok_q[1:], F32), V((WK, wr // 2, fw), F32),
                dma((128,)), dma((200,)), dma((200,)),
            ],
            compiler_params=pltpu.CompilerParams(
                collective_id=0, has_side_effects=True, vmem_limit_bytes=67_000_000
            ),
        )(x_loc, dy_loc, wg, wu, wd)
        return finish(x_loc, dy_loc, *res[: len(outs)])

    return jax.shard_map(local_step, mesh=mesh, in_specs=in_specs, out_specs=out_specs, check_vma=False)
```

```python
import functools
import heapq

import jax
import jax.numpy as jnp
from jax import lax
from jax.experimental import pallas as pl
from jax.experimental.pallas import tpu as pltpu
from jax.sharding import PartitionSpec as P

MESH = pl.DeviceIdType.MESH
F32 = jnp.float32
BF16 = jnp.bfloat16
ICI_RATE = 45.0e3
CORE_RATE = 550.0e3
HBM_RATE = 2.5e6
MARGIN = 0.3
FIRST, NEXT, EARLY = 0.5, 1, 0.01
SIDES = (0, 1)
TW, TR, TK, WK = 6, 3, 4, 5
COPIES = 224
RING = 4
AROUND = (1, 3, 2)
BLOCKS = {
    "A": (("o", 0), ("o", 1)), "B": (("-", 0), ("+", 0)), "C": (("-", 1), ("+", 1)), "D": (("2", 0),), "E": (("2", 1),),
}
STEPS = (
    "HBa", "HAa", "HBb", "HAb", "HDb", "HCb", "HDa", "HCa", "R+", "HEb",
    "W0ag1", "W0au1", "HEa", "W0bu1", "W0bg1", "R2", "W0ad1", "W0ad0", "W0ag0", "W0bd1",
    "W0au0", "W0bg0", "R-", "W2a", "W0bd0", "W0bu0", "Q+", "Ro", "W2b", "Y3",
    "Q2", "Y2", "W1a", "W1b", "W3a", "Y0", "Y1", "Q-", "Qo", "W3b",
)


def nbytes(ref):
    size = jnp.dtype(ref.dtype).itemsize
    for n in ref.shape:
        size *= n
    return size


class Place:
    def __init__(self):
        t = lax.axis_index("tp")
        d = lax.axis_index("dp")
        z, y, x, c = t // RING, t % RING, d // 2, d % 2
        self.z, self.y, self.x, self.c = z, y, x, c
        self.b = y % 2
        self.a = y // 2
        self.zp, self.zm, self.z2 = ((z + n) % RING for n in AROUND)
        self.xp, self.xm, self.x2 = ((x + n) % RING for n in AROUND)

        def at(z, y, x, c):
            return {"tp": z * RING + y, "dp": x * 2 + c}

        self.dev = {
            "z+": at(self.zp, y, x, c),
            "z-": at(self.zm, y, x, c),
            "x+": at(z, y, self.xp, c),
            "x-": at(z, y, self.xm, c),
            "tok": at(z, y + 1 - 2 * self.b, x, c),
            "wgt": at(z, 3 - y, x, c),
            "core": at(z, y, x, 1 - c),
        }

    def barrier(self):
        sem = pltpu.get_barrier_semaphore()
        for dev in self.dev.values():
            pl.semaphore_signal(sem, inc=1, device_id=dev, device_id_type=MESH)
        pl.semaphore_wait(sem, len(self.dev))


class Handle:
    def __init__(self, time, wait, after=None):
        self.time, self._wait, self.after, self.done = time, wait, after, False

    def wait(self):
        if not self.done:
            self.done = True
            self._wait()
            if self.after is not None:
                self.after()


class Flag:
    def __init__(self, count=1):
        self.left = count

    def hit(self):
        self.left -= 1


class Pool:
    def __init__(self, refs):
        self.refs = refs
        self.back = [[] for _ in refs]
        self.free = [True] * len(refs)

    def when_ready(self, count):
        times = sorted(max((h.time for h in self.back[i]), default=0.0) for i in range(len(self.refs)) if self.free[i])
        return times[count - 1] if len(times) >= count else float("inf")

    def take(self, count):
        order = sorted(
            (max((h.time for h in self.back[i]), default=0.0), i) for i in range(len(self.refs)) if self.free[i]
        )
        got = [i for _, i in order[:count]]
        for i in got:
            for h in self.back[i]:
                h.wait()
            self.back[i] = []
            self.free[i] = False
        return got

    def give(self, i, handles=()):
        self.free[i] = True
        self.back[i] = list(handles)


class Net:
    def __init__(self, place, local_sems, send_sems, recv_sems):
        self.place, self.local_sems, self.send_sems, self.recv_sems = place, local_sems, send_sems, recv_sems
        self.used = 0
        self.local_used = 0
        self.local_free = []
        self.open = []
        self.heap = []
        self.jobs = []
        self.seq = 0
        self.now = 0.0
        self.free = {}
        self.log = []

    def send(self, link, src, dst, land=None):
        land = dst if land is None else land
        i = self.used
        self.used += 1
        dev = self.place.dev[link]

        def copy_of(a, b):
            return pltpu.make_async_remote_copy(
                src_ref=a, dst_ref=b, send_sem=self.send_sems.at[i], recv_sem=self.recv_sems.at[i],
                device_id=dev, device_id_type=MESH,
            )

        copy = copy_of(src, dst)
        copy.start()
        arrive = copy_of(land, land)
        rate = CORE_RATE if link == "core" else ICI_RATE
        end = max(self.now, self.free.get(link, 0.0)) + nbytes(land) / rate
        self.free[link] = end
        sent = Handle(end + 0.5, copy.wait_send)
        self.open.append(sent)
        return Handle(end + (1.0 if link == "core" else 2.0), arrive.wait_recv), sent

    def copy(self, src, dst):
        if self.local_free:
            i = self.local_free.pop(0)
        else:
            i = self.local_used
            self.local_used += 1
        copy = pltpu.make_async_copy(src, dst, self.local_sems.at[i])
        copy.start()
        end = max(self.now, self.free.get("hbm", 0.0)) + nbytes(src) / HBM_RATE
        self.free["hbm"] = end
        handle = Handle(end + 0.8, copy.wait, lambda: self.local_free.append(i))
        self.open.append(handle)
        return handle

    def when(self, handles, then):
        self.seq += 1
        heapq.heappush(self.heap, (max(h.time for h in handles), self.seq, handles, then))

    def job(self, flags, needs, then, rank, line=None, cost=0.1):
        self.seq += 1
        self.jobs.append((rank, self.seq, flags, needs, then, cost, line))
        self.jobs.sort(key=lambda j: j[:2])

    def run(self):
        while True:
            if self.heap and self.heap[0][0] + MARGIN <= self.now:
                self.event()
                continue
            chosen = None
            soonest = float("inf")
            held = set()
            for j in self.jobs:
                if j[6] is not None:
                    if j[6] in held:
                        continue
                    held.add(j[6])
                if any(f.left > 0 for f in j[2]):
                    continue
                ready = max((pool.when_ready(n) for pool, n in j[3]), default=0.0)
                if ready <= self.now:
                    chosen = j
                    break
                soonest = min(soonest, ready)
            if chosen is not None:
                self.jobs.remove(chosen)
                _, _, _, needs, then, cost, _ = chosen
                slots = [pool.take(n) for pool, n in needs]
                self.now += cost
                then(*slots)
                continue
            if self.heap and self.heap[0][0] <= soonest:
                self.event()
            elif soonest < float("inf"):
                self.now = max(self.now, soonest)
            else:
                break
        assert not self.jobs, "jobs left"
        for handle in self.open:
            handle.wait()

    def event(self):
        time, _, handles, then = heapq.heappop(self.heap)
        self.now = max(self.now, time)
        for h in handles:
            h.wait()
        then()

    def arrive(self, handle, flag):
        self.when([handle], flag.hit)


def nothing():
    pass


def gather_ring_first(net, own, slot, half, ring, pair, me, each):
    r, rp, rm, r2, p = me
    up, down = ring
    from_down, _ = net.send(up, own, slot(r, p), slot(rm, p))
    from_up, _ = net.send(down, own, slot(r, p), slot(rp, p))
    other, _ = net.send(pair, own, slot(r, p), slot(r, 1 - p))
    net.when([other], lambda: each("o", 1, r, 1 - p))

    def pass_on(name, q):
        got, _ = net.send(pair, slot(q, p), slot(q, p), slot(q, 1 - p))
        net.when([got], lambda: each(name, 1, q, 1 - p))

    far = []

    def got_near(name, q, h, link):
        def then():
            ref = half(slot(q, p), h)
            far.append(net.send(link, ref, ref, half(slot(r2, p), h))[0])
            pass_on(name, q)
            each(name, 0, q, p)
            if len(far) == 2:
                net.when(far, got_far)
        return then

    def got_far():
        pass_on("2", r2)
        each("2", 0, r2, p)

    net.when([from_down], got_near("-", rm, 0, up))
    net.when([from_up], got_near("+", rp, 1, down))


def gather_pair_first(net, own, slot, half, ring, pair, me, each, late=False):
    r, rp, rm, r2, p = me
    up, down = ring

    def around(src, q, k):
        from_down, _ = net.send(up, src, slot(r, q), slot(rm, q))
        from_up, _ = net.send(down, src, slot(r, q), slot(rp, q))
        far = []

        def got_near(name, s, h, link):
            def then():
                ref = half(slot(s, q), h)
                far.append(net.send(link, ref, ref, half(slot(r2, q), h))[0])
                each(name, k, s, q)
                if k == 0 and late:
                    go_other()
                if len(far) == 2:
                    net.when(far, lambda: each("2", k, r2, q))
            return then

        net.when([from_down], got_near("-", rm, 0, up))
        net.when([from_up], got_near("+", rp, 1, down))

    other, _ = net.send(pair, own, slot(r, p), slot(r, 1 - p))
    before = Flag(3 if late else 1)

    def go_other():
        before.hit()
        if before.left == 0:
            around(slot(r, 1 - p), 1 - p, 1)

    def got_other():
        each("o", 1, r, 1 - p)
        go_other()

    net.when([other], got_other)
    around(own, p, 0)


def sum_rows(dst, srcs):
    if len(dst.shape) > 2:
        for i in range(dst.shape[0]):
            sum_rows(dst.at[i], [s.at[i] for s in srcs])
        return
    step = 16

    @pl.loop(0, dst.shape[0] // step)
    def _(i):
        at = pl.ds(pl.multiple_of(i * step, step), step)
        total = dst[at, :]
        for s in srcs:
            total = total + s[at, :]
        dst[at, :] = total


def dot(a, b, ca, cb):
    return lax.dot_general(a, b, (((ca,), (cb,)), ((), ())), preferred_element_type=F32)


def nth(refs, i, n):
    size = refs.shape[0] // n
    return refs.at[pl.ds(i * size, size)]


ORDER = ("2", "+", "-", "o")


class Adder:
    def __init__(self, net, pool, view):
        self.net, self.pool, self.view = net, pool, view

    def add(self, flags, srcs, outs, then):
        net, pool = self.net, self.pool

        def begin(slots):
            refs = [self.view(pool.refs[i], srcs[0].shape) for i in slots]
            loads = [net.copy(src, ref) for src, ref in zip(srcs, refs)]

            def done():
                sum_rows(refs[0], refs[1:])
                net.now += 0.25 * len(refs) * nbytes(refs[0]) / 1.0e6
                for i in slots[1:]:
                    pool.give(i)
                copies = [net.copy(src, dst) for src, dst in outs(refs[0])]
                pool.give(slots[0], copies)
                net.when(copies, then)

            net.when(loads, done)

        net.job(flags, [(pool, len(srcs))], begin, NEXT)


def ring_reduce(net, adder, ready, srcs, l1, l2, links, near):
    come = [Flag(), Flag()]

    def go(name, h, more, flags, link, dst, flag):
        terms = srcs(name, h) + more

        def send():
            got, _ = net.send(link, terms[0], dst)
            net.arrive(got, flag)

        if len(terms) == 1:
            net.job(ready(name, h) + flags, [], send, NEXT)
        else:
            adder.add(ready(name, h) + flags, terms, lambda ref: [(ref, terms[0])], send)

    for h, link in enumerate(links):
        go("2", h, [], [], link, l1.at[h], come[h])
    for k, link in enumerate(links):
        name = link[-1]
        go(name, 1 - k, [], [], link, l2(k, 1 - k), near[1 - k][1])
        go(name, k, [l1.at[k]], [come[k]], link, l2(k, k), near[k][0])


def layer_kernel(
    x_ref, dy_ref, wg_ref, wu_ref, wd_ref,
    y_own, y_late, r_own, r_lp, q_own, q_late, g_own, g_lp, u_own, u_lp, v_own, v_late, d_own, d_late,
    x_all, dy_all, wd_ext, y_pt, y_mine, r_pt, q_pt, w_pt, y_l1, y_soon, r_l1, r_l2, q_lp, q_l1, q_soon, w_lc,
    g_l1, g_l2, u_l1, u_l2, v_lp, v_l1, v_soon, d_lp, d_l1, d_soon,
    wg_all, wu_all, wd_all, h_all, da_all, db_all, h_ext, xb, db, xs, ds, r_out, q_out, y_out, wx, tw, tr, tk, wk,
    local_sems, send_sems, recv_sems,
):
    here = Place()
    here.barrier()
    net = Net(here, local_sems, send_sems, recv_sems)
    z, zp, zm, z2, b = here.z, here.zp, here.zm, here.z2, here.b
    x, xp, xm, x2, a, c = here.x, here.xp, here.xm, here.x2, here.a, here.c
    micro, rows, width = x_ref.shape
    wr, wc = wg_ref.shape
    r_cols = width // 3
    q_cols = width - r_cols
    edge = width * 5 // 24
    m_blk = micro * rows
    n_blk = 2 * m_blk
    zs = {"o": z, "+": zp, "-": zm, "2": z2}
    xs_of = {"o": x, "+": xp, "-": xm, "2": x2}
    ring_z, ring_x = ("z+", "z-"), ("x+", "x-")

    def rows_at(start, size):
        return pl.ds(pl.multiple_of(start, size), size)

    weights_in = [Flag(24), Flag(24)]
    pieces = [(name, side) for name in zs for side in range(2)]
    tokens_in = {piece: Flag(2 if piece == ("o", 0) else 3) for piece in pieces}
    ext_in = Flag(16)

    def up_slot(ref, core):
        return lambda q, p: ref.at[rows_at((q * 2 + core) * wr, wr), rows_at(p * wc, wc)]

    def down_slot(ref, core):
        return lambda q, p: ref.at[rows_at(p * wc, wc), rows_at((q * 2 + core) * wr, wr)]

    def row_half(ref, h):
        return nth(ref, h, 2)

    def tok_half(ref, h):
        return ref.at[h]

    in_z = (z, zp, zm, z2, b)
    in_x = (x, xp, xm, x2, a)

    def across(mine, theirs):
        def each(name, k, q, p):
            weights_in[k].hit()
            got, _ = net.send("core", mine(q, p), mine(q, p), theirs(q, p))
            net.arrive(got, weights_in[k])
        return each

    for fn, own, mine, theirs in (
        (gather_ring_first, wg_ref, up_slot(wg_all, c), up_slot(wg_all, 1 - c)),
        (functools.partial(gather_pair_first, late=True), wu_ref, up_slot(wu_all, c), up_slot(wu_all, 1 - c)),
        (functools.partial(gather_pair_first, late=True), wd_ref, down_slot(wd_all, c), down_slot(wd_all, 1 - c)),
    ):
        fn(net, own, mine, row_half, ring_x, "wgt", in_x, across(mine, theirs))
        got, _ = net.send("core", own, mine(x, a), theirs(x, a))
        net.arrive(got, weights_in[0])
        net.arrive(net.copy(own, mine(x, a)), weights_in[0])

    ext, ext_side = down_slot(wd_ext, c), down_slot(wd_ext, 1 - c)

    def ext_each(q, p):
        ext_in.hit()
        got, _ = net.send("core", ext(q, p), ext(q, p), ext_side(q, p))
        net.arrive(got, ext_in)

    def ext_round(p):
        from_down, _ = net.send("x+", ext(x, p), ext(x, p), ext(xm, p))
        from_up, _ = net.send("x-", ext(x, p), ext(x, p), ext(xp, p))
        far = []

        def near(q, h, link):
            def then():
                ref = row_half(ext(q, p), h)
                far.append(net.send(link, ref, ref, row_half(ext(x2, p), h))[0])
                ext_each(q, p)
                if len(far) == 2:
                    net.when(far, lambda: ext_each(x2, p))
            return then

        net.when([from_down], near(xm, 0, "x+"))
        net.when([from_up], near(xp, 1, "x-"))
        ext_each(x, p)

    def ext_start():
        got, _ = net.send("tok", wd_ref, ext(x, a))

        def pass_on():
            more, _ = net.send("wgt", ext(x, a), ext(x, a), ext(x, 1 - a))
            net.when([more], lambda: ext_round(1 - a))
            ext_round(a)

        net.when([got], pass_on)

    started = []

    def count_tokens(name, k, q, p):
        tokens_in[name, k].hit()

    def count_main(name, k, q, p):
        count_tokens(name, k, q, p)
        if name == "-" and not started:
            started.append(True)
            ext_start()

    for fn, own, dst, cols, each in (
        (gather_pair_first, x_ref, x_all, pl.ds(width - edge, edge), count_tokens),
        (gather_ring_first, x_ref, x_all, pl.ds(0, width - edge), count_main),
        (gather_pair_first, dy_ref, dy_all, pl.ds(0, width), count_tokens),
    ):
        slot = functools.partial(lambda q, p, dst, cols: dst.at[q, p, :, :, cols], dst=dst, cols=cols)
        fn(net, own.at[:, :, cols], slot, tok_half, ring_z, "tok", in_z, each)

    tok_pool = Pool([(xb.at[i], db.at[i]) for i in range(xb.shape[0])])
    cut_pool = Pool([(xs.at[i], ds.at[i]) for i in range(xs.shape[0])])
    r_pool = Pool([r_out.at[i] for i in range(r_out.shape[0])])
    q_pool = Pool([q_out.at[i] for i in range(q_out.shape[0])])
    y_pool = Pool([y_out.at[i] for i in range(y_out.shape[0])])
    ext_pool = Pool([wx.at[i] for i in range(wx.shape[0])])
    wout_pool = Pool([tw.at[i] for i in range(tw.shape[0])])
    pair_pool = Pool([tr.at[i] for i in range(tr.shape[0])])
    row_pool = Pool([tk.at[i] for i in range(tk.shape[0])])
    wk_pool = Pool([wk.at[i] for i in range(wk.shape[0])])

    first_slot = tok_pool.take(1)[0]
    bounce = tok_pool.refs[first_slot]
    into = [net.copy(src, ref.at[0]) for src, ref in zip((x_ref, dy_ref), bounce)]

    def own_rows():
        out = [net.copy(ref.at[0], dst.at[z, b]) for ref, dst in zip(bounce, (x_all, dy_all))]
        tok_pool.give(first_slot, out)
        for handle in out:
            net.arrive(handle, tokens_in["o", 0])

    net.when(into, own_rows)

    ranks = {step: 10 + i for i, step in enumerate(STEPS)}

    hidden = {(piece, turn): Flag() for piece in pieces for turn in SIDES}
    ext_rows = Flag(4)
    tile_h = min(256, wc)

    def piece_rows(piece):
        name, side = piece
        return rows_at(zs[name] * n_blk + (b if side == 0 else 1 - b) * m_blk, m_blk)

    def hidden_of(key, turn):
        block = BLOCKS[key]
        count = len(block)
        cols_at = a * wc if turn == 0 else (1 - a) * wc
        rank = ranks["H" + key + "ab"[turn]]
        loaded = Flag()
        held = []

        def load(slots):
            i = slots[0]
            held.append(i)
            copies = []
            for n, (name, side) in enumerate(block):
                for ref, src in zip(tok_pool.refs[i], (x_all, dy_all)):
                    copies.append(net.copy(src.at[zs[name], b if side == 0 else 1 - b], ref.at[n]))
            net.when(copies, loaded.hit)

        def multiply():
            i = held[0]
            one, two = tok_pool.refs[i]

            @pl.loop(0, wc // tile_h)
            def _(j):
                cols = rows_at(cols_at + j * tile_h, tile_h)
                x_blk = one[:count].reshape(count * m_blk, width)
                dy_blk = two[:count].reshape(count * m_blk, width)
                pre = dot(x_blk, wg_all[:, cols], 1, 0)
                up = dot(x_blk, wu_all[:, cols], 1, 0)
                g = dot(dy_blk, wd_all[cols, :], 1, 1)
                s = jax.nn.sigmoid(pre)
                act = pre * s
                h = (act * up).astype(BF16)
                da = (g * up * s * (1.0 + pre * (1.0 - s))).astype(BF16)
                db = (g * act).astype(BF16)
                for n, piece in enumerate(block):
                    at = piece_rows(piece)
                    cut = slice(n * m_blk, (n + 1) * m_blk)
                    h_all[at, cols] = h[cut]
                    da_all[at, cols] = da[cut]
                    db_all[at, cols] = db[cut]

            tok_pool.give(i)
            for piece in block:
                hidden[piece, turn].hit()

        net.job([tokens_in[piece] for piece in block], [(tok_pool, 1)], load, rank * EARLY, "load")
        net.job([loaded, weights_in[turn]], [], multiply, rank, "mxu", 1.3 + 0.85 * count)

    def both(piece):
        return [hidden[piece, turn] for turn in SIDES]

    def give_hidden(name):
        def go():
            got, _ = net.send("tok", h_all.at[piece_rows((name, 1)), :], h_ext.at[rows_at(zs[name] * m_blk, m_blk), :])
            net.arrive(got, ext_rows)
        net.job(both((name, 1)), [], go, NEXT)

    for key in BLOCKS:
        hidden_of(key, 0)
        hidden_of(key, 1)
    for name in zs:
        give_hidden(name)

    r_in = {k: Flag() for k in zs}
    q_in = {k: Flag() for k in zs}
    tile_dx = r_cols

    def rows_of(name, pool, part, flag, col0, cols, rank):
        at = rows_at(zs[name] * n_blk, n_blk)

        def multiply(slots):
            i = slots[0]
            ref = pool.refs[i]

            @pl.loop(0, cols // tile_dx)
            def _(j):
                src = rows_at(col0 + j * tile_dx, tile_dx)
                val = dot(da_all[at, :], wg_all[src, :], 1, 1) + dot(db_all[at, :], wu_all[src, :], 1, 1)
                ref[:, :, :, rows_at(j * tile_dx, tile_dx)] = val.reshape(2, micro, rows, tile_dx)

            done = net.copy(ref, part.at[zs[name]])
            pool.give(i, [done])
            net.when([done], flag.hit)

        net.job(both((name, 0)) + both((name, 1)), [(pool, 1)], multiply, rank, "mxu", 1.4 * cols // tile_dx)

    for name in zs:
        rows_of(name, r_pool, r_pt, r_in[name], 0, r_cols, ranks["R" + name])
        rows_of(name, q_pool, q_pt, q_in[name], r_cols, q_cols, ranks["Q" + name])

    quarter = width // 4
    tile_y = quarter // 3 if quarter % 3 == 0 else quarter
    y_in = [Flag(2), Flag(2)]

    def y_of(j):
        loaded = Flag()
        held = []
        cols = pl.ds(j * quarter, quarter)

        def load(slots):
            held.append(slots[0])
            net.when([net.copy(wd_ext.at[:, cols], ext_pool.refs[slots[0]])], loaded.hit)

        def multiply(slots):
            i = slots[0]
            ref = y_pool.refs[i]
            w_ref = ext_pool.refs[held[0]]
            mine = [rows_at(zs[name] * n_blk + b * m_blk, m_blk) for name in ORDER]
            other = [rows_at(zs[name] * m_blk, m_blk) for name in ORDER]

            @pl.loop(0, quarter // tile_y)
            def _(n):
                near = jnp.concatenate([h_all[at, :] for at in mine], axis=0)
                far = jnp.concatenate([h_ext[at, :] for at in other], axis=0)
                at = rows_at(n * tile_y, tile_y)
                val = dot(near, wd_all[:, rows_at(j * quarter + n * tile_y, tile_y)], 1, 0) + dot(far, w_ref[:, at], 1, 0)
                ref[:, :, :, at] = val.reshape(4, micro, rows, tile_y)

            ext_pool.give(held[0])
            half = pl.ds((j % 2) * quarter, quarter)
            out = [net.copy(ref.at[k], y_pt.at[j // 2, k, :, :, half]) for k in range(3)]
            out.append(net.copy(ref.at[3], y_mine.at[j // 2, :, :, half]))
            y_pool.give(i, out)
            net.when(out, y_in[j // 2].hit)

        net.job([ext_in], [(ext_pool, 1)], load, ranks["Y%d" % j] * EARLY, "ext")
        own = [flag for name in zs for flag in both((name, 0))]
        net.job([loaded, ext_rows] + own, [(y_pool, 1)], multiply, ranks["Y%d" % j], "mxu", 2.3)

    for j in range(4):
        y_of(j)

    pair_add = Adder(net, pair_pool, lambda ref, shape: ref)
    row_add = Adder(net, row_pool, lambda ref, shape: ref.at[:, pl.ds(0, shape[-1])])
    names = {name: k for k, name in enumerate(ORDER)}

    r_near = [[Flag(), Flag()] for _ in SIDES]
    ring_reduce(
        net, pair_add, lambda name, h: [r_in[name]], lambda name, h: [r_pt.at[zs[name], :, h]],
        r_l1, lambda k, h: r_l2.at[k, h], ring_z, r_near,
    )

    def r_last(h):
        away = r_pt.at[z, 1 - b, h]

        def go():
            got, _ = net.send("tok", away, r_lp.at[h])
            net.when([got], nothing)

        pair_add.add(
            [r_in["o"], *r_near[h]], [r_pt.at[z, :, h], r_l2.at[0, h], r_l2.at[1, h]],
            lambda ref: [(ref.at[1 - b], away), (ref.at[b], r_own.at[h])], go,
        )

    r_last(0)
    r_last(1)

    for j in range(2):
        y_near = [[Flag(), Flag()] for _ in SIDES]
        ring_reduce(
            net, row_add, lambda name, h, j=j: [y_in[j]], lambda name, h, j=j: [y_pt.at[j, names[name], h]],
            y_l1.at[j], lambda k, h, j=j: (y_late if k == h else y_soon).at[j, h], ring_z, y_near,
        )
        for h in SIDES:
            row_add.add(
                [y_in[j], y_near[h][1]], [y_mine.at[j, h], y_soon.at[j, h]],
                lambda ref, j=j, h=h: [(ref, y_own.at[j, h])], nothing,
            )

    q_pair = {k: Flag() for k in zs}

    def pair_q(name):
        def go():
            got, _ = net.send("tok", q_pt.at[zs[name], 1 - b], q_lp.at[names[name]])
            net.arrive(got, q_pair[name])
        net.job([q_in[name]], [], go, NEXT)

    for name in ORDER:
        pair_q(name)
    q_near = [[Flag(), Flag()] for _ in SIDES]
    ring_reduce(
        net, row_add, lambda name, h: [q_in[name], q_pair[name]],
        lambda name, h: [q_pt.at[zs[name], b, h], q_lp.at[names[name], h]],
        q_l1, lambda k, h: (q_late if k == h else q_soon).at[h], ring_z, q_near,
    )
    for h in SIDES:
        row_add.add(
            [q_in["o"], q_pair["o"], q_near[h][1]], [q_pt.at[z, b, h], q_lp.at[3, h], q_soon.at[h]],
            lambda ref, h=h: [(ref, q_own.at[h])], nothing,
        )

    n_tok = 4 * n_blk
    mats = range(3)
    keys = [(m, k, h) for m in mats for k in range(RING) for h in SIDES]
    w_in = {key: Flag() for key in keys}
    w_side = {key: Flag() for key in keys}
    columns = (rows_at(a * wc, wc), rows_at((1 - a) * wc, wc))

    def grads_of(k, name, core, turn):
        loaded = Flag()
        held = []
        cols = rows_at((xs_of[name] * 2 + core) * wr, wr)
        step = "W%d%s" % (k, "ab"[turn])
        places = {}
        uses = Flag(len(mats) * 2 if k == 0 else 1)

        def load(slots):
            i = slots[0]
            held.append(i)
            one, two = cut_pool.refs[i]
            net.when([net.copy(x_all.at[:, :, :, :, cols], one), net.copy(dy_all.at[:, :, :, :, cols], two)], loaded.hit)

        def out(m, h):
            j, spent = places[m]
            ref = wout_pool.refs[j].at[:, columns[h]]

            def through(handle):
                spent.append(handle)
                if len(spent) == 2:
                    wout_pool.give(j, spent)

            if turn == 0:
                got, sent = net.send("core", ref, w_lc.at[m, k, :, columns[h]])
                through(sent)
                net.arrive(got, w_side[m, k, h])
                return

            def begin(slots):
                slot = wk_pool.refs[slots[0]]

                def add():
                    sum_rows(ref, [slot])
                    net.now += 0.4
                    wk_pool.give(slots[0])
                    done = net.copy(ref, w_pt.at[m, k, :, columns[h]])
                    through(done)
                    net.when([done], w_in[m, k, h].hit)

                net.when([net.copy(w_lc.at[m, k, :, columns[h]], slot)], add)

            net.job([w_side[m, k, h]], [(wk_pool, 1)], begin, FIRST)

        def product(m, at):
            one, two = cut_pool.refs[held[0]]
            cut = (two if m == 2 else one)[...].reshape(n_tok, wr)
            wout_pool.refs[places[m][0]][:, at] = dot(cut, (da_all, db_all, h_all)[m][:, at], 0, 0)

        def used():
            uses.hit()
            if uses.left == 0:
                cut_pool.give(held[0])

        def some(m, h):
            def then(*slots):
                if slots:
                    places[m] = (slots[0][0], [])
                product(m, columns[h])
                used()
                out(m, h)
            return then

        def all_of_it(slots):
            for m in mats:
                places[m] = (slots[m], [])

            @pl.loop(0, 2)
            def _(j):
                for m in mats:
                    product(m, rows_at(j * wc, wc))

            used()
            for h in SIDES:
                for m in mats:
                    out(m, h)

        parts = [(m, h, ranks["%s%s%d" % (step, "gud"[m], h)]) for m in mats for h in SIDES] if k == 0 else []
        first = min(rank for _, _, rank in parts) if parts else ranks[step]
        net.job(list(tokens_in.values()), [(cut_pool, 1)], load, first * EARLY, "cut")
        own = [hidden[piece, 0] for piece in pieces]
        other = [hidden[piece, 1] for piece in pieces]
        for m, h, rank in parts:
            begins = rank < ranks["%s%s%d" % (step, "gud"[m], 1 - h)]
            needs = [(wout_pool, 1)] if begins else []
            net.job([loaded] + (other if h else own), needs, some(m, h), rank, "mxu", 0.65)
        if not parts:
            net.job([loaded] + own + other, [(wout_pool, len(mats))], all_of_it, ranks[step], "mxu", 3.0)

    for k, name in enumerate(ORDER):
        grads_of(k, name, 1 - c, 0)
        grads_of(k, name, c, 1)

    def w_view(ref, shape):
        return ref.at[pl.ds(0, shape[0]), pl.ds(0, shape[1])]

    w_add = Adder(net, wk_pool, w_view)
    mine, other = columns

    def w_ring_first(m, row0, size, l1, l2, lp, own, links):
        def part(k, h):
            return w_pt.at[m, k, pl.ds(row0, size), columns[h]]

        near = [[Flag(), Flag()] for _ in SIDES]
        ring_reduce(
            net, w_add, lambda name, h: [w_in[m, names[name], h]], lambda name, h: [part(names[name], h)],
            l1, lambda k, h: l2.at[k, h], links, near,
        )

        def last(h, outs, then):
            w_add.add([w_in[m, 3, h], *near[h]], [part(3, h), l2.at[0, h], l2.at[1, h]], outs, then)

        def go():
            got, _ = net.send("wgt", part(3, 1), lp)
            net.when([got], nothing)

        last(1, lambda ref: [(ref, part(3, 1))], go)
        last(0, lambda ref: [(ref, own)], nothing)

    def w_pair_first(m, row0, size, lp, l1, soon, late, own):
        def part(ref, h):
            return ref.at[pl.ds(row0 + h * (size // 2), size // 2)]

        pair = {(k, h): Flag() for k in range(4) for h in range(2)}

        def away(k, h):
            def go():
                got, _ = net.send("wgt", part(w_pt.at[m, k], h).at[:, other], row_half(lp.at[k], h))
                net.arrive(got, pair[k, h])

            net.job([w_in[m, k, 1]], [], go, NEXT)

        for k in range(4):
            for h in range(2):
                away(k, h)

        def terms(name, h):
            k = names[name]
            return [part(w_pt.at[m, k], h).at[:, mine], row_half(lp.at[k], h)]

        def ready(name, h):
            return [w_in[m, names[name], 0], pair[names[name], h]]

        near = [[Flag(), Flag()] for _ in SIDES]
        ring_reduce(
            net, w_add, ready, terms, l1, lambda k, h: row_half(late if k == h else soon, h), ring_x, near,
        )
        for h in SIDES:
            w_add.add(
                ready("o", h) + [near[h][1]], terms("o", h) + [row_half(soon, h)],
                lambda ref, h=h: [(ref, row_half(own, h))], nothing,
            )

    most = wr * 2 // 3
    w_ring_first(0, 0, wr, g_l1, g_l2, g_lp, g_own, ring_x)
    w_pair_first(2, 0, wr, d_lp, d_l1, d_soon, d_late, d_own)
    w_ring_first(1, 0, most, u_l1, u_l2, u_lp, u_own, ring_x[::-1])
    w_pair_first(1, most, wr - most, v_lp, v_l1, v_soon, v_late, v_own)
    net.run()


def finish_kernel(
    x_ref, dy_ref, y_own, y_late, r_own, r_lp, q_own, q_late, g_own, g_lp, u_own, u_lp, v_own, v_late, d_own, d_late,
    y_ref, dx_ref, g_ref, u_ref, d_ref,
):
    half, low = y_own.shape[-1], r_own.shape[-1]
    for j in range(2):
        cols = pl.ds(j * half, half)
        y_ref[:, :, cols] = (x_ref[:, :, cols].astype(F32) + (y_own[j] + y_late[j])).astype(BF16)
    for cols, own, late in ((pl.ds(0, low), r_own, r_lp), (pl.ds(low, q_own.shape[-1]), q_own, q_late)):
        dx_ref[:, :, cols] = (dy_ref[:, :, cols].astype(F32) + (own[...] + late[...])).astype(BF16)
    g_ref[...] = g_own[...] + g_lp[...]
    row = 0
    for own, late in ((u_own, u_lp), (v_own, v_late)):
        size = own.shape[0]
        at = pl.multiple_of(row + pl.program_id(0) * size, size)
        u_ref[pl.ds(at, size), :] = own[...] + late[...]
        row = size * pl.num_programs(0)
    d_ref[...] = (d_own[...] + d_late[...]).T


def finish(x, dy, y_own, y_late, *others):
    micro, rows, width = x.shape
    r_own, g_own = others[0], others[4]
    wr, wc = g_own.shape
    n = 8
    S = jax.ShapeDtypeStruct

    def tok(array):
        return pl.BlockSpec((micro, rows // n, array.shape[-1]), lambda i: (0, i, 0))

    def flat(array):
        return pl.BlockSpec((array.shape[0] // n, wc), lambda i: (i, 0))

    halves = pl.BlockSpec((2, micro, rows // n, width // 2), lambda i: (0, 0, i, 0))
    lanes = wc // 4
    turned = pl.BlockSpec((wr, lanes), lambda i: (0, i // 2))
    return pl.pallas_call(
        finish_kernel,
        name="finish",
        grid=(n,),
        out_shape=(S(x.shape, BF16), S(x.shape, BF16), S((wr, wc), F32), S((wr, wc), F32), S((wc, wr), F32)),
        in_specs=[
            tok(x), tok(x), halves, halves, *map(tok, others[:4]), *map(flat, others[4:10]), turned, turned,
        ],
        out_specs=[
            tok(x), tok(x), flat(g_own), pl.BlockSpec((wr, wc), lambda i: (0, 0)), pl.BlockSpec((lanes, wr), lambda i: (i // 2, 0)),
        ],
        compiler_params=pltpu.CompilerParams(vmem_limit_bytes=60 * 2**20),
    )(x, dy, y_own, y_late, *others)


def solution(mesh):
    row_spec = P(None, ("dp", "tp"), None)
    in_specs = (row_spec, P("dp", "tp"), P("dp", "tp"), P("tp", "dp"), row_spec)
    out_specs = (row_spec, row_spec, P("dp", "tp"), P("dp", "tp"), P("tp", "dp"))
    hbm = pl.BlockSpec(memory_space=pl.ANY)
    dma = pltpu.SemaphoreType.DMA
    V = pltpu.VMEM
    S = jax.ShapeDtypeStruct

    def local_step(x_loc, wg, wu, wd, dy_loc):
        micro, rows, width = x_loc.shape
        wr, wc = wg.shape
        fw = 2 * wc
        most = wr * 2 // 3
        few = wr - most
        r_cols = width // 3
        n = 8 * micro * rows
        tok = (micro, rows, width)
        half, tok_r, tok_q = ((micro, rows, w) for w in (width // 2, r_cols, width - r_cols))
        two = (2,)

        def f32(*shape):
            return S(shape, F32)

        outs = [
            f32(*two, *half), f32(*two, *half), f32(*tok_r), f32(*tok_r), f32(*tok_q), f32(*tok_q),
            *[f32(size, wc) for size in (wr, wr, most, most, few, few, wr, wr)],
        ]
        weights = f32(3, 4, wr, fw)
        space = [
            S((4, 2) + tok, BF16), S((4, 2) + tok, BF16), S((fw, width), BF16),
            f32(2, 3, *half), f32(*two, *half), f32(4, 2, *tok_r), f32(4, 2, *tok_q), weights,
            f32(*two, *half), f32(*two, *half), f32(*two, *tok_r), f32(*two, *two, *tok_r),
            f32(4, *tok_q), f32(*tok_q), f32(*tok_q), weights,
        ]
        for size in (wr, most):
            space += [f32(*two, size, wc), f32(*two, *two, size, wc)]
        for size in (few, wr):
            space += [f32(4, size, wc), f32(*two, size // 2, wc), f32(size, wc)]
        res = pl.pallas_call(
            layer_kernel,
            name="layer",
            out_shape=tuple(outs + space),
            in_specs=[hbm] * 5,
            out_specs=[hbm] * (len(outs) + len(space)),
            scratch_shapes=[
                V((width, fw), BF16), V((width, fw), BF16), V((fw, width), BF16),
                V((n, fw), BF16), V((n, fw), BF16), V((n, fw), BF16), V((n // 2, fw), BF16),
                V((2, 2) + tok, BF16), V((2, 2) + tok, BF16),
                V((2, 4, 2, micro, rows, wr), BF16), V((2, 4, 2, micro, rows, wr), BF16),
                V((1, 2) + tok_r, F32), V((2, 2) + tok_q, F32),
                V((2, 4, micro, rows, width // 4), F32), V((2, fw, width // 4), BF16), V((TW, wr, fw), F32),
                V((TR,) + tok_r, F32), V((TK,) + tok_q[1:], F32), V((WK, wr, wc), F32),
                dma((64,)), dma((COPIES,)), dma((COPIES,)),
            ],
            compiler_params=pltpu.CompilerParams(
                collective_id=0, has_side_effects=True, vmem_limit_bytes=67_000_000
            ),
        )(x_loc, dy_loc, wg, wu, wd)
        return finish(x_loc, dy_loc, *res[: len(outs)])

    return jax.shard_map(local_step, mesh=mesh, in_specs=in_specs, out_specs=out_specs, check_vma=False)
```
